32 devices in a mesh: shot: 8 (over y, x, core), slab: 4 (over z).
Axes of the slice: x: 2, y: 2, z: 4, core: 2. Of those that a mesh axis runs over, the one named last changes fastest.
Arguments:
- model_tiles: float32 [64, 32, 1024], P('shot', 'slab'), may hold values from -0.3 to 0.3
- background: float32 [8, 32, 128, 128], P('shot', 'slab'), may hold values from 0.05 to 0.18
- u_prev: float32 [8, 32, 128, 128], P('shot', 'slab'), may hold values from -6 to 6
- u_now: float32 [8, 32, 128, 128], P('shot', 'slab'), may hold values from -6 to 6
- du_prev: float32 [8, 32, 128, 128], P('shot', 'slab'), may hold values from -2 to 2
- du_now: float32 [8, 32, 128, 128], P('shot', 'slab'), may hold values from -2 to 2
- w_prev: float32 [8, 32, 128, 128], P('shot', 'slab'), may hold values from -6 to 6
- w_now: float32 [8, 32, 128, 128], P('shot', 'slab'), may hold values from -6 to 6
- wavelet: float32 [8, 3], P('shot'), may hold values from -4 to 4
- source_cell: int32 [8], P('shot'), may hold values from 0 to 524287
- receiver_cells: int32 [8, 256], P('shot'), may hold values from 0 to 524287
- aperture: int32 [8, 16], replicated, may hold values from 0 to 63, as said below
- tile_slot: int32 [64], replicated, may hold values from 0 to 63, as said below
Outputs:
- sensitivity: float32 [64, 32, 1024], P('shot', 'slab')
- u_final: float32 [8, 32, 128, 128], P('shot', 'slab')
- du_final: float32 [8, 32, 128, 128], P('shot', 'slab')
- w_final: float32 [8, 32, 128, 128], P('shot', 'slab')
- record: float32 [8, 3, 256], P('shot')
The draws below stay inside these ranges and needn't reach their ends.
Inputs may be any that keep to these rules, and one draw needn't show every extreme that they name: `aperture`: each row lists the 16 tiles of a square window of 4 x 4 tiles of the lateral tile grid (4 rows of 16 tiles, tile id = row * 4 * 4 + column), row by row; windows of different shots may intersect. `tile_slot`: A permutation of the 64 storage slots; slot q is stored by shot index q // 8 as its local tile q % 8. The shot indices fall into four sets of 2, each of which stores exactly 4 tiles of every aperture; so at most 4 tiles of one aperture lie on one shot index, and exactly 4 do for some shot index and aperture in every draw.
All inputs are finite; a program needn't handle non-finite values.
Results may differ from the reference program's by a relative error of at most 0.00002.
Values sent between devices are 32-bit elements; how exact they have to be, the bound alone decides.
No kernel may reach another device: no remote copies, remote signals or barrier semaphores. Data moves between devices by JAX's collectives and lax.ppermute only.
A program may use at most 128 MiB of HBM per device.

```python
import math
import jax
import jax.numpy as jnp
from jax import lax

TW = 32
AT = 4
LAT_DEV = 8
NREC = 256
STEPS = 3
CAP = 4
LAT = 64
NZ = 32
AW = 128
TC = 1024
N_SHOT = 8


def tile_layout(key):
    base_key = jax.random.fold_in(key, 11)
    subkeys = jax.random.split(base_key, 5)
    grid_cols = 4 * AT
    grid_rows = LAT // grid_cols
    corner_r = jax.random.randint(subkeys[0], (N_SHOT,), 0, grid_rows - AT + 1)
    corner_c = jax.random.randint(subkeys[1], (N_SHOT,), 0, grid_cols - AT + 1)
    places = jnp.arange(AT * AT, dtype=jnp.int32)
    aperture = (corner_r[:, None] + places[None, :] // AT) * grid_cols + corner_c[:, None] + places[None, :] % AT
    tile_ids = jnp.arange(LAT, dtype=jnp.int32)
    tile_class = tile_ids // grid_cols % AT * AT + tile_ids % grid_cols % AT
    class_order = jax.random.permutation(subkeys[2], AT * AT).astype(jnp.int32)
    class_set = jnp.zeros((AT * AT,), jnp.int32).at[class_order].set(jnp.arange(AT * AT, dtype=jnp.int32) // CAP)
    tile_set = class_set[tile_class]
    in_first = jnp.any(aperture[0][None, :] == tile_ids[:, None], axis=1)
    favour = jnp.where(in_first & (tile_set == 0), 0, 1)
    shuffle = jax.random.permutation(subkeys[3], LAT).astype(jnp.int32)
    scores = tile_set * (2 * LAT) + favour * LAT + shuffle
    ordering = jnp.argsort(scores).astype(jnp.int32)
    ordinal = jnp.arange(LAT, dtype=jnp.int32)
    per_set = LAT // 4
    owners_set = N_SHOT // 4
    owner_perm = jax.random.permutation(subkeys[4], N_SHOT).astype(jnp.int32)
    within = ordinal % per_set
    owner_of = owner_perm[ordinal // per_set * owners_set + within // LAT_DEV]
    slot_values = owner_of * LAT_DEV + within % LAT_DEV
    tile_slot = jnp.zeros((LAT,), jnp.int32).at[ordering].set(slot_values)
    return (aperture.astype(jnp.int32), tile_slot)


def draw_aperture(key, part):
    return tile_layout(key)[0]


def draw_tile_slot(key, part):
    return tile_layout(key)[1]


def touch_ends(drawn, stream_key, smallest, high):
    spot = [jax.random.randint(jax.random.fold_in(stream_key, axis), (), 0, length) for axis, length in enumerate(drawn.shape)]
    longest = drawn.shape.index(max(drawn.shape))
    neighbour = spot[:longest] + [(spot[longest] + 1) % drawn.shape[longest]] + spot[longest + 1:]
    return drawn.at[tuple(spot)].set(smallest).at[tuple(neighbour)].set(high)


def levels(rng, dims, shards, smallest, largest):
    def one(axis_at, shards_of):
        steps = jax.random.uniform(jax.random.fold_in(jax.random.fold_in(rng, 6), axis_at), (shards_of,), jnp.float32, smallest / len(shards), largest / len(shards))
        return jnp.repeat(jnp.exp(steps), dims[axis_at] // shards_of).reshape((-1,) + (1,) * (len(dims) - axis_at - 1))

    level = one(*shards[0])
    for cut in shards[1:]:
        level = level * one(*cut)
    return level


def centred(stream_key, extent, width, limit, pieces=(), kind=jnp.bfloat16):
    loudness = levels(stream_key, extent, pieces, -0.22, 0.18) if pieces else 1.0
    array = jax.random.normal(stream_key, extent, jnp.float32) * width * loudness
    return jnp.minimum(jnp.maximum(array, -limit), limit).astype(kind)


def setup_inputs(seed: int = 0) -> dict:
    streams_of = jax.random.split(jax.random.key(seed), 14)
    model_tiles = centred(streams_of[0], (LAT, NZ, TC), 0.05, 0.3, ((0, 8), (1, 4)), jnp.float32)
    background = jnp.clip(jnp.exp(math.log(0.18) - 1.2809339 * jax.random.uniform(streams_of[1], (N_SHOT, NZ, AW, AW), jnp.float32) ** levels(streams_of[1], (N_SHOT, NZ, AW, AW), ((0, 8), (1, 4)), -0.2, 0.2)), 0.05, 0.18)
    u_prev = centred(streams_of[2], (N_SHOT, NZ, AW, AW), 1.0, 6.0, ((0, 8), (1, 4)), jnp.float32)
    u_now = centred(streams_of[3], (N_SHOT, NZ, AW, AW), 1.0, 6.0, ((0, 8), (1, 4)), jnp.float32)
    du_prev = centred(streams_of[4], (N_SHOT, NZ, AW, AW), 0.3, 2.0, ((0, 8), (1, 4)), jnp.float32)
    du_now = centred(streams_of[5], (N_SHOT, NZ, AW, AW), 0.3, 2.0, ((0, 8), (1, 4)), jnp.float32)
    w_prev = centred(streams_of[6], (N_SHOT, NZ, AW, AW), 1.0, 6.0, ((0, 8), (1, 4)), jnp.float32)
    w_now = centred(streams_of[7], (N_SHOT, NZ, AW, AW), 1.0, 6.0, ((0, 8), (1, 4)), jnp.float32)
    wavelet = centred(streams_of[8], (N_SHOT, STEPS), 1.0, 4.0, ((0, 8),), jnp.float32)
    source_cell = touch_ends(jax.random.randint(streams_of[9], (N_SHOT,), 0, NZ * AW * AW), jax.random.fold_in(streams_of[9], 1), 0, (NZ * AW * AW) - 1).astype(jnp.int32)
    receiver_cells = touch_ends(jax.random.randint(streams_of[10], (N_SHOT, NREC), 0, NZ * AW * AW), jax.random.fold_in(streams_of[10], 1), 0, (NZ * AW * AW) - 1).astype(jnp.int32)
    aperture = draw_aperture(jax.random.fold_in(streams_of[13], 71), 0)
    tile_slot = draw_tile_slot(jax.random.fold_in(streams_of[13], 71), 0)
    return dict(model_tiles=model_tiles, background=background, u_prev=u_prev, u_now=u_now, du_prev=du_prev, du_now=du_now, w_prev=w_prev, w_now=w_now, wavelet=wavelet, source_cell=source_cell, receiver_cells=receiver_cells, aperture=aperture, tile_slot=tile_slot)


COEFFS = (-205.0 / 72.0, 8.0 / 5.0, -1.0 / 5.0, 8.0 / 315.0, -1.0 / 560.0)


def stencil(padded, depth_cells, side_cells):
    def window(along_z, along_x, along_y):
        return padded[..., 4 + along_z:4 + along_z + depth_cells, 4 + along_x:4 + along_x + side_cells, 4 + along_y:4 + along_y + side_cells]

    result_sum = 3.0 * COEFFS[0] * window(0, 0, 0)
    for offset in range(1, 5):
        cycle_sum = window(offset, 0, 0) + window(-offset, 0, 0) + window(0, offset, 0) + window(0, -offset, 0) + window(0, 0, offset) + window(0, 0, -offset)
        result_sum = result_sum + COEFFS[offset] * cycle_sum
    return result_sum


def laplace(field):
    return stencil(jnp.pad(field, 4), field.shape[0], field.shape[1])


def reference(model_tiles, background, u_prev, u_now, du_prev, du_now, w_prev, w_now, wavelet, source_cell, receiver_cells, aperture, tile_slot):
    def one_shot(inputs):
        speed_sq, older_u, newer_u, older_d, newer_d, older_w, newer_w, pulses, source_index, receiver_index, window_tiles = inputs
        chosen = model_tiles[tile_slot[window_tiles]]
        perturb = chosen.reshape(AT, AT, NZ, TW, TW).transpose(2, 0, 3, 1, 4).reshape(NZ, AW, AW)
        correlate = jnp.zeros((NZ, AW, AW), jnp.float32)
        traces = []
        for step_index in range(STEPS):
            lap_u = laplace(newer_u)
            lap_d = laplace(newer_d)
            lap_w = laplace(newer_w)
            correlate = correlate + lap_u * newer_w
            next_u = 2.0 * newer_u - older_u + speed_sq * lap_u
            next_u = next_u.reshape(-1).at[source_index].add(pulses[step_index]).reshape(NZ, AW, AW)
            next_d = 2.0 * newer_d - older_d + speed_sq * lap_d + perturb * lap_u
            sample = next_d.reshape(-1)[receiver_index]
            next_w = (2.0 * newer_w - older_w + speed_sq * lap_w).reshape(-1).at[receiver_index].add(sample).reshape(NZ, AW, AW)
            traces.append(sample)
            older_u, newer_u = newer_u, next_u
            older_d, newer_d = newer_d, next_d
            older_w, newer_w = newer_w, next_w
        sens_tiles = correlate.reshape(NZ, AT, TW, AT, TW).transpose(1, 3, 0, 2, 4).reshape(AT * AT, NZ, TW * TW)
        return newer_u, newer_d, newer_w, jnp.stack(traces), sens_tiles

    final_u, final_d, final_w, record, sens_all = lax.map(one_shot, (background, u_prev, u_now, du_prev, du_now, w_prev, w_now, wavelet, source_cell, receiver_cells, aperture))
    targets = tile_slot[aperture].reshape(-1).astype(jnp.int32)
    sensitivity = jnp.zeros((LAT, NZ, TW * TW), jnp.float32).at[targets].add(sens_all.reshape(-1, NZ, TW * TW))
    return sensitivity, final_u, final_d, final_w, record
```

```python
import functools
import math

import jax
import jax.numpy as jnp
from jax import lax
from jax.experimental import pallas as pl
from jax.experimental.pallas import tpu as pltpu
from jax.sharding import PartitionSpec as P

COEFFS = (-205.0 / 72.0, 8.0 / 5.0, -1.0 / 5.0, 8.0 / 315.0, -1.0 / 560.0)
HALO = len(COEFFS) - 1
SUB = 8
F32 = jnp.float32
VMEM = pl.BlockSpec(memory_space=pltpu.VMEM)
SMEM = pl.BlockSpec(memory_space=pltpu.SMEM)


def params(mib):
    return pltpu.CompilerParams(vmem_limit_bytes=mib * 1024 * 1024)


def sds(shape, dtype=F32):
    return jax.ShapeDtypeStruct(shape, dtype)


def fill_pad(pad_ref, now_ref, below_ref, above_ref):
    depth, side, _ = now_ref.shape
    zeros = jnp.zeros((SUB, side), F32)
    for z in range(HALO):
        pad_ref[z, pl.ds(SUB, side), :] = below_ref[z]
        pad_ref[HALO + depth + z, pl.ds(SUB, side), :] = above_ref[z]

    def plane(z, carry):
        pad_ref[HALO + z, pl.ds(0, SUB), :] = zeros
        pad_ref[HALO + z, pl.ds(SUB + side, SUB), :] = zeros
        pad_ref[HALO + z, pl.ds(SUB, side), :] = now_ref[z]
        return carry

    lax.fori_loop(0, depth, plane, 0)


def each_laplacian(pad_ref, depth, side, emit, rows=16):
    lane = lax.broadcasted_iota(jnp.int32, (rows, side), 1)
    left = [None] + [jnp.where(lane >= k, COEFFS[k], 0.0).astype(F32) for k in range(1, HALO + 1)]
    right = [None] + [jnp.where(lane < side - k, COEFFS[k], 0.0).astype(F32) for k in range(1, HALO + 1)]

    def plane(z, carry):
        for row in range(0, side, rows):
            centre = pad_ref[HALO + z, pl.ds(SUB + row, rows), :]
            total = (3.0 * COEFFS[0]) * centre
            for k in range(1, HALO + 1):
                ring = (
                    pad_ref[HALO + z + k, pl.ds(SUB + row, rows), :]
                    + pad_ref[HALO + z - k, pl.ds(SUB + row, rows), :]
                ) + (
                    pad_ref[HALO + z, pl.ds(SUB + row + k, rows), :]
                    + pad_ref[HALO + z, pl.ds(SUB + row - k, rows), :]
                )
                total = total + COEFFS[k] * ring
                total = total + (
                    left[k] * pltpu.roll(centre, k, 1) + right[k] * pltpu.roll(centre, side - k, 1)
                )
            emit(z, pl.ds(row, rows), centre, total)
        return carry

    lax.fori_loop(0, depth, plane, 0)


def copy_sends(next_ref, sends):
    if sends:
        down_ref, up_ref = sends
        depth = next_ref.shape[0]
        for z in range(HALO):
            down_ref[z] = next_ref[z]
            up_ref[z] = next_ref[depth - HALO + z]


def u_kernel(step, last, where_ref, wavelet_ref, source_ref, now_ref, prev_ref, below_ref, above_ref, speed_ref, w_ref, *rest):
    if step:
        corr_in, rest = rest[0], rest[1:]
    next_ref, lap_ref, corr_ref, *sends, pad_ref = rest
    depth, side, _ = now_ref.shape
    fill_pad(pad_ref, now_ref, below_ref, above_ref)

    def emit(z, block, centre, lap):
        lap_ref[z, block, :] = lap
        part = lap * w_ref[z, block, :]
        corr_ref[z, block, :] = corr_in[z, block, :] + part if step else part
        next_ref[z, block, :] = (2.0 * centre - prev_ref[z, block, :]) + speed_ref[z, block, :] * lap

    each_laplacian(pad_ref, depth, side, emit)
    local = source_ref[0] - where_ref[0]

    @pl.when((local >= 0) & (local < depth * side * side))
    def _():
        z = lax.div(local, side * side)
        x = lax.rem(lax.div(local, side), side)
        y = lax.rem(local, side)
        lane = lax.broadcasted_iota(jnp.int32, (1, side), 1)
        row = next_ref[z, pl.ds(x, 1), :]
        next_ref[z, pl.ds(x, 1), :] = row + jnp.where(lane == y, wavelet_ref[0, step], 0.0)

    copy_sends(next_ref, sends)


def d_kernel(now_ref, prev_ref, below_ref, above_ref, speed_ref, perturb_ref, lap_u_ref, *rest):
    next_ref, *sends, pad_ref = rest
    depth, side, _ = now_ref.shape
    fill_pad(pad_ref, now_ref, below_ref, above_ref)

    def emit(z, block, centre, lap):
        next_ref[z, block, :] = (
            (2.0 * centre - prev_ref[z, block, :])
            + speed_ref[z, block, :] * lap
            + perturb_ref[z, block, :] * lap_u_ref[z, block, :]
        )

    each_laplacian(pad_ref, depth, side, emit)
    copy_sends(next_ref, sends)


def w_kernel(now_ref, prev_ref, below_ref, above_ref, speed_ref, count_ref, d_next_ref, *rest):
    next_ref, *sends, pad_ref = rest
    depth, side, _ = now_ref.shape
    fill_pad(pad_ref, now_ref, below_ref, above_ref)

    def emit(z, block, centre, lap):
        next_ref[z, block, :] = (
            (2.0 * centre - prev_ref[z, block, :])
            + speed_ref[z, block, :] * lap
            + count_ref[z, block, :] * d_next_ref[z, block, :]
        )

    each_laplacian(pad_ref, depth, side, emit)
    copy_sends(next_ref, sends)


def wave_call(body, name, args, n_smem, last, extra_outs):
    depth, side, _ = args[n_smem].shape
    field = sds((depth, side, side))
    halo = sds((HALO, side, side))
    outs = [field] * (1 + extra_outs) + ([] if last else [halo, halo])
    return pl.pallas_call(
        body,
        out_shape=outs,
        in_specs=[SMEM] * n_smem + [VMEM] * (len(args) - n_smem),
        out_specs=[VMEM] * len(outs),
        scratch_shapes=[pltpu.VMEM((depth + 2 * HALO, side + 2 * SUB, side), F32)],
        compiler_params=params(16),
        cost_estimate=pl.CostEstimate(flops=60 * depth * side * side, transcendentals=0, bytes_accessed=0),
        name=name,
    )(*args)


def count_kernel(where_ref, cells_ref, count_ref):
    depth, side, _ = count_ref.shape
    local = cells_ref[...] - where_ref[0]
    n = local.shape[1]
    row_of = jnp.where(local >= 0, lax.div(local, side), -1)
    lane_of = lax.rem(jnp.maximum(local, 0), side)
    lanes = lax.broadcasted_iota(jnp.int32, (side, n), 0)
    lane_hot = jnp.where(lanes == lane_of, 1.0, 0.0).astype(jnp.bfloat16)
    rows = lax.broadcasted_iota(jnp.int32, (side, n), 0)

    def plane(z, carry):
        row_hot = jnp.where(rows + z * side == row_of, 1.0, 0.0).astype(jnp.bfloat16)
        count_ref[z] = lax.dot_general(
            row_hot, lane_hot, (((1,), (1,)), ((), ())), preferred_element_type=F32
        )
        return carry

    lax.fori_loop(0, depth, plane, 0)


def count_call(where, cells, depth, side):
    return pl.pallas_call(
        count_kernel,
        out_shape=sds((depth, side, side)),
        in_specs=[SMEM, VMEM],
        out_specs=VMEM,
        compiler_params=params(8),
        name="count",
    )(where, cells)


def record_kernel(where_ref, cells_smem, cells_ref, *rest):
    *fields, out_ref, rows_ref = rest
    depth, side, _ = fields[0].shape
    n = cells_ref.shape[1]
    total = depth * side * side
    local = cells_ref[...] - where_ref[0]
    mine = (local >= 0) & (local < total)
    lane_of = jnp.where(mine, lax.rem(jnp.maximum(local, 0), side), -1)
    lanes = lax.broadcasted_iota(jnp.int32, (side, n), 0)
    hit = lanes == lane_of
    for step, field_ref in enumerate(fields):

        def gather(r, carry):
            cell = jnp.clip(cells_smem[0, r] - where_ref[0], 0, total - 1)
            z = lax.div(cell, side * side)
            x = lax.rem(lax.div(cell, side), side)
            rows_ref[pl.ds(r, 1), :] = field_ref[z, pl.ds(x, 1), :]
            return carry

        lax.fori_loop(0, n, gather, 0, unroll=8)
        turned = rows_ref[...].T
        out_ref[pl.ds(step, 1), :] = jnp.sum(jnp.where(hit, turned, 0.0), axis=0, keepdims=True)


def record_call(where, cells, fields):
    side = fields[0].shape[-1]
    n = cells.shape[1]
    return pl.pallas_call(
        record_kernel,
        out_shape=sds((len(fields), n)),
        in_specs=[SMEM, SMEM, VMEM] + [VMEM] * len(fields),
        out_specs=VMEM,
        scratch_shapes=[pltpu.VMEM((n, side), F32)],
        compiler_params=params(8),
        name="record",
    )(where, cells, cells, *fields)


def swap_segments(parts, segment):
    count = len(parts)
    lanes = count * segment
    lane = lax.broadcasted_iota(jnp.int32, parts[0].shape, 1)
    parts = list(parts)
    bit = count // 2
    while bit:
        low = lax.rem(lax.div(lane, bit * segment), 2) == 0
        for a in range(count):
            if not a & bit:
                first, second = parts[a], parts[a + bit]
                parts[a] = jnp.where(low, first, pltpu.roll(second, bit * segment, 1))
                parts[a + bit] = jnp.where(low, pltpu.roll(first, lanes - bit * segment, 1), second)
        bit //= 2
    return parts


def ranks(aperture_ref, slot_ref, shot, lat_dev, seen_ref, visit):
    for h in range(seen_ref.shape[0]):
        seen_ref[h] = 0
    for p in range(aperture_ref.shape[1]):
        slot = slot_ref[aperture_ref[shot, p]]
        holder = lax.div(slot, lat_dev)
        rank = seen_ref[holder]
        seen_ref[holder] = rank + 1
        visit(p, holder, lax.rem(slot, lat_dev), rank)


def pack_kernel(where_ref, aperture_ref, slot_ref, tiles_ref, out_ref, table_ref):
    lat_dev = tiles_ref.shape[0]
    n_shot, capacity = out_ref.shape[:2]
    me = where_ref[1]
    n_tiles = aperture_ref.shape[1]

    def shot(s, carry):
        for r in range(capacity):
            table_ref[s * (capacity + 1) + r] = 0

        def tile(p, seen):
            slot = slot_ref[aperture_ref[s, p]]
            mine = lax.div(slot, lat_dev) == me

            @pl.when(mine)
            def _():
                table_ref[s * (capacity + 1) + seen] = lax.rem(slot, lat_dev)

            return seen + mine.astype(jnp.int32)

        table_ref[s * (capacity + 1) + capacity] = lax.fori_loop(0, n_tiles, tile, jnp.int32(0), unroll=4)
        for r in range(capacity):
            out_ref[s, r] = tiles_ref[table_ref[s * (capacity + 1) + r]]
        return carry

    lax.fori_loop(0, n_shot, shot, 0)


def pack_call(where, aperture, tile_slot, model_tiles, capacity):
    n_shot = aperture.shape[0]
    lat_dev, depth, cells = model_tiles.shape
    return pl.pallas_call(
        pack_kernel,
        out_shape=[sds((n_shot, capacity, depth, cells)), sds((n_shot * (capacity + 1),), jnp.int32)],
        in_specs=[SMEM, SMEM, SMEM, VMEM],
        out_specs=[VMEM, SMEM],
        compiler_params=params(8),
        name="pack",
    )(where, aperture, tile_slot, model_tiles)


def perturb_kernel(where_ref, aperture_ref, slot_ref, in_ref, out_ref, seen_ref, place_ref, *, lat_dev, tile_side):
    capacity, depth, cells = in_ref.shape[1:]
    side = out_ref.shape[1]
    across = side // tile_side
    flat_ref = out_ref.reshape(depth * side, side)

    def visit(p, holder, slot, rank):
        place_ref[p] = holder * capacity + rank

    ranks(aperture_ref, slot_ref, where_ref[1], lat_dev, seen_ref, visit)

    def tile_row(i, carry):
        for high in range(cells // side):
            parts = []
            for j in range(across):
                place = place_ref[i * across + j]
                parts.append(in_ref[lax.div(place, capacity), lax.rem(place, capacity), :, pl.ds(high * side, side)])
            for low, part in enumerate(swap_segments(parts, tile_side)):
                flat_ref[pl.ds(i * tile_side + high * across + low, depth, stride=side), :] = part
        return carry

    lax.fori_loop(0, across, tile_row, 0)


def perturb_call(where, aperture, tile_slot, incoming, side, lat_dev, tile_side):
    depth = incoming.shape[2]
    n_shot = incoming.shape[0]
    return pl.pallas_call(
        functools.partial(perturb_kernel, lat_dev=lat_dev, tile_side=tile_side),
        out_shape=sds((depth, side, side)),
        in_specs=[SMEM, SMEM, SMEM, VMEM],
        out_specs=VMEM,
        scratch_shapes=[pltpu.SMEM((n_shot,), jnp.int32), pltpu.SMEM((aperture.shape[1],), jnp.int32)],
        compiler_params=params(8),
        name="perturb",
    )(where, aperture, tile_slot, incoming)


def back_kernel(where_ref, aperture_ref, slot_ref, corr_ref, out_ref, seen_ref, place_ref, *, lat_dev, tile_side):
    n_shot, capacity, depth, cells = out_ref.shape
    side = corr_ref.shape[1]
    across = side // tile_side
    flat_ref = corr_ref.reshape(depth * side, side)

    def visit(p, holder, slot, rank):
        place_ref[p] = holder * capacity + rank

    ranks(aperture_ref, slot_ref, where_ref[1], lat_dev, seen_ref, visit)

    def clear(s, carry):
        for r in range(capacity):
            out_ref[s, r] = jnp.zeros((depth, cells), F32)
        return carry

    lax.fori_loop(0, n_shot, clear, 0)

    def tile_row(i, carry):
        for high in range(cells // side):
            parts = [
                flat_ref[pl.ds(i * tile_side + high * across + low, depth, stride=side), :] for low in range(across)
            ]
            for j, part in enumerate(swap_segments(parts, tile_side)):
                place = place_ref[i * across + j]
                out_ref[lax.div(place, capacity), lax.rem(place, capacity), :, pl.ds(high * side, side)] = part
        return carry

    lax.fori_loop(0, across, tile_row, 0)


def back_call(where, aperture, tile_slot, corr, n_shot, capacity, lat_dev, tile_side):
    depth = corr.shape[0]
    return pl.pallas_call(
        functools.partial(back_kernel, lat_dev=lat_dev, tile_side=tile_side),
        out_shape=sds((n_shot, capacity, depth, tile_side * tile_side)),
        in_specs=[SMEM, SMEM, SMEM, VMEM],
        out_specs=VMEM,
        scratch_shapes=[pltpu.SMEM((n_shot,), jnp.int32), pltpu.SMEM((aperture.shape[1],), jnp.int32)],
        compiler_params=params(8),
        name="back",
    )(where, aperture, tile_slot, corr)


def sum_kernel(table_ref, in_ref, out_ref):
    n_shot, capacity = in_ref.shape[:2]
    out_ref[...] = jnp.zeros(out_ref.shape, F32)

    def shot(s, carry):
        base = s * (capacity + 1)
        for r in range(capacity):

            @pl.when(r < table_ref[base + capacity])
            def _():
                slot = table_ref[base + r]
                out_ref[slot] = out_ref[slot] + in_ref[s, r]

        return carry

    lax.fori_loop(0, n_shot, shot, 0)


def sum_call(table, arrived, lat_dev):
    depth, cells = arrived.shape[2:]
    return pl.pallas_call(
        sum_kernel,
        out_shape=sds((lat_dev, depth, cells)),
        in_specs=[SMEM, VMEM],
        out_specs=VMEM,
        compiler_params=params(8),
        name="gather_sum",
    )(table, arrived)


def halos(down, up):
    count = lax.axis_size("slab")
    below = lax.ppermute(up, "slab", [(i, i + 1) for i in range(count - 1)])
    above = lax.ppermute(down, "slab", [(i + 1, i) for i in range(count - 1)])
    return below, above


def slab_sum(part):
    count = lax.axis_size("slab")
    total = part
    for shift in range(1, count):
        total = total + lax.ppermute(part, "slab", [(i, (i + shift) % count) for i in range(count)])
    return total


def per_device(
    model_tiles,
    background,
    u_prev,
    u_now,
    du_prev,
    du_now,
    w_prev,
    w_now,
    wavelet,
    source_cell,
    receiver_cells,
    aperture,
    tile_slot,
):
    lat_dev, depth, tile_cells = model_tiles.shape
    side = background.shape[-1]
    tile_side = math.isqrt(tile_cells)
    capacity = aperture.shape[1] // 4
    n_shot = lax.axis_size("shot")
    steps = wavelet.shape[1]
    cells_dev = depth * side * side
    where = jnp.stack([lax.axis_index("slab") * cells_dev, lax.axis_index("shot")]).astype(jnp.int32)
    speed = background[0]
    u, d, w = u_now[0], du_now[0], w_now[0]
    up_, dp_, wp_ = u_prev[0], du_prev[0], w_prev[0]

    u_halo = halos(u[:HALO], u[depth - HALO :])
    d_halo = halos(d[:HALO], d[depth - HALO :])
    w_halo = halos(w[:HALO], w[depth - HALO :])
    outgoing, table = pack_call(where, aperture, tile_slot, model_tiles, capacity)
    incoming = lax.all_to_all(outgoing, "shot", split_axis=0, concat_axis=0, tiled=True)
    count = count_call(where, receiver_cells, depth, side)
    perturb = perturb_call(where, aperture, tile_slot, incoming, side, lat_dev, tile_side)

    corr = None
    d_fields = []
    for step in range(steps):
        last = step == steps - 1
        args = [where, wavelet, source_cell, u, up_, *u_halo, speed, w] + ([corr] if step else [])
        u_next, lap_u, corr, *sends = wave_call(
            functools.partial(u_kernel, step, last), f"u{step}", args, 3, last, 2
        )
        if sends:
            u_halo = halos(*sends)
        d_next, *sends = wave_call(d_kernel, f"d{step}", [d, dp_, *d_halo, speed, perturb, lap_u], 0, last, 0)
        if sends:
            d_halo = halos(*sends)
        w_next, *sends = wave_call(w_kernel, f"w{step}", [w, wp_, *w_halo, speed, count, d_next], 0, last, 0)
        if sends:
            w_halo = halos(*sends)
        d_fields.append(d_next)
        u, up_ = u_next, u
        d, dp_ = d_next, d
        w, wp_ = w_next, w
    returning = back_call(where, aperture, tile_slot, corr, n_shot, capacity, lat_dev, tile_side)
    arrived = lax.all_to_all(returning, "shot", split_axis=0, concat_axis=0, tiled=True)
    sensitivity = sum_call(table, arrived, lat_dev)
    traces = slab_sum(record_call(where, receiver_cells, d_fields))
    return (sensitivity, u[None], d[None], w[None], traces[None])


def solution(mesh):
    field = P("shot", "slab", None, None)
    tiles = P("shot", "slab", None)
    in_specs = (tiles,) + (field,) * 7 + (P("shot", None), P("shot"), P("shot", None), P(), P())
    out_specs = (tiles, field, field, field, P("shot", None, None))
    return jax.shard_map(
        per_device, mesh=mesh, in_specs=in_specs, out_specs=out_specs, check_vma=False
    )
```

```python
import functools
import math

import jax
import jax.numpy as jnp
from jax import lax
from jax.experimental import pallas as pl
from jax.experimental.pallas import tpu as pltpu
from jax.sharding import PartitionSpec as P


COEFFS = (-205.0 / 72.0, 8.0 / 5.0, -1.0 / 5.0, 8.0 / 315.0, -1.0 / 560.0)
HALO = len(COEFFS) - 1
SUB = 8
F32 = jnp.float32
VMEM = pl.BlockSpec(memory_space=pltpu.VMEM)
SMEM = pl.BlockSpec(memory_space=pltpu.SMEM)
HBM = pl.BlockSpec(memory_space=pltpu.HBM)


def params(mib):
    return pltpu.CompilerParams(vmem_limit_bytes=mib * 1024 * 1024)


def sds(shape, dtype=F32):
    return jax.ShapeDtypeStruct(shape, dtype)


def place():
    slab, count = lax.axis_index("slab"), lax.axis_size("slab")
    odd = lax.bitwise_and(slab, 1)
    above, below = slab < count - 1, slab > 0
    is_odd = odd == 1
    return odd, (is_odd & below) | (~is_odd & above), (is_odd & above) | (~is_odd & below)


def quotient(x, m):
    return lax.shift_right_logical(x, m.bit_length() - 1) if m & (m - 1) == 0 else lax.div(x, m)


def remainder(x, m):
    return lax.bitwise_and(x, m - 1) if m & (m - 1) == 0 else lax.rem(x, m)


SCALE = 5040.0
PARTS = 4


def band_weights(side):
    i = lax.broadcasted_iota(jnp.int32, (2 * side, 2 * side), 0)
    j = lax.broadcasted_iota(jnp.int32, (2 * side, 2 * side), 1)
    far = jnp.where((i < side) == (j < side), jnp.abs(i - j), 0)
    out = jnp.zeros((2 * side, 2 * side), F32)
    for k in range(1, HALO + 1):
        out = jnp.where(far == k, round(COEFFS[k] * SCALE) * 1.0, out)
    out = out.astype(jnp.bfloat16)
    return jnp.concatenate([out, out, out], axis=0)


def split3(x):
    high = x.astype(jnp.bfloat16)
    rest = x - high.astype(F32)
    mid = rest.astype(jnp.bfloat16)
    low = (rest - mid.astype(F32)).astype(jnp.bfloat16)
    return high, mid, low


def prepare(work, now_ref, first_ref, second_ref, index, weights, inject=None):
    rows_ref, halo_ref, lanes_ref = work
    depth, side, _ = now_ref.shape
    odd, has_first, has_second = place()
    zeros = jnp.zeros((SUB, side), F32)
    half = depth // 2
    parts = []
    for low, high in zip(split3(now_ref[pl.ds(0, half)]), split3(now_ref[pl.ds(half, half)])):
        parts += [low.reshape(half * side, side), high.reshape(half * side, side)]
    lanes = jnp.dot(jnp.concatenate(parts, axis=1), weights, preferred_element_type=F32)
    lanes_ref[pl.ds(0, half)] = lanes[:, :side].reshape(half, side, side)
    lanes_ref[pl.ds(half, half)] = lanes[:, side:].reshape(half, side, side)
    for z in range(depth):
        rows_ref[z, pl.ds(0, SUB), :] = zeros
        rows_ref[z, pl.ds(SUB + side, SUB), :] = zeros
        rows_ref[z, pl.ds(SUB, side), :] = now_ref[z]

    def halo(z, carry):
        halo_ref[1 - odd, z] = jnp.where(has_first, first_ref[index, z], 0.0)
        halo_ref[odd, z] = jnp.where(has_second, second_ref[index, z], 0.0)
        return carry

    lax.fori_loop(0, HALO, halo, 0)
    if inject:
        outer_ref, other_ref = inject
        for end in range(2):
            for z in range(HALO):
                halo_ref[end, z] = halo_ref[end, z] + outer_ref[end, z] * other_ref[end, z]


def each_laplacian(work, now_ref, emit, finish=None, parts=1):
    rows_ref, halo_ref, lanes_ref = work
    depth, side, _ = now_ref.shape

    def block(g, carry):
        start = pl.multiple_of(g * SUB, SUB)
        rows = pl.ds(start, SUB)
        column = [halo_ref[0, z, rows, :] for z in range(HALO)]
        column += [now_ref[z, rows, :] for z in range(depth)]
        column += [halo_ref[1, z, rows, :] for z in range(HALO)]
        for z in range(depth):
            centre = column[HALO + z]
            total = (3.0 * COEFFS[0]) * centre + (1.0 / SCALE) * lanes_ref[z, rows, :]
            for k in range(1, HALO + 1):
                ring = (column[HALO + z + k] + column[HALO + z - k]) + (
                    rows_ref[z, pl.ds(start + (SUB + k), SUB), :] + rows_ref[z, pl.ds(start + (SUB - k), SUB), :]
                )
                total = total + COEFFS[k] * ring
            emit(z, rows, centre, total)
        return carry

    blocks = side // SUB // parts
    for part in range(parts):
        lax.fori_loop(part * blocks, (part + 1) * blocks, block, 0)
        if finish:
            finish(part, parts)


def work_space(depth, side):
    return [
        pltpu.VMEM((depth, side + 2 * SUB, side), F32),
        pltpu.VMEM((2, HALO, side, side), F32),
        pltpu.VMEM((depth, side, side), F32),
    ]


def copy_sends(next_ref, first_ref, second_ref, index):
    depth = next_ref.shape[0]
    odd = place()[0] == 1
    first = jnp.where(odd, 0, depth - HALO)
    second = jnp.where(odd, depth - HALO, 0)
    for z in range(HALO):
        first_ref[index, z] = next_ref[first + z]
        second_ref[index, z] = next_ref[second + z]


def store_out(next_ref, out_ref, sems, step, steps):
    rows = pl.ds(step * (next_ref.shape[1] // steps), next_ref.shape[1] // steps)
    return pltpu.make_async_copy(next_ref.at[:, rows], out_ref.at[0, :, rows], sems.at[step])


class Refs:
    def __init__(self, refs):
        self.refs = list(refs)

    def take(self, n=None):
        if n is None:
            return self.refs.pop(0)
        return [self.refs.pop(0) for _ in range(n)]


def u_kernel(step, last, tiles, *refs):
    refs = Refs(refs)
    source_ref, wavelet_ref, now_ref, prev_ref, ha_ref, hb_ref, speed_ref, w_ref = refs.take(8)
    corr_in = refs.take() if step else None
    if last:
        tables = refs.take(2)
        out_ref, lap_ref = refs.take(2)
        blocks = refs.take(tiles[0])
        sends = []
        next_ref, corr_ref = refs.take(2)
    else:
        next_ref, lap_ref, corr_ref = refs.take(3)
        sends = refs.take(2)
    work = refs.take(3)
    if last:
        fetched = refs.take(2)
        tiles_ref, seen_ref, place_ref, sems, table_sems = refs.take(5)
        copies = [pltpu.make_async_copy(a, b, table_sems.at[i]) for i, (a, b) in enumerate(zip(tables, fetched))]
        for copy in copies:
            copy.start()
    depth, side, _ = now_ref.shape
    prepare(work, now_ref, ha_ref, hb_ref, 0, band_weights(side))

    def emit(z, block, centre, lap):
        lap_ref[z, block, :] = lap
        part = lap * w_ref[z, block, :]
        corr_ref[z, block, :] = corr_in[z, block, :] + part if step else part
        next_ref[z, block, :] = (2.0 * centre - prev_ref[z, block, :]) + speed_ref[z, block, :] * lap

    local = source_ref[0] - lax.axis_index("slab") * (depth * side * side)
    mine = (local >= 0) & (local < depth * side * side)
    cell = jnp.where(mine, local, 0)
    z = quotient(cell, side * side)
    x = remainder(quotient(cell, side), side)
    lane = lax.broadcasted_iota(jnp.int32, (1, side), 1)
    add = jnp.where((lane == remainder(cell, side)) & mine, wavelet_ref[:, step : step + 1], 0.0)

    def finish(part, parts):
        size = side // parts

        @pl.when((x >= part * size) & (x < (part + 1) * size))
        def _():
            next_ref[z, pl.ds(x, 1), :] = next_ref[z, pl.ds(x, 1), :] + add

        if last:
            store_out(next_ref, out_ref, sems, part, parts).start()

    parts = PARTS if last else 1
    each_laplacian(work, now_ref, emit, finish, parts)
    if sends:
        copy_sends(next_ref, *sends, 0)
    if last:
        for copy in copies:
            copy.wait()
        pack_back(*tiles[1:], *fetched, corr_ref, blocks, tiles_ref, seen_ref, place_ref)
        for part in range(parts):
            store_out(next_ref, out_ref, sems, part, parts).wait()


def w_bare_kernel(index, now_ref, prev_ref, ha_ref, hb_ref, speed_ref, next_ref, *rest):
    sends, work = rest[:2], rest[2:]
    _, side, _ = now_ref.shape
    prepare(work, now_ref, ha_ref, hb_ref, index, band_weights(side))

    def emit(z, block, centre, lap):
        next_ref[z, block, :] = (2.0 * centre - prev_ref[z, block, :]) + speed_ref[z, block, :] * lap

    each_laplacian(work, now_ref, emit)
    copy_sends(next_ref, *sends, 0)


def d_kernel(index, now_ref, prev_ref, ha_ref, hb_ref, speed_ref, perturb_ref, lap_u_ref, bare_ref, count_ref, *rest):
    next_ref, w_ref, *sends = rest[:4]
    work = rest[4:]
    _, side, _ = now_ref.shape
    prepare(work, now_ref, ha_ref, hb_ref, index, band_weights(side))

    def emit(z, block, centre, lap):
        new = ((2.0 * centre - prev_ref[z, block, :]) + speed_ref[z, block, :] * lap) + (
            perturb_ref[z, block, :] * lap_u_ref[z, block, :]
        )
        next_ref[z, block, :] = new
        w_ref[z, block, :] = bare_ref[z, block, :] + count_ref[z, block, :] * new

    each_laplacian(work, now_ref, emit)
    copy_sends(next_ref, *sends, 0)


def dw_kernel(bare, *refs):
    refs = Refs(refs)
    speed_ref, d_ref, d_prev, w_ref, w_prev, perturb_ref, lap_u_ref, count_ref = refs.take(8)
    d_halo, w_halo = refs.take(2), refs.take(2)
    outer_ref = refs.take() if bare else None
    d_next, w_next = refs.take(2)
    d_sends, w_sends = refs.take(2), refs.take(2)
    d_work, w_work = refs.take(3), refs.take(3)
    _, side, _ = speed_ref.shape
    weights = band_weights(side)
    prepare(d_work, d_ref, *d_halo, 0, weights)
    prepare(w_work, w_ref, *w_halo, 0, weights, (outer_ref, d_work[1]) if bare else None)

    def emit_d(z, block, centre, lap):
        d_next[z, block, :] = ((2.0 * centre - d_prev[z, block, :]) + speed_ref[z, block, :] * lap) + (
            perturb_ref[z, block, :] * lap_u_ref[z, block, :]
        )

    def emit_w(z, block, centre, lap):
        w_next[z, block, :] = ((2.0 * centre - w_prev[z, block, :]) + speed_ref[z, block, :] * lap) + (
            count_ref[z, block, :] * d_next[z, block, :]
        )

    each_laplacian(d_work, d_ref, emit_d)
    copy_sends(d_next, *d_sends, 0)
    each_laplacian(w_work, w_ref, emit_w)
    copy_sends(w_next, *w_sends, 0)


def last_d_kernel(before, *refs):
    refs = Refs(refs)
    now_ref, prev_ref, ha_ref, hb_ref, speed_ref, perturb_ref, lap_u_ref, cells_hbm, cells_ref = refs.take(9)
    early_ref = refs.take() if before else None
    out_ref, next_ref, record_ref = refs.take(3)
    work = refs.take(3)
    cells_smem, rows_ref, sems, table_sem = refs.take(4)
    fetch = pltpu.make_async_copy(cells_hbm, cells_smem, table_sem)
    fetch.start()
    _, side, _ = now_ref.shape
    prepare(work, now_ref, ha_ref, hb_ref, 0, band_weights(side))

    def emit(z, block, centre, lap):
        next_ref[z, block, :] = ((2.0 * centre - prev_ref[z, block, :]) + speed_ref[z, block, :] * lap) + (
            perturb_ref[z, block, :] * lap_u_ref[z, block, :]
        )

    def finish(part, parts):
        store_out(next_ref, out_ref, sems, part, parts).start()

    each_laplacian(work, now_ref, emit, finish, PARTS)
    fetch.wait()
    if before:
        record_ref[pl.ds(0, before), :] = early_ref[...]
    fields = [now_ref, next_ref] if record_ref.shape[0] > before + 1 else [next_ref]
    gather_records(before, cells_smem, cells_ref, fields, record_ref, rows_ref)
    for part in range(PARTS):
        store_out(next_ref, out_ref, sems, part, PARTS).wait()


def last_w_kernel(bare, *refs):
    refs = Refs(refs)
    now_ref, prev_ref, ha_ref, hb_ref, speed_ref, count_ref, d_next, table_hbm = refs.take(8)
    d_halo = refs.take(2) if bare else None
    outer_ref = refs.take() if bare else None
    blocks = refs.take(lax.axis_size("shot"))
    out_ref, sum_ref = refs.take(2)
    next_ref = refs.take()
    work = refs.take(3)
    table_ref, sems, table_sem = refs.take(3)
    fetch = pltpu.make_async_copy(table_hbm, table_ref, table_sem)
    fetch.start()
    _, side, _ = now_ref.shape
    prepare(work, now_ref, ha_ref, hb_ref, 0, band_weights(side))

    def emit(z, block, centre, lap):
        next_ref[z, block, :] = ((2.0 * centre - prev_ref[z, block, :]) + speed_ref[z, block, :] * lap) + (
            count_ref[z, block, :] * d_next[z, block, :]
        )

    def finish(part, parts):
        store_out(next_ref, out_ref, sems, part, parts).start()

    each_laplacian(work, now_ref, emit, finish, PARTS)
    fetch.wait()
    sum_tiles(table_ref, blocks, sum_ref)
    for part in range(PARTS):
        store_out(next_ref, out_ref, sems, part, PARTS).wait()


def stencil_call(body, in_specs, args, outs, kinds, scratch):
    return pl.pallas_call(
        body, out_shape=outs, in_specs=in_specs, out_specs=kinds, scratch_shapes=scratch, compiler_params=params(20)
    )(*args)


def u_call(step, last, wavelet, source, u, u_prev, halo, speed, w, corr, aperture, tile_slot, lat_dev, tile_side):
    field = sds(u.shape)
    edge = sds((1, HALO) + u.shape[1:])
    args = [source, wavelet, u, u_prev, *halo, speed, w] + ([corr] if step else [])
    specs = [SMEM] + [VMEM] * (len(args) - 1)
    scratch = work_space(*u.shape[:2])
    n_shot, n_tiles = aperture.shape
    cells = tile_side * tile_side
    capacity = n_tiles // 4
    if last:
        args += [aperture, tile_slot]
        specs += [HBM, HBM]
        outs = [sds((1,) + u.shape), field] + [sds((capacity, u.shape[0], cells))] * n_shot
        kinds = [HBM] + [VMEM] * (1 + n_shot)
        scratch = [pltpu.VMEM(u.shape, F32)] * 2 + scratch + [
            pltpu.SMEM(aperture.shape, jnp.int32),
            pltpu.SMEM(tile_slot.shape, jnp.int32),
            *tile_scratch(n_shot, capacity, u.shape[0], cells, n_tiles),
            pltpu.SemaphoreType.DMA((PARTS,)),
            pltpu.SemaphoreType.DMA((2,)),
        ]
    else:
        outs, kinds = [field] * 3 + [edge] * 2, [VMEM] * 5
    body = functools.partial(u_kernel, step, last, (n_shot, lat_dev, tile_side))
    return stencil_call(body, specs, args, outs, kinds, scratch)


def w_bare_call(w, w_prev, halo, index, speed):
    field, edge = sds(w.shape), sds((1, HALO) + w.shape[1:])
    args = [w, w_prev, *halo, speed]
    body = functools.partial(w_bare_kernel, index)
    return stencil_call(body, [VMEM] * 5, args, [field, edge, edge], [VMEM] * 3, work_space(*w.shape[:2]))


def d_call(d, d_prev, halo, index, speed, perturb, lap_u, bare, count):
    field, edge = sds(d.shape), sds((1, HALO) + d.shape[1:])
    args = [d, d_prev, *halo, speed, perturb, lap_u, bare, count]
    body = functools.partial(d_kernel, index)
    outs = [field, field, edge, edge]
    return stencil_call(body, [VMEM] * 9, args, outs, [VMEM] * 4, work_space(*d.shape[:2]))


def dw_call(d, d_prev, w, w_prev, d_halo, w_halo, speed, perturb, lap_u, count, outer):
    field, edge = sds(d.shape), sds((1, HALO) + d.shape[1:])
    bare = outer is not None
    args = [speed, d, d_prev, w, w_prev, perturb, lap_u, count, *d_halo, *w_halo] + ([outer] if bare else [])
    outs = [field, field] + [edge] * 4
    body = functools.partial(dw_kernel, bare)
    return stencil_call(body, [VMEM] * len(args), args, outs, [VMEM] * 6, work_space(*d.shape[:2]) * 2)


def last_d_call(step, d, d_prev, halo, speed, perturb, lap_u, cells, early):
    before = 0 if early is None else early.shape[0]
    n = cells.shape[1]
    fields = step + 1 - before
    args = [d, d_prev, *halo, speed, perturb, lap_u, cells, cells] + ([early] if before else [])
    specs = [VMEM] * len(args)
    specs[7] = HBM
    scratch = work_space(*d.shape[:2]) + [
        pltpu.SMEM(cells.shape, jnp.int32),
        pltpu.VMEM((fields, n, d.shape[-1]), F32),
        pltpu.SemaphoreType.DMA((PARTS,)),
        pltpu.SemaphoreType.DMA(()),
    ]
    outs = [sds((1,) + d.shape), sds(d.shape), sds((step + 1, n))]
    body = functools.partial(last_d_kernel, before)
    return stencil_call(body, specs, args, outs, [HBM, VMEM, VMEM], scratch)


def last_w_call(w, w_prev, halo, speed, count, d_next, table, blocks, lat_dev):
    _, depth, cells = blocks[0].shape
    args = [w, w_prev, *halo, speed, count, d_next, table, *blocks]
    specs = [VMEM] * len(args)
    specs[7] = HBM
    scratch = [pltpu.VMEM(w.shape, F32)] + work_space(*w.shape[:2]) + [
        pltpu.SMEM(table.shape, jnp.int32),
        pltpu.SemaphoreType.DMA((PARTS,)),
        pltpu.SemaphoreType.DMA(()),
    ]
    outs = [sds((1,) + w.shape), sds((lat_dev, depth, cells))]
    body = functools.partial(last_w_kernel, False)
    return stencil_call(body, specs, args, outs, [HBM, VMEM], scratch)


def count_kernel(cells_ref, count_ref, outer_ref):
    depth, side, _ = count_ref.shape
    local = cells_ref[...] - (lax.axis_index("slab") * depth - HALO) * (side * side)
    n = local.shape[1]
    row_of = jnp.where(local >= 0, quotient(jnp.maximum(local, 0), side), -1)
    lane_of = remainder(jnp.maximum(local, 0), side)
    lanes = lax.broadcasted_iota(jnp.int32, (side, n), 0)
    lane_hot = jnp.where(lanes == lane_of, 1.0, 0.0).astype(jnp.bfloat16)
    for z in range(depth + 2 * HALO):
        row_hot = jnp.where(lanes + z * side == row_of, 1.0, 0.0).astype(jnp.bfloat16)
        plane = lax.dot_general(row_hot, lane_hot, (((1,), (1,)), ((), ())), preferred_element_type=F32)
        if z < HALO:
            outer_ref[0, z] = plane
        elif z < HALO + depth:
            count_ref[z - HALO] = plane
        else:
            outer_ref[1, z - HALO - depth] = plane


def count_call(cells, depth, side):
    return pl.pallas_call(
        count_kernel,
        out_shape=[sds((depth, side, side)), sds((2, HALO, side, side))],
        in_specs=[VMEM],
        out_specs=[VMEM, VMEM],
        compiler_params=params(8),
        name="count",
    )(cells)


def gather_records(before, cells_smem, cells_ref, fields, out_ref, rows_ref):
    depth, side, _ = fields[0].shape
    n = cells_ref.shape[1]
    total = depth * side * side
    start = lax.axis_index("slab") * total
    local = cells_ref[...] - start
    mine = (local >= 0) & (local < total)
    lane_of = jnp.where(mine, remainder(jnp.maximum(local, 0), side), -1)
    lanes = lax.broadcasted_iota(jnp.int32, (side, n), 0)
    hit = lanes == lane_of
    flat = [field_ref.reshape(depth * side, side) for field_ref in fields]

    def gather(r, carry):
        cell = jnp.clip(cells_smem[0, r] - start, 0, total - 1)
        row = quotient(cell, side)
        for step, field_ref in enumerate(flat):
            rows_ref[step, pl.ds(r, 1), :] = field_ref[pl.ds(row, 1), :]
        return carry

    lax.fori_loop(0, n, gather, 0, unroll=32)
    for step in range(len(fields)):
        turned = rows_ref[step].T
        out_ref[pl.ds(before + step, 1), :] = jnp.sum(jnp.where(hit, turned, 0.0), axis=0, keepdims=True)


def record_kernel(before, cells_smem, cells_ref, *rest):
    if before:
        early_ref, rest = rest[0], rest[1:]
    *fields, out_ref, rows_ref = rest
    if before:
        out_ref[pl.ds(0, before), :] = early_ref[...]
    gather_records(before, cells_smem, cells_ref, fields, out_ref, rows_ref)


def record_call(cells, early, fields):
    side = fields[0].shape[-1]
    n = cells.shape[1]
    before = 0 if early is None else early.shape[0]
    args = [cells, cells] + ([early] if before else []) + list(fields)
    return pl.pallas_call(
        functools.partial(record_kernel, before),
        out_shape=sds((before + len(fields), n)),
        in_specs=[SMEM] + [VMEM] * (len(args) - 1),
        out_specs=VMEM,
        scratch_shapes=[pltpu.VMEM((len(fields), n, side), F32)],
        compiler_params=params(8),
    )(*args)


def total_kernel(*refs):
    *parts, out_ref = refs
    total = parts[0][...]
    for part in parts[1:]:
        total = total + part[...]
    for step in range(total.shape[0]):
        out_ref[step] = total[step : step + 1]


def total_call(parts):
    steps, n = parts[0].shape
    return pl.pallas_call(
        total_kernel,
        out_shape=sds((steps, 1, n)),
        in_specs=[VMEM] * len(parts),
        out_specs=VMEM,
        compiler_params=params(4),
        name="total",
    )(*parts)


def swap_segments(parts, segment):
    count = len(parts)
    lanes = count * segment
    lane = lax.broadcasted_iota(jnp.int32, parts[0].shape, 1)
    parts = list(parts)
    bit = count // 2
    while bit:
        low = lax.rem(lax.div(lane, bit * segment), 2) == 0
        for a in range(count):
            if not a & bit:
                first, second = parts[a], parts[a + bit]
                parts[a] = jnp.where(low, first, pltpu.roll(second, bit * segment, 1))
                parts[a + bit] = jnp.where(low, pltpu.roll(first, lanes - bit * segment, 1), second)
        bit //= 2
    return parts


def partner_of(me, k, count):
    if count & (count - 1) == 0:
        return lax.bitwise_xor(me, k)
    return lax.rem(k - me + count, count)


def round_of(me, other, count):
    if count & (count - 1) == 0:
        return lax.bitwise_xor(me, other)
    return lax.rem(me + other, count)


def pack_kernel(aperture_hbm, slot_hbm, tiles_hbm, *rest):
    *outs, table_ref, aperture_ref, slot_ref, tiles_ref, sems = rest
    pairs = ((aperture_hbm, aperture_ref), (slot_hbm, slot_ref), (tiles_hbm, tiles_ref))
    copies = [pltpu.make_async_copy(a, b, sems.at[i]) for i, (a, b) in enumerate(pairs)]
    for copy in copies:
        copy.start()
    lat_dev = tiles_ref.shape[0]
    n_shot = len(outs)
    capacity = outs[0].shape[0]
    me = lax.axis_index("shot")
    n_tiles = aperture_ref.shape[1]
    copies[0].wait()
    copies[1].wait()

    def shot(s, carry):
        for r in range(capacity):
            table_ref[s * (capacity + 1) + r] = 0
        seen = jnp.int32(0)
        for p in range(n_tiles):
            slot = slot_ref[aperture_ref[s, p]]
            mine = quotient(slot, lat_dev) == me

            @pl.when(mine)
            def _():
                table_ref[s * (capacity + 1) + seen] = remainder(slot, lat_dev)

            seen = seen + mine.astype(jnp.int32)
        table_ref[s * (capacity + 1) + capacity] = seen
        return carry

    lax.fori_loop(0, n_shot, shot, 0)
    copies[2].wait()
    for k in range(n_shot):
        base = partner_of(me, k, n_shot) * (capacity + 1)
        for r in range(capacity):
            outs[k][r] = tiles_ref[table_ref[base + r]]


def pack_call(aperture, tile_slot, model_tiles, capacity):
    n_shot = aperture.shape[0]
    _, depth, cells = model_tiles.shape
    *blocks, table = pl.pallas_call(
        pack_kernel,
        out_shape=[sds((capacity, depth, cells))] * n_shot + [sds((n_shot * (capacity + 1),), jnp.int32)],
        in_specs=[HBM, HBM, HBM],
        out_specs=[VMEM] * n_shot + [SMEM],
        scratch_shapes=[
            pltpu.SMEM(aperture.shape, jnp.int32),
            pltpu.SMEM(tile_slot.shape, jnp.int32),
            pltpu.VMEM(model_tiles.shape, F32),
            pltpu.SemaphoreType.DMA((3,)),
        ],
        compiler_params=params(8),
        name="pack",
    )(aperture, tile_slot, model_tiles)
    return blocks, table


def places(aperture_ref, slot_ref, lat_dev, n_shot, capacity, seen_ref, place_ref):
    me = lax.axis_index("shot")
    for h in range(n_shot):
        seen_ref[h] = 0

    def tile(p, carry):
        holder = quotient(slot_ref[aperture_ref[me, p]], lat_dev)
        rank = seen_ref[holder]
        seen_ref[holder] = rank + 1
        place_ref[p] = round_of(me, holder, n_shot) * capacity + rank
        return carry

    lax.fori_loop(0, aperture_ref.shape[1], tile, 0)


def perturb_kernel(lat_dev, tile_side, aperture_ref, slot_ref, *rest):
    *blocks, out_ref, tiles_ref, seen_ref, place_ref = rest
    n_shot = len(blocks)
    capacity, depth, cells = blocks[0].shape
    side = out_ref.shape[1]
    across = side // tile_side
    flat_ref = out_ref.reshape(depth * side, side)
    places(aperture_ref, slot_ref, lat_dev, n_shot, capacity, seen_ref, place_ref)
    for k in range(n_shot):
        tiles_ref[pl.ds(k * capacity, capacity)] = blocks[k][...]

    def tile_row(i, carry):
        for high in range(cells // side):
            parts = [tiles_ref[place_ref[i * across + j], :, pl.ds(high * side, side)] for j in range(across)]
            for low, part in enumerate(swap_segments(parts, tile_side)):
                flat_ref[pl.ds(i * tile_side + high * across + low, depth, stride=side), :] = part
        return carry

    lax.fori_loop(0, across, tile_row, 0)


def pack_back(lat_dev, tile_side, aperture_ref, slot_ref, corr_ref, blocks, tiles_ref, seen_ref, place_ref):
    n_shot = len(blocks)
    capacity, depth, cells = blocks[0].shape
    side = corr_ref.shape[1]
    across = side // tile_side
    flat_ref = corr_ref.reshape(depth * side, side)
    places(aperture_ref, slot_ref, lat_dev, n_shot, capacity, seen_ref, place_ref)
    tiles_ref[...] = jnp.zeros(tiles_ref.shape, F32)

    def tile_row(i, carry):
        for high in range(cells // side):
            parts = [
                flat_ref[pl.ds(i * tile_side + high * across + low, depth, stride=side), :] for low in range(across)
            ]
            for j, part in enumerate(swap_segments(parts, tile_side)):
                tiles_ref[place_ref[i * across + j], :, pl.ds(high * side, side)] = part
        return carry

    lax.fori_loop(0, across, tile_row, 0)
    for k in range(n_shot):
        blocks[k][...] = tiles_ref[pl.ds(k * capacity, capacity)]


def tile_scratch(n_shot, capacity, depth, cells, n_tiles):
    return [
        pltpu.VMEM((n_shot * capacity, depth, cells), F32),
        pltpu.SMEM((n_shot,), jnp.int32),
        pltpu.SMEM((n_tiles,), jnp.int32),
    ]


def perturb_call(aperture, tile_slot, blocks, side, lat_dev, tile_side):
    capacity, depth, cells = blocks[0].shape
    return pl.pallas_call(
        functools.partial(perturb_kernel, lat_dev, tile_side),
        out_shape=sds((depth, side, side)),
        in_specs=[SMEM, SMEM] + [VMEM] * len(blocks),
        out_specs=VMEM,
        scratch_shapes=tile_scratch(len(blocks), capacity, depth, cells, aperture.shape[1]),
        compiler_params=params(8),
        name="perturb",
    )(aperture, tile_slot, *blocks)


def sum_tiles(table_ref, blocks, out_ref):
    n_shot = len(blocks)
    capacity = blocks[0].shape[0]
    out_ref[...] = jnp.zeros(out_ref.shape, F32)
    for k in range(n_shot):
        base = partner_of(lax.axis_index("shot"), k, n_shot) * (capacity + 1)
        for r in range(capacity):

            @pl.when(r < table_ref[base + capacity])
            def _():
                slot = table_ref[base + r]
                out_ref[slot] = out_ref[slot] + blocks[k][r]


def swap(edges):
    count = lax.axis_size("slab")
    shots = lax.axis_size("shot")
    got = []
    for start, edge in enumerate(edges):
        pairs = {}
        for shot in range(shots):
            for i in range(count):
                other = i + 1 if (i - start) % 2 == 0 else i - 1
                if 0 <= other < count:
                    pairs[shot * count + i] = shot * count + other
                elif shots % 2 == 0:
                    pairs[shot * count + i] = (shot ^ 1) * count + i
        got.append(lax.ppermute(edge, ("shot", "slab"), sorted(pairs.items())))
    return tuple(got)


def edges_kernel(groups, *refs):
    refs = Refs(refs)
    fields = [refs.take(n) for n in groups]
    for group in fields:
        depth = group[0].shape[1]
        low = jnp.where(place()[0] == 1, 0, depth - HALO)
        for out_ref, at in zip(refs.take(2), (low, depth - HALO - low)):
            for index, field_ref in enumerate(group):
                for z in range(HALO):
                    out_ref[index, z] = field_ref[0, at + z]


def first_edges(groups):
    outs = []
    for group in groups:
        outs += [sds((len(group), HALO) + group[0].shape[2:])] * 2
    fields = [field for group in groups for field in group]
    edges = pl.pallas_call(
        functools.partial(edges_kernel, [len(group) for group in groups]),
        out_shape=outs,
        in_specs=[VMEM] * len(fields),
        out_specs=[VMEM] * len(outs),
        compiler_params=params(8),
        name="edges",
    )(*fields)
    return [edges[2 * i : 2 * i + 2] for i in range(len(groups))]


def partners():
    count = lax.axis_size("shot")
    if count & (count - 1) == 0:
        return [[s ^ k for s in range(count)] for k in range(count)]
    return [[(k - s) % count for s in range(count)] for k in range(count)]


def rounds(count):
    return sorted(range(count), key=lambda k: (-(k >> 1).bit_count(), k))


def exchange(blocks):
    got = [None] * len(blocks)
    for k in rounds(len(blocks)):
        block, to = blocks[k], partners()[k]
        moves = [(s, t) for s, t in enumerate(to) if s != t]
        kept = [s for s, t in enumerate(to) if s == t]
        if kept and moves:
            moves = moves + [(s, s) for s in kept]
        got[k] = lax.ppermute(block, "shot", moves) if moves else block
    return got


def slab_sum(part):
    count = lax.axis_size("slab")
    parts = [part]
    for k in range(1, count):
        to = [s ^ k for s in range(count)] if count & (count - 1) == 0 else [(s + k) % count for s in range(count)]
        parts.append(lax.ppermute(part, "slab", list(enumerate(to))))
    return total_call(parts)


def per_device(
    model_tiles,
    background,
    u_prev,
    u_now,
    du_prev,
    du_now,
    w_prev,
    w_now,
    wavelet,
    source_cell,
    receiver_cells,
    aperture,
    tile_slot,
):
    lat_dev, depth, tile_cells = model_tiles.shape
    side = background.shape[-1]
    tile_side = math.isqrt(tile_cells)
    capacity = aperture.shape[1] // 4
    steps = wavelet.shape[1]
    speed = background[0]
    u, d, w = u_now[0], du_now[0], w_now[0]
    up, dp, wp = u_prev[0], du_prev[0], w_prev[0]

    tiling = (aperture, tile_slot, lat_dev, tile_side)
    u_edges, dw_edges = first_edges([[u_now], [du_now, w_now]])
    u_halo = swap(u_edges)
    dw_halo = swap(dw_edges)
    outgoing, table = pack_call(aperture, tile_slot, model_tiles, capacity)
    incoming = exchange(outgoing)
    count, outer = count_call(receiver_cells, depth, side)
    perturb = perturb_call(aperture, tile_slot, incoming, side, lat_dev, tile_side)

    u_next, lap, corr, *edges = u_call(0, False, wavelet, source_cell, u, up, u_halo, speed, w, None, *tiling)
    u_halo = swap(edges)
    bare, *edges = w_bare_call(w, wp, dw_halo, 1, speed)
    w_halo = swap(edges)
    d_next, w_next, *edges = d_call(d, dp, dw_halo, 0, speed, perturb, lap, bare, count)
    d_halo = swap(edges)
    traces = None
    for step in range(1, steps - 1):
        traces = record_call(receiver_cells, traces, [d_next])
        u, up, d, dp, w, wp = u_next, u, d_next, d, w_next, w
        u_next, lap, corr, *edges = u_call(step, False, wavelet, source_cell, u, up, u_halo, speed, w, corr, *tiling)
        u_halo = swap(edges)
        d_next, w_next, *edges = dw_call(
            d, dp, w, wp, d_halo, w_halo, speed, perturb, lap, count, outer if step == 1 else None
        )
        d_halo = swap(edges[:2])
        w_halo = swap(edges[2:])
    u, up, d, dp, w, wp = u_next, u, d_next, d, w_next, w
    step = steps - 1
    u_final, lap, *returning = u_call(step, True, wavelet, source_cell, u, up, u_halo, speed, w, corr, *tiling)
    arrived = exchange(returning)
    d_final, d_next, traces = last_d_call(step, d, dp, d_halo, speed, perturb, lap, receiver_cells, traces)
    traces = slab_sum(traces)
    w_final, sensitivity = last_w_call(w, wp, w_halo, speed, count, d_next, table, arrived, lat_dev)
    return (sensitivity, u_final, d_final, w_final, jnp.transpose(traces, (1, 0, 2)))


def solution(mesh):
    field = P("shot", "slab", None, None)
    tiles = P("shot", "slab", None)
    in_specs = (tiles,) + (field,) * 7 + (P("shot", None), P("shot"), P("shot", None), P(), P())
    out_specs = (tiles, field, field, field, P("shot", None, None))


    return jax.shard_map(per_device, mesh=mesh, in_specs=in_specs, out_specs=out_specs, check_vma=False)
```

```python
import functools
import math

import jax
import jax.numpy as jnp
from jax import lax
from jax.experimental import pallas as pl
from jax.experimental.pallas import tpu as pltpu
from jax.sharding import PartitionSpec as P


COEFFS = (-205.0 / 72.0, 8.0 / 5.0, -1.0 / 5.0, 8.0 / 315.0, -1.0 / 560.0)
HALO = len(COEFFS) - 1
SUB = 8
F32 = jnp.float32
VMEM = pl.BlockSpec(memory_space=pltpu.VMEM)
SMEM = pl.BlockSpec(memory_space=pltpu.SMEM)
HBM = pl.BlockSpec(memory_space=pltpu.HBM)


def params(mib):
    return pltpu.CompilerParams(vmem_limit_bytes=mib * 1024 * 1024)


def in_hbm(x):
    return pltpu.with_memory_space_constraint(x, pltpu.HBM)


def sds(shape, dtype=F32):
    return jax.ShapeDtypeStruct(shape, dtype)


def place():
    slab, count = lax.axis_index("slab"), lax.axis_size("slab")
    odd = lax.bitwise_and(slab, 1)
    above, below = slab < count - 1, slab > 0
    is_odd = odd == 1
    return odd, (is_odd & below) | (~is_odd & above), (is_odd & above) | (~is_odd & below)


def quotient(x, m):
    return lax.shift_right_logical(x, m.bit_length() - 1) if m & (m - 1) == 0 else lax.div(x, m)


def remainder(x, m):
    return lax.bitwise_and(x, m - 1) if m & (m - 1) == 0 else lax.rem(x, m)


SCALE = 5040.0
PARTS = 4


def band_weights(side):
    i = lax.broadcasted_iota(jnp.int32, (2 * side, 2 * side), 0)
    j = lax.broadcasted_iota(jnp.int32, (2 * side, 2 * side), 1)
    far = jnp.where((i < side) == (j < side), jnp.abs(i - j), 0)
    out = jnp.zeros((2 * side, 2 * side), F32)
    for k in range(1, HALO + 1):
        out = jnp.where(far == k, round(COEFFS[k] * SCALE) * 1.0, out)
    out = out.astype(jnp.bfloat16)
    return jnp.concatenate([out, out, out], axis=0)


def split3(x):
    high = x.astype(jnp.bfloat16)
    rest = x - high.astype(F32)
    mid = rest.astype(jnp.bfloat16)
    low = (rest - mid.astype(F32)).astype(jnp.bfloat16)
    return high, mid, low


def prepare_local(rows_ref, lanes_ref, now_ref, weights):
    depth, side, _ = now_ref.shape
    zeros = jnp.zeros((SUB, side), F32)
    half = depth // 2
    parts = []
    for low, high in zip(split3(now_ref[pl.ds(0, half)]), split3(now_ref[pl.ds(half, half)])):
        parts += [low.reshape(half * side, side), high.reshape(half * side, side)]
    lanes = jnp.dot(jnp.concatenate(parts, axis=1), weights, preferred_element_type=F32)
    lanes_ref[pl.ds(0, half)] = lanes[:, :side].reshape(half, side, side)
    lanes_ref[pl.ds(half, half)] = lanes[:, side:].reshape(half, side, side)
    for z in range(depth):
        rows_ref[z, pl.ds(0, SUB), :] = zeros
        rows_ref[z, pl.ds(SUB + side, SUB), :] = zeros
        rows_ref[z, pl.ds(SUB, side), :] = now_ref[z]


def prepare_halo(halo_ref, first_ref, second_ref, index, inject=None):
    odd, has_first, has_second = place()

    def halo(z, carry):
        halo_ref[1 - odd, z] = jnp.where(has_first, first_ref[index, z], 0.0)
        halo_ref[odd, z] = jnp.where(has_second, second_ref[index, z], 0.0)
        return carry

    lax.fori_loop(0, HALO, halo, 0)
    if inject:
        outer_ref, other_ref = inject
        for end in range(2):
            for z in range(HALO):
                halo_ref[end, z] = halo_ref[end, z] + outer_ref[end, z] * other_ref[end, z]


def prepare(work, now_ref, first_ref, second_ref, index, weights):
    rows_ref, halo_ref, lanes_ref = work
    prepare_local(rows_ref, lanes_ref, now_ref, weights)
    prepare_halo(halo_ref, first_ref, second_ref, index)


def each_laplacian(work, now_ref, emit, finish=None, parts=1):
    rows_ref, halo_ref, lanes_ref = work
    depth, side, _ = now_ref.shape

    def block(g, carry):
        start = pl.multiple_of(g * SUB, SUB)
        rows = pl.ds(start, SUB)
        column = [halo_ref[0, z, rows, :] for z in range(HALO)]
        column += [now_ref[z, rows, :] for z in range(depth)]
        column += [halo_ref[1, z, rows, :] for z in range(HALO)]
        for z in range(depth):
            centre = column[HALO + z]
            total = (3.0 * COEFFS[0]) * centre + (1.0 / SCALE) * lanes_ref[z, rows, :]
            for k in range(1, HALO + 1):
                ring = (column[HALO + z + k] + column[HALO + z - k]) + (
                    rows_ref[z, pl.ds(start + (SUB + k), SUB), :] + rows_ref[z, pl.ds(start + (SUB - k), SUB), :]
                )
                total = total + COEFFS[k] * ring
            emit(z, rows, centre, total)
        return carry

    blocks = side // SUB // parts
    for part in range(parts):
        lax.fori_loop(part * blocks, (part + 1) * blocks, block, 0)
        if finish:
            finish(part, parts)


def halo_space(side):
    return pltpu.VMEM((2, HALO, side, side), F32)


def work_space(depth, side):
    return [
        pltpu.VMEM((depth, side + 2 * SUB, side), F32),
        halo_space(side),
        pltpu.VMEM((depth, side, side), F32),
    ]


def ahead_kernel(n, *refs):
    weights = band_weights(refs[0].shape[-1])
    for i in range(n):
        prepare_local(refs[n + 2 * i], refs[n + 2 * i + 1], refs[i], weights)


def ahead_call(fields):
    depth, side, _ = fields[0].shape
    outs = [sds((depth, side + 2 * SUB, side)), sds((depth, side, side))] * len(fields)
    res = pl.pallas_call(
        functools.partial(ahead_kernel, len(fields)),
        out_shape=outs,
        in_specs=[VMEM] * len(fields),
        out_specs=[VMEM] * len(outs),
        compiler_params=params(16),
    )(*fields)
    return [res[2 * i : 2 * i + 2] for i in range(len(fields))]


def copy_sends(next_ref, first_ref, second_ref, index):
    depth = next_ref.shape[0]
    odd = place()[0] == 1
    first = jnp.where(odd, 0, depth - HALO)
    second = jnp.where(odd, depth - HALO, 0)
    for z in range(HALO):
        first_ref[index, z] = next_ref[first + z]
        second_ref[index, z] = next_ref[second + z]


def store_out(next_ref, out_ref, sems, step, steps):
    rows = pl.ds(step * (next_ref.shape[1] // steps), next_ref.shape[1] // steps)
    return pltpu.make_async_copy(next_ref.at[:, rows], out_ref.at[0, :, rows], sems.at[step])


class Refs:
    def __init__(self, refs):
        self.refs = list(refs)

    def take(self, n=None):
        if n is None:
            return self.refs.pop(0)
        return [self.refs.pop(0) for _ in range(n)]


def u_kernel(step, last, ahead, tiles, *refs):
    refs = Refs(refs)
    source_ref, wavelet_hbm, now_ref, prev_ref, ha_ref, hb_ref, speed_ref, w_in = refs.take(8)
    corr_in = refs.take() if step else None
    local_work = refs.take(2) if ahead else None
    tables = refs.take(2) if last else []
    if last:
        out_ref, lap_ref = refs.take(2)
        blocks = refs.take(tiles[0])
        sends = []
        next_ref, corr_ref = refs.take(2)
    else:
        next_ref, lap_ref, corr_ref = refs.take(3)
        sends = refs.take(2)
    halo_ref = refs.take()
    if not ahead:
        local_work = refs.take(2)
    wavelet_ref, own_sems = refs.take(2)
    copies = [pltpu.make_async_copy(wavelet_hbm, wavelet_ref, own_sems.at[0])]
    w_ref = w_in
    if not step:
        w_ref = refs.take()
        half = w_ref.shape[0] // 2
        for i in range(2):
            part = pl.ds(i * half, half)
            copies.append(pltpu.make_async_copy(w_in.at[0, part], w_ref.at[part], own_sems.at[1 + i]))
    if last:
        fetched = refs.take(2)
        tiles_ref, seen_ref, place_ref, sems = refs.take(4)
        for i, (a, b) in enumerate(zip(tables, fetched)):
            copies.append(pltpu.make_async_copy(a, b, own_sems.at[1 + i]))
    for copy in copies:
        copy.start()
    depth, side, _ = now_ref.shape
    work = (local_work[0], halo_ref, local_work[1])
    if not ahead:
        prepare_local(*local_work, now_ref, band_weights(side))
    prepare_halo(halo_ref, ha_ref, hb_ref, 0)
    for copy in copies:
        copy.wait()

    def emit(z, block, centre, lap):
        lap_ref[z, block, :] = lap
        part = lap * w_ref[z, block, :]
        corr_ref[z, block, :] = corr_in[z, block, :] + part if step else part
        next_ref[z, block, :] = (2.0 * centre - prev_ref[z, block, :]) + speed_ref[z, block, :] * lap

    local = source_ref[0] - lax.axis_index("slab") * (depth * side * side)
    mine = (local >= 0) & (local < depth * side * side)
    cell = jnp.where(mine, local, 0)
    z = quotient(cell, side * side)
    x = remainder(quotient(cell, side), side)
    lane = lax.broadcasted_iota(jnp.int32, (1, side), 1)
    add = jnp.where((lane == remainder(cell, side)) & mine, wavelet_ref[0, step], 0.0)

    def finish(part, parts):
        size = side // parts

        @pl.when((x >= part * size) & (x < (part + 1) * size))
        def _():
            next_ref[z, pl.ds(x, 1), :] = next_ref[z, pl.ds(x, 1), :] + add

        if last:
            store_out(next_ref, out_ref, sems, part, parts).start()

    parts = PARTS if last else 1
    each_laplacian(work, now_ref, emit, finish, parts)
    if sends:
        copy_sends(next_ref, *sends, 0)
    if last:
        pack_back(*tiles[1:], *fetched, corr_ref, blocks, tiles_ref, seen_ref, place_ref)
        for part in range(parts):
            store_out(next_ref, out_ref, sems, part, parts).wait()


def w_bare_kernel(index, now_ref, prev_ref, ha_ref, hb_ref, speed_ref, next_ref, *rest):
    sends, work = rest[:2], rest[2:]
    _, side, _ = now_ref.shape
    prepare(work, now_ref, ha_ref, hb_ref, index, band_weights(side))

    def emit(z, block, centre, lap):
        next_ref[z, block, :] = (2.0 * centre - prev_ref[z, block, :]) + speed_ref[z, block, :] * lap

    each_laplacian(work, now_ref, emit)
    copy_sends(next_ref, *sends, 0)


def d_kernel(index, now_ref, prev_ref, ha_ref, hb_ref, speed_ref, perturb_ref, lap_u_ref, bare_ref, count_ref, *rest):
    next_ref, w_ref, *sends = rest[:4]
    work = rest[4:]
    _, side, _ = now_ref.shape
    prepare(work, now_ref, ha_ref, hb_ref, index, band_weights(side))

    def emit(z, block, centre, lap):
        new = ((2.0 * centre - prev_ref[z, block, :]) + speed_ref[z, block, :] * lap) + (
            perturb_ref[z, block, :] * lap_u_ref[z, block, :]
        )
        next_ref[z, block, :] = new
        w_ref[z, block, :] = bare_ref[z, block, :] + count_ref[z, block, :] * new

    each_laplacian(work, now_ref, emit)
    copy_sends(next_ref, *sends, 0)


def dw_kernel(bare, *refs):
    refs = Refs(refs)
    speed_ref, d_ref, d_prev, w_ref, w_prev, perturb_ref, lap_u_ref, count_ref = refs.take(8)
    d_halo, w_halo = refs.take(2), refs.take(2)
    d_local, w_local = refs.take(2), refs.take(2)
    outer_ref = refs.take() if bare else None
    d_next, w_next = refs.take(2)
    d_sends, w_sends = refs.take(2), refs.take(2)
    d_halos, w_halos = refs.take(2)
    prepare_halo(d_halos, *d_halo, 0)
    prepare_halo(w_halos, *w_halo, 0, (outer_ref, d_halos) if bare else None)
    d_work, w_work = (d_local[0], d_halos, d_local[1]), (w_local[0], w_halos, w_local[1])

    def emit_d(z, block, centre, lap):
        d_next[z, block, :] = ((2.0 * centre - d_prev[z, block, :]) + speed_ref[z, block, :] * lap) + (
            perturb_ref[z, block, :] * lap_u_ref[z, block, :]
        )

    def emit_w(z, block, centre, lap):
        w_next[z, block, :] = ((2.0 * centre - w_prev[z, block, :]) + speed_ref[z, block, :] * lap) + (
            count_ref[z, block, :] * d_next[z, block, :]
        )

    each_laplacian(d_work, d_ref, emit_d)
    copy_sends(d_next, *d_sends, 0)
    each_laplacian(w_work, w_ref, emit_w)
    copy_sends(w_next, *w_sends, 0)


def last_d_kernel(before, *refs):
    refs = Refs(refs)
    now_ref, prev_ref, ha_ref, hb_ref, speed_ref, perturb_ref, lap_u_ref, cells_hbm, cells_ref = refs.take(9)
    early_ref = refs.take() if before else None
    out_ref, next_ref, record_ref = refs.take(3)
    work = refs.take(3)
    cells_smem, rows_ref, sems, table_sem = refs.take(4)
    fetch = pltpu.make_async_copy(cells_hbm, cells_smem, table_sem)
    fetch.start()
    _, side, _ = now_ref.shape
    prepare(work, now_ref, ha_ref, hb_ref, 0, band_weights(side))

    def emit(z, block, centre, lap):
        next_ref[z, block, :] = ((2.0 * centre - prev_ref[z, block, :]) + speed_ref[z, block, :] * lap) + (
            perturb_ref[z, block, :] * lap_u_ref[z, block, :]
        )

    def finish(part, parts):
        store_out(next_ref, out_ref, sems, part, parts).start()

    each_laplacian(work, now_ref, emit, finish, PARTS)
    fetch.wait()
    if before:
        record_ref[pl.ds(0, before), :] = early_ref[...]
    fields = [now_ref, next_ref] if record_ref.shape[0] > before + 1 else [next_ref]
    gather_records(before, cells_smem, cells_ref, fields, record_ref, rows_ref)
    for part in range(PARTS):
        store_out(next_ref, out_ref, sems, part, PARTS).wait()


def last_w_kernel(*refs):
    refs = Refs(refs)
    now_ref, prev_ref, ha_ref, hb_ref, speed_ref, count_ref, d_next = refs.take(7)
    out_ref, next_ref = refs.take(2)
    work = refs.take(3)
    sems = refs.take()
    _, side, _ = now_ref.shape
    prepare(work, now_ref, ha_ref, hb_ref, 0, band_weights(side))

    def emit(z, block, centre, lap):
        next_ref[z, block, :] = ((2.0 * centre - prev_ref[z, block, :]) + speed_ref[z, block, :] * lap) + (
            count_ref[z, block, :] * d_next[z, block, :]
        )

    def finish(part, parts):
        store_out(next_ref, out_ref, sems, part, parts).start()

    each_laplacian(work, now_ref, emit, finish, PARTS)
    for part in range(PARTS):
        store_out(next_ref, out_ref, sems, part, PARTS).wait()


def stencil_call(body, in_specs, args, outs, kinds, scratch):
    return pl.pallas_call(
        body, out_shape=outs, in_specs=in_specs, out_specs=kinds, scratch_shapes=scratch, compiler_params=params(20)
    )(*args)


def u_call(step, last, wavelet, source, u, u_prev, halo, speed, w, corr, local, aperture, tile_slot, lat_dev, tile_side):
    field = sds(u.shape)
    edge = sds((1, HALO) + u.shape[1:])
    args = [source, in_hbm(wavelet), u, u_prev, *halo, speed, w] + ([corr] if step else [])
    specs = [SMEM, HBM] + [VMEM] * (len(args) - 2)
    if not step:
        args[7], specs[7] = in_hbm(w), HBM
    ahead = local is not None
    if ahead:
        args, specs = args + list(local), specs + [VMEM] * 2
    n_shot, n_tiles = aperture.shape
    cells = tile_side * tile_side
    capacity = n_tiles // 4
    rows, halos, lanes = work_space(*u.shape[:2])
    scratch = [halos] + ([] if ahead else [rows, lanes])
    scratch += [pltpu.SMEM(wavelet.shape, F32), pltpu.SemaphoreType.DMA((3,))]
    if not step:
        scratch += [pltpu.VMEM(u.shape, F32)]
    if last:
        args += [in_hbm(aperture), in_hbm(tile_slot)]
        specs += [HBM, HBM]
        outs = [sds((1,) + u.shape), field] + [sds((capacity, u.shape[0], cells))] * n_shot
        kinds = [HBM] + [VMEM] * (1 + n_shot)
        scratch = [pltpu.VMEM(u.shape, F32)] * 2 + scratch + [
            pltpu.SMEM(aperture.shape, jnp.int32),
            pltpu.SMEM(tile_slot.shape, jnp.int32),
            *tile_scratch(n_shot, capacity, u.shape[0], cells, n_tiles),
            pltpu.SemaphoreType.DMA((PARTS,)),
        ]
    else:
        outs, kinds = [field] * 3 + [edge] * 2, [VMEM] * 5
    body = functools.partial(u_kernel, step, last, ahead, (n_shot, lat_dev, tile_side))
    return stencil_call(body, specs, args, outs, kinds, scratch)


def w_bare_call(w, w_prev, halo, index, speed):
    field, edge = sds(w.shape), sds((1, HALO) + w.shape[1:])
    args = [w, w_prev, *halo, speed]
    body = functools.partial(w_bare_kernel, index)
    return stencil_call(body, [VMEM] * 5, args, [field, edge, edge], [VMEM] * 3, work_space(*w.shape[:2]))


def d_call(d, d_prev, halo, index, speed, perturb, lap_u, bare, count):
    field, edge = sds(d.shape), sds((1, HALO) + d.shape[1:])
    args = [d, d_prev, *halo, speed, perturb, lap_u, bare, count]
    body = functools.partial(d_kernel, index)
    outs = [field, field, edge, edge]
    return stencil_call(body, [VMEM] * 9, args, outs, [VMEM] * 4, work_space(*d.shape[:2]))


def dw_call(d, d_prev, w, w_prev, d_halo, w_halo, d_local, w_local, speed, perturb, lap_u, count, outer):
    field, edge = sds(d.shape), sds((1, HALO) + d.shape[1:])
    bare = outer is not None
    args = [speed, d, d_prev, w, w_prev, perturb, lap_u, count, *d_halo, *w_halo, *d_local, *w_local]
    args += [outer] if bare else []
    outs = [field, field] + [edge] * 4
    body = functools.partial(dw_kernel, bare)
    return stencil_call(body, [VMEM] * len(args), args, outs, [VMEM] * 6, [halo_space(d.shape[1])] * 2)


def last_d_call(step, d, d_prev, halo, speed, perturb, lap_u, cells, early):
    before = 0 if early is None else early.shape[0]
    n = cells.shape[1]
    fields = step + 1 - before
    args = [d, d_prev, *halo, speed, perturb, lap_u, cells, cells] + ([early] if before else [])
    specs = [VMEM] * len(args)
    specs[7] = HBM
    scratch = work_space(*d.shape[:2]) + [
        pltpu.SMEM(cells.shape, jnp.int32),
        pltpu.VMEM((fields, n, d.shape[-1]), F32),
        pltpu.SemaphoreType.DMA((PARTS,)),
        pltpu.SemaphoreType.DMA(()),
    ]
    outs = [sds((1,) + d.shape), sds(d.shape), sds((step + 1, n))]
    body = functools.partial(last_d_kernel, before)
    return stencil_call(body, specs, args, outs, [HBM, VMEM, VMEM], scratch)


def last_w_call(w, w_prev, halo, speed, count, d_next):
    args = [w, w_prev, *halo, speed, count, d_next]
    scratch = [pltpu.VMEM(w.shape, F32)] + work_space(*w.shape[:2]) + [pltpu.SemaphoreType.DMA((PARTS,))]
    return stencil_call(last_w_kernel, [VMEM] * len(args), args, [sds((1,) + w.shape)], [HBM], scratch)


def count_kernel(cells_ref, count_ref, outer_ref):
    depth, side, _ = count_ref.shape
    local = cells_ref[...] - (lax.axis_index("slab") * depth - HALO) * (side * side)
    n = local.shape[1]
    row_of = jnp.where(local >= 0, quotient(jnp.maximum(local, 0), side), -1)
    lane_of = remainder(jnp.maximum(local, 0), side)
    lanes = lax.broadcasted_iota(jnp.int32, (side, n), 0)
    lane_hot = jnp.where(lanes == lane_of, 1.0, 0.0).astype(jnp.bfloat16)
    for z in range(depth + 2 * HALO):
        row_hot = jnp.where(lanes + z * side == row_of, 1.0, 0.0).astype(jnp.bfloat16)
        plane = lax.dot_general(row_hot, lane_hot, (((1,), (1,)), ((), ())), preferred_element_type=F32)
        if z < HALO:
            outer_ref[0, z] = plane
        elif z < HALO + depth:
            count_ref[z - HALO] = plane
        else:
            outer_ref[1, z - HALO - depth] = plane


def count_call(cells, depth, side):
    return pl.pallas_call(
        count_kernel,
        out_shape=[sds((depth, side, side)), sds((2, HALO, side, side))],
        in_specs=[VMEM],
        out_specs=[VMEM, VMEM],
        compiler_params=params(8),
        name="count",
    )(cells)


def gather_records(before, cells_smem, cells_ref, fields, out_ref, rows_ref):
    depth, side, _ = fields[0].shape
    n = cells_ref.shape[1]
    total = depth * side * side
    start = lax.axis_index("slab") * total
    local = cells_ref[...] - start
    mine = (local >= 0) & (local < total)
    lane_of = jnp.where(mine, remainder(jnp.maximum(local, 0), side), -1)
    lanes = lax.broadcasted_iota(jnp.int32, (side, n), 0)
    hit = lanes == lane_of
    flat = [field_ref.reshape(depth * side, side) for field_ref in fields]

    def gather(r, carry):
        cell = jnp.clip(cells_smem[0, r] - start, 0, total - 1)
        row = quotient(cell, side)
        for step, field_ref in enumerate(flat):
            rows_ref[step, pl.ds(r, 1), :] = field_ref[pl.ds(row, 1), :]
        return carry

    lax.fori_loop(0, n, gather, 0, unroll=32)
    for step in range(len(fields)):
        turned = rows_ref[step].T
        out_ref[pl.ds(before + step, 1), :] = jnp.sum(jnp.where(hit, turned, 0.0), axis=0, keepdims=True)


def record_kernel(before, cells_smem, cells_ref, *rest):
    if before:
        early_ref, rest = rest[0], rest[1:]
    *fields, out_ref, rows_ref = rest
    if before:
        out_ref[pl.ds(0, before), :] = early_ref[...]
    gather_records(before, cells_smem, cells_ref, fields, out_ref, rows_ref)


def record_call(cells, early, fields):
    side = fields[0].shape[-1]
    n = cells.shape[1]
    before = 0 if early is None else early.shape[0]
    args = [cells, cells] + ([early] if before else []) + list(fields)
    return pl.pallas_call(
        functools.partial(record_kernel, before),
        out_shape=sds((before + len(fields), n)),
        in_specs=[SMEM] + [VMEM] * (len(args) - 1),
        out_specs=VMEM,
        scratch_shapes=[pltpu.VMEM((len(fields), n, side), F32)],
        compiler_params=params(8),
    )(*args)


def swap_segments(parts, segment):
    count = len(parts)
    lanes = count * segment
    lane = lax.broadcasted_iota(jnp.int32, parts[0].shape, 1)
    parts = list(parts)
    bit = count // 2
    while bit:
        low = lax.rem(lax.div(lane, bit * segment), 2) == 0
        for a in range(count):
            if not a & bit:
                first, second = parts[a], parts[a + bit]
                parts[a] = jnp.where(low, first, pltpu.roll(second, bit * segment, 1))
                parts[a + bit] = jnp.where(low, pltpu.roll(first, lanes - bit * segment, 1), second)
        bit //= 2
    return parts


def partner_of(me, k, count):
    if count & (count - 1) == 0:
        return lax.bitwise_xor(me, k)
    return lax.rem(k - me + count, count)


def round_of(me, other, count):
    if count & (count - 1) == 0:
        return lax.bitwise_xor(me, other)
    return lax.rem(me + other, count)


def pack_kernel(aperture_hbm, slot_hbm, tiles_hbm, *rest):
    *outs, table_ref, aperture_ref, slot_ref, tiles_ref, sems = rest
    pairs = ((aperture_hbm, aperture_ref), (slot_hbm, slot_ref), (tiles_hbm, tiles_ref))
    copies = [pltpu.make_async_copy(a, b, sems.at[i]) for i, (a, b) in enumerate(pairs)]
    for copy in copies:
        copy.start()
    lat_dev = tiles_ref.shape[0]
    n_shot = len(outs)
    capacity = outs[0].shape[0]
    me = lax.axis_index("shot")
    n_tiles = aperture_ref.shape[1]
    copies[0].wait()
    copies[1].wait()

    def shot(s, carry):
        for r in range(capacity):
            table_ref[s * (capacity + 1) + r] = 0
        seen = jnp.int32(0)
        for p in range(n_tiles):
            slot = slot_ref[aperture_ref[s, p]]
            mine = quotient(slot, lat_dev) == me

            @pl.when(mine)
            def _():
                table_ref[s * (capacity + 1) + seen] = remainder(slot, lat_dev)

            seen = seen + mine.astype(jnp.int32)
        table_ref[s * (capacity + 1) + capacity] = seen
        return carry

    lax.fori_loop(0, n_shot, shot, 0)
    copies[2].wait()
    for k in range(n_shot):
        base = partner_of(me, k, n_shot) * (capacity + 1)
        for r in range(capacity):
            outs[k][r] = tiles_ref[table_ref[base + r]]


def pack_call(aperture, tile_slot, model_tiles, capacity):
    n_shot = aperture.shape[0]
    _, depth, cells = model_tiles.shape
    *blocks, table = pl.pallas_call(
        pack_kernel,
        out_shape=[sds((capacity, depth, cells))] * n_shot + [sds((n_shot * (capacity + 1),), jnp.int32)],
        in_specs=[HBM, HBM, HBM],
        out_specs=[VMEM] * n_shot + [SMEM],
        scratch_shapes=[
            pltpu.SMEM(aperture.shape, jnp.int32),
            pltpu.SMEM(tile_slot.shape, jnp.int32),
            pltpu.VMEM(model_tiles.shape, F32),
            pltpu.SemaphoreType.DMA((3,)),
        ],
        compiler_params=params(8),
        name="pack",
    )(in_hbm(aperture), in_hbm(tile_slot), in_hbm(model_tiles))
    return blocks, table


def places(aperture_ref, slot_ref, lat_dev, n_shot, capacity, seen_ref, place_ref):
    me = lax.axis_index("shot")
    for h in range(n_shot):
        seen_ref[h] = 0

    def tile(p, carry):
        holder = quotient(slot_ref[aperture_ref[me, p]], lat_dev)
        rank = seen_ref[holder]
        seen_ref[holder] = rank + 1
        place_ref[p] = round_of(me, holder, n_shot) * capacity + rank
        return carry

    lax.fori_loop(0, aperture_ref.shape[1], tile, 0)


def perturb_kernel(lat_dev, tile_side, aperture_ref, slot_ref, *rest):
    *blocks, out_ref, tiles_ref, seen_ref, place_ref = rest
    n_shot = len(blocks)
    capacity, depth, cells = blocks[0].shape
    side = out_ref.shape[1]
    across = side // tile_side
    flat_ref = out_ref.reshape(depth * side, side)
    places(aperture_ref, slot_ref, lat_dev, n_shot, capacity, seen_ref, place_ref)
    for k in range(n_shot):
        tiles_ref[pl.ds(k * capacity, capacity)] = blocks[k][...]

    def tile_row(i, carry):
        for high in range(cells // side):
            parts = [tiles_ref[place_ref[i * across + j], :, pl.ds(high * side, side)] for j in range(across)]
            for low, part in enumerate(swap_segments(parts, tile_side)):
                flat_ref[pl.ds(i * tile_side + high * across + low, depth, stride=side), :] = part
        return carry

    lax.fori_loop(0, across, tile_row, 0)


def pack_back(lat_dev, tile_side, aperture_ref, slot_ref, corr_ref, blocks, tiles_ref, seen_ref, place_ref):
    n_shot = len(blocks)
    capacity, depth, cells = blocks[0].shape
    side = corr_ref.shape[1]
    across = side // tile_side
    flat_ref = corr_ref.reshape(depth * side, side)
    places(aperture_ref, slot_ref, lat_dev, n_shot, capacity, seen_ref, place_ref)
    tiles_ref[...] = jnp.zeros(tiles_ref.shape, F32)

    def tile_row(i, carry):
        for high in range(cells // side):
            parts = [
                flat_ref[pl.ds(i * tile_side + high * across + low, depth, stride=side), :] for low in range(across)
            ]
            for j, part in enumerate(swap_segments(parts, tile_side)):
                tiles_ref[place_ref[i * across + j], :, pl.ds(high * side, side)] = part
        return carry

    lax.fori_loop(0, across, tile_row, 0)
    for k in range(n_shot):
        blocks[k][...] = tiles_ref[pl.ds(k * capacity, capacity)]


def tile_scratch(n_shot, capacity, depth, cells, n_tiles):
    return [
        pltpu.VMEM((n_shot * capacity, depth, cells), F32),
        pltpu.SMEM((n_shot,), jnp.int32),
        pltpu.SMEM((n_tiles,), jnp.int32),
    ]


def perturb_call(aperture, tile_slot, blocks, side, lat_dev, tile_side):
    capacity, depth, cells = blocks[0].shape
    return pl.pallas_call(
        functools.partial(perturb_kernel, lat_dev, tile_side),
        out_shape=sds((depth, side, side)),
        in_specs=[SMEM, SMEM] + [VMEM] * len(blocks),
        out_specs=VMEM,
        scratch_shapes=tile_scratch(len(blocks), capacity, depth, cells, aperture.shape[1]),
        compiler_params=params(8),
        name="perturb",
    )(aperture, tile_slot, *blocks)


def finish_kernel(n_shot, table_hbm, *refs):
    refs = Refs(refs)
    blocks = refs.take(n_shot)
    parts = refs.refs[:-4]
    sum_ref, record_ref, table_ref, sem = refs.refs[-4:]
    fetch = pltpu.make_async_copy(table_hbm, table_ref, sem)
    fetch.start()
    capacity = blocks[0].shape[0]
    total = parts[0][...]
    for part in parts[1:]:
        total = total + part[...]
    for step in range(total.shape[0]):
        record_ref[step] = total[step : step + 1]
    sum_ref[...] = jnp.zeros(sum_ref.shape, F32)
    fetch.wait()
    for k in range(n_shot):
        base = partner_of(lax.axis_index("shot"), k, n_shot) * (capacity + 1)
        for r in range(capacity):

            @pl.when(r < table_ref[base + capacity])
            def _():
                slot = table_ref[base + r]
                sum_ref[slot] = sum_ref[slot] + blocks[k][r]


def finish_call(table, blocks, parts, lat_dev):
    depth, cells = blocks[0].shape[1:]
    steps, n = parts[0].shape
    return pl.pallas_call(
        functools.partial(finish_kernel, len(blocks)),
        out_shape=[sds((lat_dev, depth, cells)), sds((steps, 1, n))],
        in_specs=[HBM] + [VMEM] * (len(blocks) + len(parts)),
        out_specs=[VMEM, VMEM],
        scratch_shapes=[pltpu.SMEM(table.shape, jnp.int32), pltpu.SemaphoreType.DMA(())],
        compiler_params=params(8),
        name="finish",
    )(table, *blocks, *parts)


def swap(edges):
    count = lax.axis_size("slab")
    shots = lax.axis_size("shot")
    got = []
    for start, edge in enumerate(edges):
        pairs = {}
        for shot in range(shots):
            for i in range(count):
                other = i + 1 if (i - start) % 2 == 0 else i - 1
                if 0 <= other < count:
                    pairs[shot * count + i] = shot * count + other
                elif shots % 2 == 0:
                    pairs[shot * count + i] = (shot ^ 1) * count + i
        got.append(lax.ppermute(edge, ("shot", "slab"), sorted(pairs.items())))
    return tuple(got)


def edges_kernel(groups, *refs):
    refs = Refs(refs)
    fields = [refs.take(n) for n in groups]
    copies = []
    outs = [refs.take(2) for _ in groups]
    sems = refs.take()
    for group, pair in zip(fields, outs):
        depth = group[0].shape[1]
        low = jnp.where(place()[0] == 1, 0, depth - HALO)
        for out_ref, at in zip(pair, (low, depth - HALO - low)):
            for index, field_ref in enumerate(group):
                copies.append(
                    pltpu.make_async_copy(field_ref.at[0, pl.ds(at, HALO)], out_ref.at[index], sems.at[len(copies)])
                )
    for copy in copies:
        copy.start()
    for copy in copies:
        copy.wait()


def first_edges(groups):
    outs = []
    for group in groups:
        outs += [sds((len(group), HALO) + group[0].shape[2:])] * 2
    fields = [in_hbm(field) for group in groups for field in group]
    edges = pl.pallas_call(
        functools.partial(edges_kernel, [len(group) for group in groups]),
        out_shape=outs,
        in_specs=[HBM] * len(fields),
        out_specs=[VMEM] * len(outs),
        scratch_shapes=[pltpu.SemaphoreType.DMA((2 * len(fields),))],
        compiler_params=params(8),
        name="edges",
    )(*fields)
    return [edges[2 * i : 2 * i + 2] for i in range(len(groups))]


def partners():
    count = lax.axis_size("shot")
    if count & (count - 1) == 0:
        return [[s ^ k for s in range(count)] for k in range(count)]
    return [[(k - s) % count for s in range(count)] for k in range(count)]


def rounds(count):
    return sorted(range(count), key=lambda k: (-(k >> 1).bit_count(), k))


def exchange(blocks):
    got = [None] * len(blocks)
    for k in rounds(len(blocks)):
        block, to = blocks[k], partners()[k]
        moves = [(s, t) for s, t in enumerate(to) if s != t]
        kept = [s for s, t in enumerate(to) if s == t]
        if kept and moves:
            moves = moves + [(s, s) for s in kept]
        got[k] = lax.ppermute(block, "shot", moves) if moves else block
    return got


def slab_parts(part):
    count = lax.axis_size("slab")
    parts = [part]
    if count & (count - 1) == 0:
        for bit in range(count.bit_length() - 1):
            part = functools.reduce(jnp.add, parts)
            parts = [part, lax.ppermute(part, "slab", [(s, s ^ (1 << bit)) for s in range(count)])]
    else:
        for k in range(1, count):
            parts.append(lax.ppermute(part, "slab", [(s, (s + k) % count) for s in range(count)]))
    return parts


def per_device(
    model_tiles,
    background,
    u_prev,
    u_now,
    du_prev,
    du_now,
    w_prev,
    w_now,
    wavelet,
    source_cell,
    receiver_cells,
    aperture,
    tile_slot,
):
    lat_dev, depth, tile_cells = model_tiles.shape
    side = background.shape[-1]
    tile_side = math.isqrt(tile_cells)
    capacity = aperture.shape[1] // 4
    steps = wavelet.shape[1]
    speed = background[0]
    u, d, w = u_now[0], du_now[0], w_now[0]
    up, dp, wp = u_prev[0], du_prev[0], w_prev[0]

    tiling = (aperture, tile_slot, lat_dev, tile_side)
    u_edges, dw_edges = first_edges([[u_now], [du_now, w_now]])
    u_halo = swap(u_edges)
    dw_halo = swap(dw_edges)
    outgoing, table = pack_call(aperture, tile_slot, model_tiles, capacity)
    incoming = exchange(outgoing)
    count, outer = count_call(receiver_cells, depth, side)
    perturb = perturb_call(aperture, tile_slot, incoming, side, lat_dev, tile_side)

    u_next, lap, corr, *edges = u_call(0, False, wavelet, source_cell, u, up, u_halo, speed, w_now, None, None, *tiling)
    u_halo = swap(edges)
    bare, *edges = w_bare_call(w, wp, dw_halo, 1, speed)
    w_halo = swap(edges)
    d_next, w_next, *edges = d_call(d, dp, dw_halo, 0, speed, perturb, lap, bare, count)
    d_halo = swap(edges)
    traces = u_local = None
    for step in range(1, steps - 1):
        traces = record_call(receiver_cells, traces, [d_next])
        u, up, d, dp, w, wp = u_next, u, d_next, d, w_next, w
        u_next, lap, corr, *edges = u_call(
            step, False, wavelet, source_cell, u, up, u_halo, speed, w, corr, u_local, *tiling
        )
        u_halo = swap(edges)
        u_local, d_local, w_local = ahead_call([u_next, d, w])
        d_next, w_next, *edges = dw_call(
            d, dp, w, wp, d_halo, w_halo, d_local, w_local, speed, perturb, lap, count, outer if step == 1 else None
        )
        d_halo = swap(edges[:2])
        w_halo = swap(edges[2:])
    u, up, d, dp, w, wp = u_next, u, d_next, d, w_next, w
    step = steps - 1
    u_final, lap, *returning = u_call(step, True, wavelet, source_cell, u, up, u_halo, speed, w, corr, u_local, *tiling)
    arrived = exchange(returning)
    d_final, d_next, traces = last_d_call(step, d, dp, d_halo, speed, perturb, lap, receiver_cells, traces)
    parts = slab_parts(traces)
    (w_final,) = last_w_call(w, wp, w_halo, speed, count, d_next)
    sensitivity, traces = finish_call(table, arrived, parts, lat_dev)
    return (sensitivity, u_final, d_final, w_final, jnp.transpose(traces, (1, 0, 2)))


def solution(mesh):
    field = P("shot", "slab", None, None)
    tiles = P("shot", "slab", None)
    in_specs = (tiles,) + (field,) * 7 + (P("shot", None), P("shot"), P("shot", None), P(), P())
    out_specs = (tiles, field, field, field, P("shot", None, None))


    return jax.shard_map(per_device, mesh=mesh, in_specs=in_specs, out_specs=out_specs, check_vma=False)
```

```python
import functools
import math

import jax
import jax.numpy as jnp
from jax import lax
from jax.experimental import pallas as pl
from jax.experimental.pallas import tpu as pltpu
from jax.sharding import PartitionSpec as P


COEFFS = (-205.0 / 72.0, 8.0 / 5.0, -1.0 / 5.0, 8.0 / 315.0, -1.0 / 560.0)
HALO = len(COEFFS) - 1
SUB = 8
F32 = jnp.float32
VMEM = pl.BlockSpec(memory_space=pltpu.VMEM)
SMEM = pl.BlockSpec(memory_space=pltpu.SMEM)
HBM = pl.BlockSpec(memory_space=pltpu.HBM)


def params(mib):
    return pltpu.CompilerParams(vmem_limit_bytes=mib * 1024 * 1024)


def in_hbm(x):
    return pltpu.with_memory_space_constraint(x, pltpu.HBM)


def sds(shape, dtype=F32):
    return jax.ShapeDtypeStruct(shape, dtype)


def place():
    slab, count = lax.axis_index("slab"), lax.axis_size("slab")
    odd = lax.bitwise_and(slab, 1)
    above, below = slab < count - 1, slab > 0
    is_odd = odd == 1
    return odd, (is_odd & below) | (~is_odd & above), (is_odd & above) | (~is_odd & below)


def quotient(x, m):
    return lax.shift_right_logical(x, m.bit_length() - 1) if m & (m - 1) == 0 else lax.div(x, m)


def remainder(x, m):
    return lax.bitwise_and(x, m - 1) if m & (m - 1) == 0 else lax.rem(x, m)


SCALE = 5040.0
PARTS = 4


def band_weights(side):
    i = lax.broadcasted_iota(jnp.int32, (2 * side, 2 * side), 0)
    j = lax.broadcasted_iota(jnp.int32, (2 * side, 2 * side), 1)
    far = jnp.where((i < side) == (j < side), jnp.abs(i - j), 0)
    out = jnp.zeros((2 * side, 2 * side), F32)
    for k in range(1, HALO + 1):
        out = jnp.where(far == k, round(COEFFS[k] * SCALE) * 1.0, out)
    out = out.astype(jnp.bfloat16)
    return jnp.concatenate([out, out, out], axis=0)


def split3(x):
    high = x.astype(jnp.bfloat16)
    rest = x - high.astype(F32)
    mid = rest.astype(jnp.bfloat16)
    low = (rest - mid.astype(F32)).astype(jnp.bfloat16)
    return high, mid, low


def prepare_local(rows_ref, lanes_ref, now_ref, weights):
    depth, side, _ = now_ref.shape
    zeros = jnp.zeros((SUB, side), F32)
    half = depth // 2
    parts = []
    for low, high in zip(split3(now_ref[pl.ds(0, half)]), split3(now_ref[pl.ds(half, half)])):
        parts += [low.reshape(half * side, side), high.reshape(half * side, side)]
    lanes = jnp.dot(jnp.concatenate(parts, axis=1), weights, preferred_element_type=F32)
    lanes_ref[pl.ds(0, half)] = lanes[:, :side].reshape(half, side, side)
    lanes_ref[pl.ds(half, half)] = lanes[:, side:].reshape(half, side, side)
    for z in range(depth):
        rows_ref[z, pl.ds(0, SUB), :] = zeros
        rows_ref[z, pl.ds(SUB + side, SUB), :] = zeros
        rows_ref[z, pl.ds(SUB, side), :] = now_ref[z]


def prepare_halo(halo_ref, first_ref, second_ref, index, inject=None):
    odd, has_first, has_second = place()

    def halo(z, carry):
        halo_ref[1 - odd, z] = jnp.where(has_first, first_ref[index, z], 0.0)
        halo_ref[odd, z] = jnp.where(has_second, second_ref[index, z], 0.0)
        return carry

    lax.fori_loop(0, HALO, halo, 0)
    if inject:
        outer_ref, other_ref = inject
        for end in range(2):
            for z in range(HALO):
                halo_ref[end, z] = halo_ref[end, z] + outer_ref[end, z] * other_ref[end, z]


def prepare(work, now_ref, first_ref, second_ref, index, weights):
    rows_ref, halo_ref, lanes_ref = work
    prepare_local(rows_ref, lanes_ref, now_ref, weights)
    prepare_halo(halo_ref, first_ref, second_ref, index)


def each_laplacian(work, now_ref, emit, finish=None, parts=1):
    rows_ref, halo_ref, lanes_ref = work
    depth, side, _ = now_ref.shape

    def block(g, carry):
        start = pl.multiple_of(g * SUB, SUB)
        rows = pl.ds(start, SUB)
        column = [halo_ref[0, z, rows, :] for z in range(HALO)]
        column += [now_ref[z, rows, :] for z in range(depth)]
        column += [halo_ref[1, z, rows, :] for z in range(HALO)]
        for z in range(depth):
            centre = column[HALO + z]
            total = (3.0 * COEFFS[0]) * centre + (1.0 / SCALE) * lanes_ref[z, rows, :]
            for k in range(1, HALO + 1):
                ring = (column[HALO + z + k] + column[HALO + z - k]) + (
                    rows_ref[z, pl.ds(start + (SUB + k), SUB), :] + rows_ref[z, pl.ds(start + (SUB - k), SUB), :]
                )
                total = total + COEFFS[k] * ring
            emit(z, rows, centre, total)
        return carry

    blocks = side // SUB // parts
    for part in range(parts):
        lax.fori_loop(part * blocks, (part + 1) * blocks, block, 0)
        if finish:
            finish(part, parts)


def halo_space(side):
    return pltpu.VMEM((2, HALO, side, side), F32)


def work_space(depth, side):
    return [
        pltpu.VMEM((depth, side + 2 * SUB, side), F32),
        halo_space(side),
        pltpu.VMEM((depth, side, side), F32),
    ]


def ahead_kernel(n, *refs):
    weights = band_weights(refs[0].shape[-1])
    for i in range(n):
        prepare_local(refs[n + 2 * i], refs[n + 2 * i + 1], refs[i], weights)


def ahead_call(fields):
    depth, side, _ = fields[0].shape
    outs = [sds((depth, side + 2 * SUB, side)), sds((depth, side, side))] * len(fields)
    res = pl.pallas_call(
        functools.partial(ahead_kernel, len(fields)),
        out_shape=outs,
        in_specs=[VMEM] * len(fields),
        out_specs=[VMEM] * len(outs),
        compiler_params=params(16),
    )(*fields)
    return [res[2 * i : 2 * i + 2] for i in range(len(fields))]


def copy_sends(next_ref, first_ref, second_ref, index):
    depth = next_ref.shape[0]
    odd = place()[0] == 1
    first = jnp.where(odd, 0, depth - HALO)
    second = jnp.where(odd, depth - HALO, 0)
    for z in range(HALO):
        first_ref[index, z] = next_ref[first + z]
        second_ref[index, z] = next_ref[second + z]


def store_out(next_ref, out_ref, sems, step, steps):
    rows = pl.ds(step * (next_ref.shape[1] // steps), next_ref.shape[1] // steps)
    return pltpu.make_async_copy(next_ref.at[:, rows], out_ref.at[0, :, rows], sems.at[step])


def add_source(next_ref, source_ref, wavelet_ref, step, first, rows):
    depth, side, _ = next_ref.shape
    local = source_ref[0] - lax.axis_index("slab") * (depth * side * side)
    mine = (local >= 0) & (local < depth * side * side)
    cell = jnp.where(mine, local, 0)
    z = quotient(cell, side * side)
    x = remainder(quotient(cell, side), side)
    lane = lax.broadcasted_iota(jnp.int32, (1, side), 1)

    @pl.when(mine & (x >= first) & (x < first + rows))
    def _():
        add = jnp.where(lane == remainder(cell, side), wavelet_ref[0, step], 0.0)
        next_ref[z, pl.ds(x, 1), :] = next_ref[z, pl.ds(x, 1), :] + add


class Refs:
    def __init__(self, refs):
        self.refs = list(refs)

    def take(self, n=None):
        if n is None:
            return self.refs.pop(0)
        return [self.refs.pop(0) for _ in range(n)]


def u_kernel(step, last, ahead, tiles, *refs):
    refs = Refs(refs)
    now_ref, ha_ref, hb_ref, w_in = refs.take(4)
    if not last:
        source_ref, wavelet_hbm, prev_ref, speed_ref = refs.take(4)
    corr_in = refs.take() if step else None
    local_work = refs.take(2) if ahead else None
    tables = refs.take(2) if last else []
    if last:
        lap_ref = refs.take()
        blocks = refs.take(tiles[0])
        corr_ref = refs.take()
    else:
        next_ref, lap_ref, corr_ref = refs.take(3)
        sends = refs.take(2)
    halo_ref = refs.take()
    if not ahead:
        local_work = refs.take(2)
    own_sems = refs.take()
    copies = []
    if not last:
        wavelet_ref = refs.take()
        copies.append(pltpu.make_async_copy(wavelet_hbm, wavelet_ref, own_sems.at[0]))
    w_ref = w_in
    if not step:
        w_ref = refs.take()
        half = w_ref.shape[0] // 2
        for i in range(2):
            part = pl.ds(i * half, half)
            copies.append(pltpu.make_async_copy(w_in.at[0, part], w_ref.at[part], own_sems.at[1 + i]))
    if last:
        fetched = refs.take(2)
        tiles_ref, seen_ref, place_ref = refs.take(3)
        for i, (a, b) in enumerate(zip(tables, fetched)):
            copies.append(pltpu.make_async_copy(a, b, own_sems.at[1 + i]))
    for copy in copies:
        copy.start()
    _, side, _ = now_ref.shape
    work = (local_work[0], halo_ref, local_work[1])
    if not ahead:
        prepare_local(*local_work, now_ref, band_weights(side))
    prepare_halo(halo_ref, ha_ref, hb_ref, 0)
    for copy in copies:
        copy.wait()

    def emit(z, block, centre, lap):
        lap_ref[z, block, :] = lap
        part = lap * w_ref[z, block, :]
        corr_ref[z, block, :] = corr_in[z, block, :] + part if step else part
        if not last:
            next_ref[z, block, :] = (2.0 * centre - prev_ref[z, block, :]) + speed_ref[z, block, :] * lap

    each_laplacian(work, now_ref, emit)
    if last:
        pack_back(*tiles[1:], *fetched, corr_ref, blocks, tiles_ref, seen_ref, place_ref)
    else:
        add_source(next_ref, source_ref, wavelet_ref, step, 0, side)
        copy_sends(next_ref, *sends, 0)


def w_bare_kernel(index, now_ref, prev_ref, ha_ref, hb_ref, speed_ref, next_ref, *rest):
    sends, work = rest[:2], rest[2:]
    _, side, _ = now_ref.shape
    prepare(work, now_ref, ha_ref, hb_ref, index, band_weights(side))

    def emit(z, block, centre, lap):
        next_ref[z, block, :] = (2.0 * centre - prev_ref[z, block, :]) + speed_ref[z, block, :] * lap

    each_laplacian(work, now_ref, emit)
    copy_sends(next_ref, *sends, 0)


def d_kernel(index, now_ref, prev_ref, ha_ref, hb_ref, speed_ref, perturb_ref, lap_u_ref, bare_ref, count_ref, *rest):
    next_ref, w_ref, *sends = rest[:4]
    work = rest[4:]
    _, side, _ = now_ref.shape
    prepare(work, now_ref, ha_ref, hb_ref, index, band_weights(side))

    def emit(z, block, centre, lap):
        new = ((2.0 * centre - prev_ref[z, block, :]) + speed_ref[z, block, :] * lap) + (
            perturb_ref[z, block, :] * lap_u_ref[z, block, :]
        )
        next_ref[z, block, :] = new
        w_ref[z, block, :] = bare_ref[z, block, :] + count_ref[z, block, :] * new

    each_laplacian(work, now_ref, emit)
    copy_sends(next_ref, *sends, 0)


def dw_kernel(bare, *refs):
    refs = Refs(refs)
    speed_ref, d_ref, d_prev, w_ref, w_prev, perturb_ref, lap_u_ref, count_ref = refs.take(8)
    d_halo, w_halo = refs.take(2), refs.take(2)
    d_local, w_local = refs.take(2), refs.take(2)
    outer_ref = refs.take() if bare else None
    d_next, w_next = refs.take(2)
    d_sends, w_sends = refs.take(2), refs.take(2)
    d_halos, w_halos = refs.take(2)
    prepare_halo(d_halos, *d_halo, 0)
    prepare_halo(w_halos, *w_halo, 0, (outer_ref, d_halos) if bare else None)
    d_work, w_work = (d_local[0], d_halos, d_local[1]), (w_local[0], w_halos, w_local[1])

    def emit_d(z, block, centre, lap):
        d_next[z, block, :] = ((2.0 * centre - d_prev[z, block, :]) + speed_ref[z, block, :] * lap) + (
            perturb_ref[z, block, :] * lap_u_ref[z, block, :]
        )

    def emit_w(z, block, centre, lap):
        w_next[z, block, :] = ((2.0 * centre - w_prev[z, block, :]) + speed_ref[z, block, :] * lap) + (
            count_ref[z, block, :] * d_next[z, block, :]
        )

    each_laplacian(d_work, d_ref, emit_d)
    copy_sends(d_next, *d_sends, 0)
    each_laplacian(w_work, w_ref, emit_w)
    copy_sends(w_next, *w_sends, 0)


def last_d_kernel(before, *refs):
    refs = Refs(refs)
    now_ref, prev_ref, ha_ref, hb_ref, speed_ref, perturb_ref, lap_u_ref, cells_hbm, cells_ref = refs.take(9)
    u_ref, u_prev, source_ref, wavelet_hbm = refs.take(4)
    early_ref = refs.take() if before else None
    out_ref, next_ref, record_ref, u_out = refs.take(4)
    u_next = refs.take()
    work = refs.take(3)
    cells_smem, wavelet_ref, rows_ref, sems, table_sems = refs.take(5)
    fetches = [
        pltpu.make_async_copy(cells_hbm, cells_smem, table_sems.at[0]),
        pltpu.make_async_copy(wavelet_hbm, wavelet_ref, table_sems.at[1]),
    ]
    for fetch in fetches:
        fetch.start()
    _, side, _ = now_ref.shape
    prepare(work, now_ref, ha_ref, hb_ref, 0, band_weights(side))
    for fetch in fetches:
        fetch.wait()
    last_step = wavelet_ref.shape[1] - 1

    def emit(z, block, centre, lap):
        speed, lap_u = speed_ref[z, block, :], lap_u_ref[z, block, :]
        next_ref[z, block, :] = ((2.0 * centre - prev_ref[z, block, :]) + speed * lap) + (
            perturb_ref[z, block, :] * lap_u
        )
        u_next[z, block, :] = (2.0 * u_ref[z, block, :] - u_prev[z, block, :]) + speed * lap_u

    def finish(part, parts):
        size = side // parts
        add_source(u_next, source_ref, wavelet_ref, last_step, part * size, size)
        store_out(next_ref, out_ref, sems.at[0], part, parts).start()
        store_out(u_next, u_out, sems.at[1], part, parts).start()

    each_laplacian(work, now_ref, emit, finish, PARTS)
    if before:
        record_ref[pl.ds(0, before), :] = early_ref[...]
    fields = [now_ref, next_ref] if record_ref.shape[0] > before + 1 else [next_ref]
    gather_records(before, cells_smem, cells_ref, fields, record_ref, rows_ref)
    for part in range(PARTS):
        store_out(next_ref, out_ref, sems.at[0], part, PARTS).wait()
        store_out(u_next, u_out, sems.at[1], part, PARTS).wait()


def last_w_kernel(*refs):
    refs = Refs(refs)
    now_ref, prev_ref, ha_ref, hb_ref, speed_ref, count_ref, d_next = refs.take(7)
    out_ref, next_ref = refs.take(2)
    work = refs.take(3)
    sems = refs.take()
    _, side, _ = now_ref.shape
    prepare(work, now_ref, ha_ref, hb_ref, 0, band_weights(side))

    def emit(z, block, centre, lap):
        next_ref[z, block, :] = ((2.0 * centre - prev_ref[z, block, :]) + speed_ref[z, block, :] * lap) + (
            count_ref[z, block, :] * d_next[z, block, :]
        )

    def finish(part, parts):
        store_out(next_ref, out_ref, sems, part, parts).start()

    each_laplacian(work, now_ref, emit, finish, PARTS)
    for part in range(PARTS):
        store_out(next_ref, out_ref, sems, part, PARTS).wait()


def stencil_call(body, in_specs, args, outs, kinds, scratch):
    return pl.pallas_call(
        body, out_shape=outs, in_specs=in_specs, out_specs=kinds, scratch_shapes=scratch, compiler_params=params(20)
    )(*args)


def u_call(step, last, wavelet, source, u, u_prev, halo, speed, w, corr, local, aperture, tile_slot, lat_dev, tile_side):
    field = sds(u.shape)
    edge = sds((1, HALO) + u.shape[1:])
    args, specs = [u, *halo, w], [VMEM] * 4
    if not step:
        args[3], specs[3] = in_hbm(w), HBM
    if not last:
        args, specs = args + [source, in_hbm(wavelet), u_prev, speed], specs + [SMEM, HBM, VMEM, VMEM]
    if step:
        args, specs = args + [corr], specs + [VMEM]
    ahead = local is not None
    if ahead:
        args, specs = args + list(local), specs + [VMEM] * 2
    n_shot, n_tiles = aperture.shape
    cells = tile_side * tile_side
    capacity = n_tiles // 4
    rows, halos, lanes = work_space(*u.shape[:2])
    scratch = [halos] + ([] if ahead else [rows, lanes]) + [pltpu.SemaphoreType.DMA((3,))]
    if not last:
        scratch += [pltpu.SMEM(wavelet.shape, F32)]
    if not step:
        scratch += [pltpu.VMEM(u.shape, F32)]
    if last:
        args += [in_hbm(aperture), in_hbm(tile_slot)]
        specs += [HBM, HBM]
        outs = [field] + [sds((capacity, u.shape[0], cells))] * n_shot
        scratch = [pltpu.VMEM(u.shape, F32)] + scratch + [
            pltpu.SMEM(aperture.shape, jnp.int32),
            pltpu.SMEM(tile_slot.shape, jnp.int32),
            *tile_scratch(n_shot, capacity, u.shape[0], cells, n_tiles),
        ]
    else:
        outs = [field] * 3 + [edge] * 2
    body = functools.partial(u_kernel, step, last, ahead, (n_shot, lat_dev, tile_side))
    return stencil_call(body, specs, args, outs, [VMEM] * len(outs), scratch)


def w_bare_call(w, w_prev, halo, index, speed):
    field, edge = sds(w.shape), sds((1, HALO) + w.shape[1:])
    args = [w, w_prev, *halo, speed]
    body = functools.partial(w_bare_kernel, index)
    return stencil_call(body, [VMEM] * 5, args, [field, edge, edge], [VMEM] * 3, work_space(*w.shape[:2]))


def d_call(d, d_prev, halo, index, speed, perturb, lap_u, bare, count):
    field, edge = sds(d.shape), sds((1, HALO) + d.shape[1:])
    args = [d, d_prev, *halo, speed, perturb, lap_u, bare, count]
    body = functools.partial(d_kernel, index)
    outs = [field, field, edge, edge]
    return stencil_call(body, [VMEM] * 9, args, outs, [VMEM] * 4, work_space(*d.shape[:2]))


def dw_call(d, d_prev, w, w_prev, d_halo, w_halo, d_local, w_local, speed, perturb, lap_u, count, outer):
    field, edge = sds(d.shape), sds((1, HALO) + d.shape[1:])
    bare = outer is not None
    args = [speed, d, d_prev, w, w_prev, perturb, lap_u, count, *d_halo, *w_halo, *d_local, *w_local]
    args += [outer] if bare else []
    outs = [field, field] + [edge] * 4
    body = functools.partial(dw_kernel, bare)
    return stencil_call(body, [VMEM] * len(args), args, outs, [VMEM] * 6, [halo_space(d.shape[1])] * 2)


def last_d_call(step, d, d_prev, halo, speed, perturb, lap_u, cells, u, u_prev, source, wavelet, early):
    before = 0 if early is None else early.shape[0]
    n = cells.shape[1]
    fields = step + 1 - before
    args = [d, d_prev, *halo, speed, perturb, lap_u, in_hbm(cells), cells, u, u_prev, source, in_hbm(wavelet)]
    specs = [VMEM] * len(args)
    specs[7], specs[11], specs[12] = HBM, SMEM, HBM
    if before:
        args, specs = args + [early], specs + [VMEM]
    scratch = [pltpu.VMEM(u.shape, F32)] + work_space(*d.shape[:2]) + [
        pltpu.SMEM(cells.shape, jnp.int32),
        pltpu.SMEM(wavelet.shape, F32),
        pltpu.VMEM((fields, n, d.shape[-1]), F32),
        pltpu.SemaphoreType.DMA((2, PARTS)),
        pltpu.SemaphoreType.DMA((2,)),
    ]
    outs = [sds((1,) + d.shape), sds(d.shape), sds((step + 1, n)), sds((1,) + u.shape)]
    body = functools.partial(last_d_kernel, before)
    return stencil_call(body, specs, args, outs, [HBM, VMEM, VMEM, HBM], scratch)


def last_w_call(w, w_prev, halo, speed, count, d_next):
    args = [w, w_prev, *halo, speed, count, d_next]
    scratch = [pltpu.VMEM(w.shape, F32)] + work_space(*w.shape[:2]) + [pltpu.SemaphoreType.DMA((PARTS,))]
    return stencil_call(last_w_kernel, [VMEM] * len(args), args, [sds((1,) + w.shape)], [HBM], scratch)


def count_kernel(cells_ref, count_ref, outer_ref):
    depth, side, _ = count_ref.shape
    local = cells_ref[...] - (lax.axis_index("slab") * depth - HALO) * (side * side)
    n = local.shape[1]
    row_of = jnp.where(local >= 0, quotient(jnp.maximum(local, 0), side), -1)
    lane_of = remainder(jnp.maximum(local, 0), side)
    lanes = lax.broadcasted_iota(jnp.int32, (side, n), 0)
    lane_hot = jnp.where(lanes == lane_of, 1.0, 0.0).astype(jnp.bfloat16)
    for z in range(depth + 2 * HALO):
        row_hot = jnp.where(lanes + z * side == row_of, 1.0, 0.0).astype(jnp.bfloat16)
        plane = lax.dot_general(row_hot, lane_hot, (((1,), (1,)), ((), ())), preferred_element_type=F32)
        if z < HALO:
            outer_ref[0, z] = plane
        elif z < HALO + depth:
            count_ref[z - HALO] = plane
        else:
            outer_ref[1, z - HALO - depth] = plane


def count_call(cells, depth, side):
    return pl.pallas_call(
        count_kernel,
        out_shape=[sds((depth, side, side)), sds((2, HALO, side, side))],
        in_specs=[VMEM],
        out_specs=[VMEM, VMEM],
        compiler_params=params(8),
        name="count",
    )(cells)


def gather_records(before, cells_smem, cells_ref, fields, out_ref, rows_ref):
    depth, side, _ = fields[0].shape
    n = cells_ref.shape[1]
    total = depth * side * side
    start = lax.axis_index("slab") * total
    local = cells_ref[...] - start
    mine = (local >= 0) & (local < total)
    lane_of = jnp.where(mine, remainder(jnp.maximum(local, 0), side), -1)
    lanes = lax.broadcasted_iota(jnp.int32, (side, n), 0)
    hit = lanes == lane_of
    flat = [field_ref.reshape(depth * side, side) for field_ref in fields]

    def gather(r, carry):
        cell = jnp.clip(cells_smem[0, r] - start, 0, total - 1)
        row = quotient(cell, side)
        for step, field_ref in enumerate(flat):
            rows_ref[step, pl.ds(r, 1), :] = field_ref[pl.ds(row, 1), :]
        return carry

    lax.fori_loop(0, n, gather, 0, unroll=32)
    for step in range(len(fields)):
        turned = rows_ref[step].T
        out_ref[pl.ds(before + step, 1), :] = jnp.sum(jnp.where(hit, turned, 0.0), axis=0, keepdims=True)


def record_kernel(before, cells_smem, cells_ref, *rest):
    if before:
        early_ref, rest = rest[0], rest[1:]
    *fields, out_ref, rows_ref = rest
    if before:
        out_ref[pl.ds(0, before), :] = early_ref[...]
    gather_records(before, cells_smem, cells_ref, fields, out_ref, rows_ref)


def record_call(cells, early, fields):
    side = fields[0].shape[-1]
    n = cells.shape[1]
    before = 0 if early is None else early.shape[0]
    args = [cells, cells] + ([early] if before else []) + list(fields)
    return pl.pallas_call(
        functools.partial(record_kernel, before),
        out_shape=sds((before + len(fields), n)),
        in_specs=[SMEM] + [VMEM] * (len(args) - 1),
        out_specs=VMEM,
        scratch_shapes=[pltpu.VMEM((len(fields), n, side), F32)],
        compiler_params=params(8),
    )(*args)


def swap_segments(parts, segment):
    count = len(parts)
    lanes = count * segment
    lane = lax.broadcasted_iota(jnp.int32, parts[0].shape, 1)
    parts = list(parts)
    bit = count // 2
    while bit:
        low = lax.rem(lax.div(lane, bit * segment), 2) == 0
        for a in range(count):
            if not a & bit:
                first, second = parts[a], parts[a + bit]
                parts[a] = jnp.where(low, first, pltpu.roll(second, bit * segment, 1))
                parts[a + bit] = jnp.where(low, pltpu.roll(first, lanes - bit * segment, 1), second)
        bit //= 2
    return parts


def partner_of(me, k, count):
    if count & (count - 1) == 0:
        return lax.bitwise_xor(me, k)
    return lax.rem(k - me + count, count)


def round_of(me, other, count):
    if count & (count - 1) == 0:
        return lax.bitwise_xor(me, other)
    return lax.rem(me + other, count)


def pack_kernel(aperture_hbm, slot_hbm, tiles_hbm, *rest):
    *outs, table_ref, aperture_ref, slot_ref, tiles_ref, sems = rest
    pairs = ((aperture_hbm, aperture_ref), (slot_hbm, slot_ref), (tiles_hbm, tiles_ref))
    copies = [pltpu.make_async_copy(a, b, sems.at[i]) for i, (a, b) in enumerate(pairs)]
    for copy in copies:
        copy.start()
    lat_dev = tiles_ref.shape[0]
    n_shot = len(outs)
    capacity = outs[0].shape[0]
    me = lax.axis_index("shot")
    n_tiles = aperture_ref.shape[1]
    copies[0].wait()
    copies[1].wait()

    def shot(s, carry):
        for r in range(capacity):
            table_ref[s * (capacity + 1) + r] = 0
        seen = jnp.int32(0)
        for p in range(n_tiles):
            slot = slot_ref[aperture_ref[s, p]]
            mine = quotient(slot, lat_dev) == me

            @pl.when(mine)
            def _():
                table_ref[s * (capacity + 1) + seen] = remainder(slot, lat_dev)

            seen = seen + mine.astype(jnp.int32)
        table_ref[s * (capacity + 1) + capacity] = seen
        return carry

    lax.fori_loop(0, n_shot, shot, 0)
    copies[2].wait()
    for k in range(n_shot):
        base = partner_of(me, k, n_shot) * (capacity + 1)
        for r in range(capacity):
            outs[k][r] = tiles_ref[table_ref[base + r]]


def pack_call(aperture, tile_slot, model_tiles, capacity):
    n_shot = aperture.shape[0]
    _, depth, cells = model_tiles.shape
    *blocks, table = pl.pallas_call(
        pack_kernel,
        out_shape=[sds((capacity, depth, cells))] * n_shot + [sds((n_shot * (capacity + 1),), jnp.int32)],
        in_specs=[HBM, HBM, HBM],
        out_specs=[VMEM] * n_shot + [SMEM],
        scratch_shapes=[
            pltpu.SMEM(aperture.shape, jnp.int32),
            pltpu.SMEM(tile_slot.shape, jnp.int32),
            pltpu.VMEM(model_tiles.shape, F32),
            pltpu.SemaphoreType.DMA((3,)),
        ],
        compiler_params=params(8),
        name="pack",
    )(in_hbm(aperture), in_hbm(tile_slot), in_hbm(model_tiles))
    return blocks, table


def places(aperture_ref, slot_ref, lat_dev, n_shot, capacity, seen_ref, place_ref):
    me = lax.axis_index("shot")
    for h in range(n_shot):
        seen_ref[h] = 0

    def tile(p, carry):
        holder = quotient(slot_ref[aperture_ref[me, p]], lat_dev)
        rank = seen_ref[holder]
        seen_ref[holder] = rank + 1
        place_ref[p] = round_of(me, holder, n_shot) * capacity + rank
        return carry

    lax.fori_loop(0, aperture_ref.shape[1], tile, 0)


def perturb_kernel(lat_dev, tile_side, aperture_ref, slot_ref, *rest):
    *blocks, out_ref, tiles_ref, seen_ref, place_ref = rest
    n_shot = len(blocks)
    capacity, depth, cells = blocks[0].shape
    side = out_ref.shape[1]
    across = side // tile_side
    flat_ref = out_ref.reshape(depth * side, side)
    places(aperture_ref, slot_ref, lat_dev, n_shot, capacity, seen_ref, place_ref)
    for k in range(n_shot):
        tiles_ref[pl.ds(k * capacity, capacity)] = blocks[k][...]

    def tile_row(i, carry):
        for high in range(cells // side):
            parts = [tiles_ref[place_ref[i * across + j], :, pl.ds(high * side, side)] for j in range(across)]
            for low, part in enumerate(swap_segments(parts, tile_side)):
                flat_ref[pl.ds(i * tile_side + high * across + low, depth, stride=side), :] = part
        return carry

    lax.fori_loop(0, across, tile_row, 0)


def pack_back(lat_dev, tile_side, aperture_ref, slot_ref, corr_ref, blocks, tiles_ref, seen_ref, place_ref):
    n_shot = len(blocks)
    capacity, depth, cells = blocks[0].shape
    side = corr_ref.shape[1]
    across = side // tile_side
    flat_ref = corr_ref.reshape(depth * side, side)
    places(aperture_ref, slot_ref, lat_dev, n_shot, capacity, seen_ref, place_ref)

    def tile_row(i, carry):
        for high in range(cells // side):
            parts = [
                flat_ref[pl.ds(i * tile_side + high * across + low, depth, stride=side), :] for low in range(across)
            ]
            for j, part in enumerate(swap_segments(parts, tile_side)):
                tiles_ref[place_ref[i * across + j], :, pl.ds(high * side, side)] = part
        return carry

    lax.fori_loop(0, across, tile_row, 0)
    for k in range(n_shot):
        blocks[k][...] = tiles_ref[pl.ds(k * capacity, capacity)]


def tile_scratch(n_shot, capacity, depth, cells, n_tiles):
    return [
        pltpu.VMEM((n_shot * capacity, depth, cells), F32),
        pltpu.SMEM((n_shot,), jnp.int32),
        pltpu.SMEM((n_tiles,), jnp.int32),
    ]


def perturb_call(aperture, tile_slot, blocks, side, lat_dev, tile_side):
    capacity, depth, cells = blocks[0].shape
    return pl.pallas_call(
        functools.partial(perturb_kernel, lat_dev, tile_side),
        out_shape=sds((depth, side, side)),
        in_specs=[SMEM, SMEM] + [VMEM] * len(blocks),
        out_specs=VMEM,
        scratch_shapes=tile_scratch(len(blocks), capacity, depth, cells, aperture.shape[1]),
        compiler_params=params(8),
        name="perturb",
    )(aperture, tile_slot, *blocks)


def finish_kernel(n_shot, table_hbm, *refs):
    refs = Refs(refs)
    blocks = refs.take(n_shot)
    parts = refs.refs[:-4]
    sum_ref, record_ref, table_ref, sem = refs.refs[-4:]
    fetch = pltpu.make_async_copy(table_hbm, table_ref, sem)
    fetch.start()
    capacity = blocks[0].shape[0]
    total = parts[0][...]
    for part in parts[1:]:
        total = total + part[...]
    for step in range(total.shape[0]):
        record_ref[step] = total[step : step + 1]
    sum_ref[...] = jnp.zeros(sum_ref.shape, F32)
    fetch.wait()
    for k in range(n_shot):
        base = partner_of(lax.axis_index("shot"), k, n_shot) * (capacity + 1)
        for r in range(capacity):

            @pl.when(r < table_ref[base + capacity])
            def _():
                slot = table_ref[base + r]
                sum_ref[slot] = sum_ref[slot] + blocks[k][r]


def finish_call(table, blocks, parts, lat_dev):
    depth, cells = blocks[0].shape[1:]
    steps, n = parts[0].shape
    return pl.pallas_call(
        functools.partial(finish_kernel, len(blocks)),
        out_shape=[sds((lat_dev, depth, cells)), sds((steps, 1, n))],
        in_specs=[HBM] + [VMEM] * (len(blocks) + len(parts)),
        out_specs=[VMEM, VMEM],
        scratch_shapes=[pltpu.SMEM(table.shape, jnp.int32), pltpu.SemaphoreType.DMA(())],
        compiler_params=params(8),
        name="finish",
    )(table, *blocks, *parts)


def swap(edges):
    count = lax.axis_size("slab")
    shots = lax.axis_size("shot")
    got = []
    for start, edge in enumerate(edges):
        pairs = {}
        for shot in range(shots):
            for i in range(count):
                other = i + 1 if (i - start) % 2 == 0 else i - 1
                if 0 <= other < count:
                    pairs[shot * count + i] = shot * count + other
                elif shots % 2 == 0:
                    pairs[shot * count + i] = (shot ^ 1) * count + i
        got.append(lax.ppermute(edge, ("shot", "slab"), sorted(pairs.items())))
    return tuple(got)


def edges_kernel(n, *refs):
    fields, outs, sems = refs[:n], refs[n:-1], refs[-1]
    depth = fields[0].shape[1]
    low = jnp.where(place()[0] == 1, 0, depth - HALO)
    copies = []
    for out_ref, at in zip(outs, (low, depth - HALO - low)):
        for index, field_ref in enumerate(fields):
            copies.append(
                pltpu.make_async_copy(field_ref.at[0, pl.ds(at, HALO)], out_ref.at[index], sems.at[len(copies)])
            )
    for copy in copies:
        copy.start()
    for copy in copies:
        copy.wait()


def first_edges(fields):
    n = len(fields)
    edge = sds((n, HALO) + fields[0].shape[2:])
    return pl.pallas_call(
        functools.partial(edges_kernel, n),
        out_shape=[edge, edge],
        in_specs=[HBM] * n,
        out_specs=[VMEM, VMEM],
        scratch_shapes=[pltpu.SemaphoreType.DMA((2 * n,))],
        compiler_params=params(8),
    )(*map(in_hbm, fields))


def partners():
    count = lax.axis_size("shot")
    if count & (count - 1) == 0:
        return [[s ^ k for s in range(count)] for k in range(count)]
    return [[(k - s) % count for s in range(count)] for k in range(count)]


def rounds(count):
    return sorted(range(count), key=lambda k: (-(k >> 1).bit_count(), k))


def exchange(blocks):
    got = [None] * len(blocks)
    for k in rounds(len(blocks)):
        block, to = blocks[k], partners()[k]
        moves = [(s, t) for s, t in enumerate(to) if s != t]
        kept = [s for s, t in enumerate(to) if s == t]
        if kept and moves:
            moves = moves + [(s, s) for s in kept]
        got[k] = lax.ppermute(block, "shot", moves) if moves else block
    return got


def slab_parts(part):
    count = lax.axis_size("slab")
    parts = [part]
    for k in range(1, count):
        to = [s ^ k for s in range(count)] if count & (count - 1) == 0 else [(s + k) % count for s in range(count)]
        parts.append(lax.ppermute(part, "slab", list(enumerate(to))))
    return parts


def per_device(
    model_tiles,
    background,
    u_prev,
    u_now,
    du_prev,
    du_now,
    w_prev,
    w_now,
    wavelet,
    source_cell,
    receiver_cells,
    aperture,
    tile_slot,
):
    lat_dev, depth, tile_cells = model_tiles.shape
    side = background.shape[-1]
    tile_side = math.isqrt(tile_cells)
    capacity = aperture.shape[1] // 4
    steps = wavelet.shape[1]
    speed = background[0]
    u, d, w = u_now[0], du_now[0], w_now[0]
    up, dp, wp = u_prev[0], du_prev[0], w_prev[0]

    tiling = (aperture, tile_slot, lat_dev, tile_side)
    u_halo = swap(first_edges([u_now]))
    dw_halo = swap(first_edges([du_now, w_now]))
    outgoing, table = pack_call(aperture, tile_slot, model_tiles, capacity)
    incoming = exchange(outgoing)
    count, outer = count_call(receiver_cells, depth, side)
    perturb = perturb_call(aperture, tile_slot, incoming, side, lat_dev, tile_side)

    u_next, lap, corr, *edges = u_call(0, False, wavelet, source_cell, u, up, u_halo, speed, w_now, None, None, *tiling)
    u_halo = swap(edges)
    bare, *edges = w_bare_call(w, wp, dw_halo, 1, speed)
    w_halo = swap(edges)
    d_next, w_next, *edges = d_call(d, dp, dw_halo, 0, speed, perturb, lap, bare, count)
    d_halo = swap(edges)
    traces = u_local = None
    for step in range(1, steps - 1):
        traces = record_call(receiver_cells, traces, [d_next])
        u, up, d, dp, w, wp = u_next, u, d_next, d, w_next, w
        u_next, lap, corr, *edges = u_call(
            step, False, wavelet, source_cell, u, up, u_halo, speed, w, corr, u_local, *tiling
        )
        u_halo = swap(edges)
        u_local, d_local, w_local = ahead_call([u_next, d, w])
        d_next, w_next, *edges = dw_call(
            d, dp, w, wp, d_halo, w_halo, d_local, w_local, speed, perturb, lap, count, outer if step == 1 else None
        )
        d_halo = swap(edges[:2])
        w_halo = swap(edges[2:])
    u, up, d, dp, w, wp = u_next, u, d_next, d, w_next, w
    step = steps - 1
    lap, *returning = u_call(step, True, wavelet, source_cell, u, up, u_halo, speed, w, corr, u_local, *tiling)
    arrived = exchange(returning)
    d_final, d_next, traces, u_final = last_d_call(
        step, d, dp, d_halo, speed, perturb, lap, receiver_cells, u, up, source_cell, wavelet, traces
    )
    parts = slab_parts(traces)
    (w_final,) = last_w_call(w, wp, w_halo, speed, count, d_next)
    sensitivity, traces = finish_call(table, arrived, parts, lat_dev)
    return (sensitivity, u_final, d_final, w_final, jnp.transpose(traces, (1, 0, 2)))


def solution(mesh):
    field = P("shot", "slab", None, None)
    tiles = P("shot", "slab", None)
    in_specs = (tiles,) + (field,) * 7 + (P("shot", None), P("shot"), P("shot", None), P(), P())
    out_specs = (tiles, field, field, field, P("shot", None, None))


    return jax.shard_map(per_device, mesh=mesh, in_specs=in_specs, out_specs=out_specs, check_vma=False)
```

```python
import functools
import math

import jax
import jax.numpy as jnp
from jax import lax
from jax.experimental import pallas as pl
from jax.experimental.pallas import tpu as pltpu
from jax.sharding import PartitionSpec as P


COEFFS = (-205.0 / 72.0, 8.0 / 5.0, -1.0 / 5.0, 8.0 / 315.0, -1.0 / 560.0)
HALO = len(COEFFS) - 1
SUB = 8
F32 = jnp.float32
VMEM = pl.BlockSpec(memory_space=pltpu.VMEM)
SMEM = pl.BlockSpec(memory_space=pltpu.SMEM)
HBM = pl.BlockSpec(memory_space=pltpu.HBM)


def params(mib):
    return pltpu.CompilerParams(vmem_limit_bytes=mib * 1024 * 1024)


def in_hbm(x):
    return pltpu.with_memory_space_constraint(x, pltpu.HBM)


def sds(shape, dtype=F32):
    return jax.ShapeDtypeStruct(shape, dtype)


def place():
    slab, count = lax.axis_index("slab"), lax.axis_size("slab")
    odd = lax.bitwise_and(slab, 1)
    above, below = slab < count - 1, slab > 0
    is_odd = odd == 1
    return odd, (is_odd & below) | (~is_odd & above), (is_odd & above) | (~is_odd & below)


def quotient(x, m):
    return lax.shift_right_logical(x, m.bit_length() - 1) if m & (m - 1) == 0 else lax.div(x, m)


def remainder(x, m):
    return lax.bitwise_and(x, m - 1) if m & (m - 1) == 0 else lax.rem(x, m)


SCALE = 5040.0
PARTS = 4


def band_weights(side):
    i = lax.broadcasted_iota(jnp.int32, (2 * side, 2 * side), 0)
    j = lax.broadcasted_iota(jnp.int32, (2 * side, 2 * side), 1)
    far = jnp.where((i < side) == (j < side), jnp.abs(i - j), 0)
    out = jnp.zeros((2 * side, 2 * side), F32)
    for k in range(1, HALO + 1):
        out = jnp.where(far == k, round(COEFFS[k] * SCALE) * 1.0, out)
    out = out.astype(jnp.bfloat16)
    return jnp.concatenate([out, out, out], axis=0)


def split3(x):
    high = x.astype(jnp.bfloat16)
    rest = x - high.astype(F32)
    mid = rest.astype(jnp.bfloat16)
    low = (rest - mid.astype(F32)).astype(jnp.bfloat16)
    return high, mid, low


def prepare_local(rows_ref, lanes_ref, now_ref, weights):
    depth, side, _ = now_ref.shape
    zeros = jnp.zeros((SUB, side), F32)
    half = depth // 2
    parts = []
    for low, high in zip(split3(now_ref[pl.ds(0, half)]), split3(now_ref[pl.ds(half, half)])):
        parts += [low.reshape(half * side, side), high.reshape(half * side, side)]
    lanes = jnp.dot(jnp.concatenate(parts, axis=1), weights, preferred_element_type=F32)
    lanes_ref[pl.ds(0, half)] = lanes[:, :side].reshape(half, side, side)
    lanes_ref[pl.ds(half, half)] = lanes[:, side:].reshape(half, side, side)
    for z in range(depth):
        rows_ref[z, pl.ds(0, SUB), :] = zeros
        rows_ref[z, pl.ds(SUB + side, SUB), :] = zeros
        rows_ref[z, pl.ds(SUB, side), :] = now_ref[z]


def prepare_halo(halo_ref, first_ref, second_ref, index, inject=None):
    odd, has_first, has_second = place()

    def halo(z, carry):
        halo_ref[1 - odd, z] = jnp.where(has_first, first_ref[index, z], 0.0)
        halo_ref[odd, z] = jnp.where(has_second, second_ref[index, z], 0.0)
        return carry

    lax.fori_loop(0, HALO, halo, 0)
    if inject:
        outer_ref, other_ref = inject
        for end in range(2):
            for z in range(HALO):
                halo_ref[end, z] = halo_ref[end, z] + outer_ref[end, z] * other_ref[end, z]


def prepare(work, now_ref, first_ref, second_ref, index, weights):
    rows_ref, halo_ref, lanes_ref = work
    prepare_local(rows_ref, lanes_ref, now_ref, weights)
    prepare_halo(halo_ref, first_ref, second_ref, index)


def each_laplacian(work, now_ref, emit, finish=None, parts=1):
    rows_ref, halo_ref, lanes_ref = work
    depth, side, _ = now_ref.shape

    def block(g, carry):
        start = pl.multiple_of(g * SUB, SUB)
        rows = pl.ds(start, SUB)
        column = [halo_ref[0, z, rows, :] for z in range(HALO)]
        column += [now_ref[z, rows, :] for z in range(depth)]
        column += [halo_ref[1, z, rows, :] for z in range(HALO)]
        for z in range(depth):
            centre = column[HALO + z]
            total = (3.0 * COEFFS[0]) * centre + (1.0 / SCALE) * lanes_ref[z, rows, :]
            for k in range(1, HALO + 1):
                ring = (column[HALO + z + k] + column[HALO + z - k]) + (
                    rows_ref[z, pl.ds(start + (SUB + k), SUB), :] + rows_ref[z, pl.ds(start + (SUB - k), SUB), :]
                )
                total = total + COEFFS[k] * ring
            emit(z, rows, centre, total)
        return carry

    blocks = side // SUB // parts
    for part in range(parts):
        lax.fori_loop(part * blocks, (part + 1) * blocks, block, 0)
        if finish:
            finish(part, parts)


def halo_space(side):
    return pltpu.VMEM((2, HALO, side, side), F32)


def work_space(depth, side):
    return [
        pltpu.VMEM((depth, side + 2 * SUB, side), F32),
        halo_space(side),
        pltpu.VMEM((depth, side, side), F32),
    ]


def ahead_kernel(n, *refs):
    weights = band_weights(refs[0].shape[-1])
    for i in range(n):
        prepare_local(refs[n + 2 * i], refs[n + 2 * i + 1], refs[i], weights)


def ahead_call(fields):
    depth, side, _ = fields[0].shape
    outs = [sds((depth, side + 2 * SUB, side)), sds((depth, side, side))] * len(fields)
    res = pl.pallas_call(
        functools.partial(ahead_kernel, len(fields)),
        out_shape=outs,
        in_specs=[VMEM] * len(fields),
        out_specs=[VMEM] * len(outs),
        compiler_params=params(16),
    )(*fields)
    return [res[2 * i : 2 * i + 2] for i in range(len(fields))]


def copy_sends(next_ref, first_ref, second_ref, index):
    depth = next_ref.shape[0]
    odd = place()[0] == 1
    first = jnp.where(odd, 0, depth - HALO)
    second = jnp.where(odd, depth - HALO, 0)
    for z in range(HALO):
        first_ref[index, z] = next_ref[first + z]
        second_ref[index, z] = next_ref[second + z]


def store_out(next_ref, out_ref, sems, step, steps):
    rows = pl.ds(step * (next_ref.shape[1] // steps), next_ref.shape[1] // steps)
    return pltpu.make_async_copy(next_ref.at[:, rows], out_ref.at[0, :, rows], sems.at[step])


def add_source(next_ref, source_ref, wavelet_ref, step, first, rows):
    depth, side, _ = next_ref.shape
    local = source_ref[0] - lax.axis_index("slab") * (depth * side * side)
    mine = (local >= 0) & (local < depth * side * side)
    cell = jnp.where(mine, local, 0)
    z = quotient(cell, side * side)
    x = remainder(quotient(cell, side), side)
    lane = lax.broadcasted_iota(jnp.int32, (1, side), 1)

    @pl.when(mine & (x >= first) & (x < first + rows))
    def _():
        add = jnp.where(lane == remainder(cell, side), wavelet_ref[0, step], 0.0)
        next_ref[z, pl.ds(x, 1), :] = next_ref[z, pl.ds(x, 1), :] + add


class Refs:
    def __init__(self, refs):
        self.refs = list(refs)

    def take(self, n=None):
        if n is None:
            return self.refs.pop(0)
        return [self.refs.pop(0) for _ in range(n)]


def u_kernel(step, last, ahead, tiles, *refs):
    refs = Refs(refs)
    now_ref, ha_ref, hb_ref, w_in = refs.take(4)
    if not last:
        source_ref, wavelet_hbm, prev_ref, speed_ref = refs.take(4)
    corr_in = refs.take() if step else None
    local_work = refs.take(2) if ahead else None
    tables = refs.take(2) if last else []
    if last:
        lap_ref = refs.take()
        blocks = refs.take(tiles[0])
        corr_ref = refs.take()
    else:
        next_ref, lap_ref, corr_ref = refs.take(3)
        sends = refs.take(2)
    halo_ref = refs.take()
    if not ahead:
        local_work = refs.take(2)
    own_sems = refs.take()
    copies, late = [], []
    if not last:
        wavelet_ref = refs.take()
        late.append(pltpu.make_async_copy(wavelet_hbm, wavelet_ref, own_sems.at[0]))
    w_ref = w_in
    if not step:
        w_ref = refs.take()
        half = w_ref.shape[0] // 2
        for i in range(2):
            part = pl.ds(i * half, half)
            copies.append(pltpu.make_async_copy(w_in.at[0, part], w_ref.at[part], own_sems.at[1 + i]))
    if last:
        fetched = refs.take(2)
        tiles_ref, seen_ref, place_ref = refs.take(3)
        for i, (a, b) in enumerate(zip(tables, fetched)):
            late.append(pltpu.make_async_copy(a, b, own_sems.at[1 + i]))
    for copy in copies + late:
        copy.start()
    _, side, _ = now_ref.shape
    work = (local_work[0], halo_ref, local_work[1])
    if not ahead:
        prepare_local(*local_work, now_ref, band_weights(side))
    prepare_halo(halo_ref, ha_ref, hb_ref, 0)
    for copy in copies:
        copy.wait()

    def emit(z, block, centre, lap):
        lap_ref[z, block, :] = lap
        part = lap * w_ref[z, block, :]
        corr_ref[z, block, :] = corr_in[z, block, :] + part if step else part
        if not last:
            next_ref[z, block, :] = (2.0 * centre - prev_ref[z, block, :]) + speed_ref[z, block, :] * lap

    each_laplacian(work, now_ref, emit)
    for copy in late:
        copy.wait()
    if last:
        pack_back(*tiles[1:], *fetched, corr_ref, blocks, tiles_ref, seen_ref, place_ref)
    else:
        add_source(next_ref, source_ref, wavelet_ref, step, 0, side)
        copy_sends(next_ref, *sends, 0)


def w_bare_kernel(index, now_ref, prev_ref, ha_ref, hb_ref, speed_ref, next_ref, *rest):
    sends, work = rest[:2], rest[2:]
    _, side, _ = now_ref.shape
    prepare(work, now_ref, ha_ref, hb_ref, index, band_weights(side))

    def emit(z, block, centre, lap):
        next_ref[z, block, :] = (2.0 * centre - prev_ref[z, block, :]) + speed_ref[z, block, :] * lap

    each_laplacian(work, now_ref, emit)
    copy_sends(next_ref, *sends, 0)


def d_kernel(index, now_ref, prev_ref, ha_ref, hb_ref, speed_ref, perturb_ref, lap_u_ref, bare_ref, count_ref, *rest):
    next_ref, w_ref, *sends = rest[:4]
    work = rest[4:]
    _, side, _ = now_ref.shape
    prepare(work, now_ref, ha_ref, hb_ref, index, band_weights(side))

    def emit(z, block, centre, lap):
        new = ((2.0 * centre - prev_ref[z, block, :]) + speed_ref[z, block, :] * lap) + (
            perturb_ref[z, block, :] * lap_u_ref[z, block, :]
        )
        next_ref[z, block, :] = new
        w_ref[z, block, :] = bare_ref[z, block, :] + count_ref[z, block, :] * new

    each_laplacian(work, now_ref, emit)
    copy_sends(next_ref, *sends, 0)


def dw_kernel(bare, *refs):
    refs = Refs(refs)
    speed_ref, d_ref, d_prev, w_ref, w_prev, perturb_ref, lap_u_ref, count_ref = refs.take(8)
    d_halo, w_halo = refs.take(2), refs.take(2)
    d_local, w_local = refs.take(2), refs.take(2)
    outer_ref = refs.take() if bare else None
    d_next, w_next = refs.take(2)
    d_sends, w_sends = refs.take(2), refs.take(2)
    d_halos, w_halos = refs.take(2)
    prepare_halo(d_halos, *d_halo, 0)
    prepare_halo(w_halos, *w_halo, 0, (outer_ref, d_halos) if bare else None)
    d_work, w_work = (d_local[0], d_halos, d_local[1]), (w_local[0], w_halos, w_local[1])

    def emit_d(z, block, centre, lap):
        d_next[z, block, :] = ((2.0 * centre - d_prev[z, block, :]) + speed_ref[z, block, :] * lap) + (
            perturb_ref[z, block, :] * lap_u_ref[z, block, :]
        )

    def emit_w(z, block, centre, lap):
        w_next[z, block, :] = ((2.0 * centre - w_prev[z, block, :]) + speed_ref[z, block, :] * lap) + (
            count_ref[z, block, :] * d_next[z, block, :]
        )

    each_laplacian(d_work, d_ref, emit_d)
    copy_sends(d_next, *d_sends, 0)
    each_laplacian(w_work, w_ref, emit_w)
    copy_sends(w_next, *w_sends, 0)


def last_d_kernel(before, *refs):
    refs = Refs(refs)
    now_ref, prev_ref, ha_ref, hb_ref, speed_ref, perturb_ref, lap_u_ref, cells_ref, rows_hbm = refs.take(9)
    early_ref = refs.take() if before else None
    out_ref, next_ref, record_ref = refs.take(3)
    work = refs.take(3)
    rows_smem, rows_ref, sems, table_sem = refs.take(4)
    fetch = pltpu.make_async_copy(rows_hbm, rows_smem, table_sem)
    fetch.start()
    _, side, _ = now_ref.shape
    prepare(work, now_ref, ha_ref, hb_ref, 0, band_weights(side))

    def emit(z, block, centre, lap):
        next_ref[z, block, :] = ((2.0 * centre - prev_ref[z, block, :]) + speed_ref[z, block, :] * lap) + (
            perturb_ref[z, block, :] * lap_u_ref[z, block, :]
        )

    def finish(part, parts):
        store_out(next_ref, out_ref, sems, part, parts).start()

    each_laplacian(work, now_ref, emit, finish, PARTS)
    fetch.wait()
    if before:
        record_ref[pl.ds(0, before), :] = early_ref[...]
    fields = [now_ref, next_ref] if record_ref.shape[0] > before + 1 else [next_ref]
    gather_records(before, lambda r: rows_smem[0, r], cells_ref, fields, record_ref, rows_ref)
    for part in range(PARTS):
        store_out(next_ref, out_ref, sems, part, PARTS).wait()


def last_w_kernel(*refs):
    refs = Refs(refs)
    now_ref, prev_ref, ha_ref, hb_ref, speed_ref, count_ref, d_next = refs.take(7)
    u_ref, u_prev, lap_u_ref, source_ref, wavelet_hbm = refs.take(5)
    out_ref, u_out = refs.take(2)
    next_ref, u_next = refs.take(2)
    work = refs.take(3)
    wavelet_ref, sems, table_sem = refs.take(3)
    fetch = pltpu.make_async_copy(wavelet_hbm, wavelet_ref, table_sem)
    fetch.start()
    _, side, _ = now_ref.shape
    prepare(work, now_ref, ha_ref, hb_ref, 0, band_weights(side))
    last_step = wavelet_ref.shape[1] - 1

    def emit(z, block, centre, lap):
        speed = speed_ref[z, block, :]
        next_ref[z, block, :] = ((2.0 * centre - prev_ref[z, block, :]) + speed * lap) + (
            count_ref[z, block, :] * d_next[z, block, :]
        )
        u_next[z, block, :] = (2.0 * u_ref[z, block, :] - u_prev[z, block, :]) + speed * lap_u_ref[z, block, :]

    def finish(part, parts):
        size = side // parts
        if part == 0:
            fetch.wait()
        add_source(u_next, source_ref, wavelet_ref, last_step, part * size, size)
        store_out(next_ref, out_ref, sems.at[0], part, parts).start()
        store_out(u_next, u_out, sems.at[1], part, parts).start()

    each_laplacian(work, now_ref, emit, finish, PARTS)
    for part in range(PARTS):
        store_out(next_ref, out_ref, sems.at[0], part, PARTS).wait()
        store_out(u_next, u_out, sems.at[1], part, PARTS).wait()


def stencil_call(body, in_specs, args, outs, kinds, scratch):
    return pl.pallas_call(
        body, out_shape=outs, in_specs=in_specs, out_specs=kinds, scratch_shapes=scratch, compiler_params=params(20)
    )(*args)


def u_call(step, last, wavelet, source, u, u_prev, halo, speed, w, corr, local, aperture, tile_slot, lat_dev, tile_side):
    field = sds(u.shape)
    edge = sds((1, HALO) + u.shape[1:])
    args, specs = [u, *halo, w], [VMEM] * 4
    if not step:
        args[3], specs[3] = in_hbm(w), HBM
    if not last:
        args, specs = args + [source, in_hbm(wavelet), u_prev, speed], specs + [SMEM, HBM, VMEM, VMEM]
    if step:
        args, specs = args + [corr], specs + [VMEM]
    ahead = local is not None
    if ahead:
        args, specs = args + list(local), specs + [VMEM] * 2
    n_shot, n_tiles = aperture.shape
    cells = tile_side * tile_side
    capacity = n_tiles // 4
    rows, halos, lanes = work_space(*u.shape[:2])
    scratch = [halos] + ([] if ahead else [rows, lanes]) + [pltpu.SemaphoreType.DMA((3,))]
    if not last:
        scratch += [pltpu.SMEM(wavelet.shape, F32)]
    if not step:
        scratch += [pltpu.VMEM(u.shape, F32)]
    if last:
        args += [in_hbm(aperture), in_hbm(tile_slot)]
        specs += [HBM, HBM]
        outs = [field] + [sds((capacity, u.shape[0], cells))] * n_shot
        scratch = [pltpu.VMEM(u.shape, F32)] + scratch + [
            pltpu.SMEM(aperture.shape, jnp.int32),
            pltpu.SMEM(tile_slot.shape, jnp.int32),
            *tile_scratch(n_shot, capacity, u.shape[0], cells, n_tiles),
        ]
    else:
        outs = [field] * 3 + [edge] * 2
    body = functools.partial(u_kernel, step, last, ahead, (n_shot, lat_dev, tile_side))
    return stencil_call(body, specs, args, outs, [VMEM] * len(outs), scratch)


def w_bare_call(w, w_prev, halo, index, speed):
    field, edge = sds(w.shape), sds((1, HALO) + w.shape[1:])
    args = [w, w_prev, *halo, speed]
    body = functools.partial(w_bare_kernel, index)
    return stencil_call(body, [VMEM] * 5, args, [field, edge, edge], [VMEM] * 3, work_space(*w.shape[:2]))


def d_call(d, d_prev, halo, index, speed, perturb, lap_u, bare, count):
    field, edge = sds(d.shape), sds((1, HALO) + d.shape[1:])
    args = [d, d_prev, *halo, speed, perturb, lap_u, bare, count]
    body = functools.partial(d_kernel, index)
    outs = [field, field, edge, edge]
    return stencil_call(body, [VMEM] * 9, args, outs, [VMEM] * 4, work_space(*d.shape[:2]))


def dw_call(d, d_prev, w, w_prev, d_halo, w_halo, d_local, w_local, speed, perturb, lap_u, count, outer):
    field, edge = sds(d.shape), sds((1, HALO) + d.shape[1:])
    bare = outer is not None
    args = [speed, d, d_prev, w, w_prev, perturb, lap_u, count, *d_halo, *w_halo, *d_local, *w_local]
    args += [outer] if bare else []
    outs = [field, field] + [edge] * 4
    body = functools.partial(dw_kernel, bare)
    return stencil_call(body, [VMEM] * len(args), args, outs, [VMEM] * 6, [halo_space(d.shape[1])] * 2)


def last_d_call(step, d, d_prev, halo, speed, perturb, lap_u, cells, rows, early):
    before = 0 if early is None else early.shape[0]
    n = cells.shape[1]
    fields = step + 1 - before
    args = [d, d_prev, *halo, speed, perturb, lap_u, cells, rows]
    specs = [VMEM] * 8 + [HBM]
    if before:
        args, specs = args + [early], specs + [VMEM]
    scratch = work_space(*d.shape[:2]) + [
        pltpu.SMEM(cells.shape, jnp.int32),
        pltpu.VMEM((fields, n, d.shape[-1]), F32),
        pltpu.SemaphoreType.DMA((PARTS,)),
        pltpu.SemaphoreType.DMA(()),
    ]
    outs = [sds((1,) + d.shape), sds(d.shape), sds((step + 1, n))]
    body = functools.partial(last_d_kernel, before)
    return stencil_call(body, specs, args, outs, [HBM, VMEM, VMEM], scratch)


def last_w_call(w, w_prev, halo, speed, count, d_next, u, u_prev, lap_u, source, wavelet):
    args = [w, w_prev, *halo, speed, count, d_next, u, u_prev, lap_u, source, in_hbm(wavelet)]
    specs = [VMEM] * 10 + [SMEM, HBM]
    scratch = [pltpu.VMEM(w.shape, F32)] * 2 + work_space(*w.shape[:2]) + [
        pltpu.SMEM(wavelet.shape, F32),
        pltpu.SemaphoreType.DMA((2, PARTS)),
        pltpu.SemaphoreType.DMA(()),
    ]
    outs = [sds((1,) + w.shape)] * 2
    return stencil_call(last_w_kernel, specs, args, outs, [HBM] * 2, scratch)


def count_kernel(cells_ref, count_ref, outer_ref):
    depth, side, _ = count_ref.shape
    local = cells_ref[...] - (lax.axis_index("slab") * depth - HALO) * (side * side)
    n = local.shape[1]
    row_of = jnp.where(local >= 0, quotient(jnp.maximum(local, 0), side), -1)
    lane_of = remainder(jnp.maximum(local, 0), side)
    lanes = lax.broadcasted_iota(jnp.int32, (side, n), 0)
    lane_hot = jnp.where(lanes == lane_of, 1.0, 0.0).astype(jnp.bfloat16)
    for z in range(depth + 2 * HALO):
        row_hot = jnp.where(lanes + z * side == row_of, 1.0, 0.0).astype(jnp.bfloat16)
        plane = lax.dot_general(row_hot, lane_hot, (((1,), (1,)), ((), ())), preferred_element_type=F32)
        if z < HALO:
            outer_ref[0, z] = plane
        elif z < HALO + depth:
            count_ref[z - HALO] = plane
        else:
            outer_ref[1, z - HALO - depth] = plane


def count_call(cells, depth, side):
    return pl.pallas_call(
        count_kernel,
        out_shape=[sds((depth, side, side)), sds((2, HALO, side, side))],
        in_specs=[VMEM],
        out_specs=[VMEM, VMEM],
        compiler_params=params(8),
        name="count",
    )(cells)


def gather_records(before, row_of, cells_ref, fields, out_ref, rows_ref):
    depth, side, _ = fields[0].shape
    n = cells_ref.shape[1]
    total = depth * side * side
    local = cells_ref[...] - lax.axis_index("slab") * total
    mine = (local >= 0) & (local < total)
    lane_of = jnp.where(mine, remainder(jnp.maximum(local, 0), side), -1)
    lanes = lax.broadcasted_iota(jnp.int32, (side, n), 0)
    hit = lanes == lane_of
    flat = [field_ref.reshape(depth * side, side) for field_ref in fields]

    def gather(r, carry):
        row = row_of(r)
        for step, field_ref in enumerate(flat):
            rows_ref[step, pl.ds(r, 1), :] = field_ref[pl.ds(row, 1), :]
        return carry

    lax.fori_loop(0, n, gather, 0, unroll=32)
    for step in range(len(fields)):
        turned = rows_ref[step].T
        out_ref[pl.ds(before + step, 1), :] = jnp.sum(jnp.where(hit, turned, 0.0), axis=0, keepdims=True)


def record_kernel(before, cells_smem, cells_ref, *rest):
    if before:
        early_ref, rest = rest[0], rest[1:]
    *fields, out_ref, table_ref, rows_ref = rest
    if before:
        out_ref[pl.ds(0, before), :] = early_ref[...]
    depth, side, _ = fields[0].shape
    total = depth * side * side
    start = lax.axis_index("slab") * total

    def row_of(r):
        row = quotient(jnp.clip(cells_smem[0, r] - start, 0, total - 1), side)
        table_ref[0, r] = row
        return row

    gather_records(before, row_of, cells_ref, fields, out_ref, rows_ref)


def record_call(cells, early, fields):
    side = fields[0].shape[-1]
    n = cells.shape[1]
    before = 0 if early is None else early.shape[0]
    args = [cells, cells] + ([early] if before else []) + list(fields)
    return pl.pallas_call(
        functools.partial(record_kernel, before),
        out_shape=[sds((before + len(fields), n)), sds(cells.shape, jnp.int32)],
        in_specs=[SMEM] + [VMEM] * (len(args) - 1),
        out_specs=[VMEM, SMEM],
        scratch_shapes=[pltpu.VMEM((len(fields), n, side), F32)],
        compiler_params=params(8),
    )(*args)


def swap_segments(parts, segment):
    count = len(parts)
    lanes = count * segment
    lane = lax.broadcasted_iota(jnp.int32, parts[0].shape, 1)
    parts = list(parts)
    bit = count // 2
    while bit:
        low = lax.rem(lax.div(lane, bit * segment), 2) == 0
        for a in range(count):
            if not a & bit:
                first, second = parts[a], parts[a + bit]
                parts[a] = jnp.where(low, first, pltpu.roll(second, bit * segment, 1))
                parts[a + bit] = jnp.where(low, pltpu.roll(first, lanes - bit * segment, 1), second)
        bit //= 2
    return parts


def partner_of(me, k, count):
    if count & (count - 1) == 0:
        return lax.bitwise_xor(me, k)
    return lax.rem(k - me + count, count)


def round_of(me, other, count):
    if count & (count - 1) == 0:
        return lax.bitwise_xor(me, other)
    return lax.rem(me + other, count)


def pack_kernel(aperture_hbm, slot_hbm, tiles_hbm, *rest):
    *outs, table_ref, aperture_ref, slot_ref, tiles_ref, sems = rest
    pairs = ((aperture_hbm, aperture_ref), (slot_hbm, slot_ref), (tiles_hbm, tiles_ref))
    copies = [pltpu.make_async_copy(a, b, sems.at[i]) for i, (a, b) in enumerate(pairs)]
    for copy in copies:
        copy.start()
    lat_dev = tiles_ref.shape[0]
    n_shot = len(outs)
    capacity = outs[0].shape[0]
    me = lax.axis_index("shot")
    n_tiles = aperture_ref.shape[1]
    copies[0].wait()
    copies[1].wait()

    def shot(s, carry):
        for r in range(capacity):
            table_ref[s * (capacity + 1) + r] = 0
        seen = jnp.int32(0)
        for p in range(n_tiles):
            slot = slot_ref[aperture_ref[s, p]]
            mine = quotient(slot, lat_dev) == me

            @pl.when(mine)
            def _():
                table_ref[s * (capacity + 1) + seen] = remainder(slot, lat_dev)

            seen = seen + mine.astype(jnp.int32)
        table_ref[s * (capacity + 1) + capacity] = seen
        return carry

    lax.fori_loop(0, n_shot, shot, 0)
    copies[2].wait()
    for k in range(n_shot):
        base = partner_of(me, k, n_shot) * (capacity + 1)
        for r in range(capacity):
            outs[k][r] = tiles_ref[table_ref[base + r]]


def pack_call(aperture, tile_slot, model_tiles, capacity):
    n_shot = aperture.shape[0]
    _, depth, cells = model_tiles.shape
    *blocks, table = pl.pallas_call(
        pack_kernel,
        out_shape=[sds((capacity, depth, cells))] * n_shot + [sds((n_shot * (capacity + 1),), jnp.int32)],
        in_specs=[HBM, HBM, HBM],
        out_specs=[VMEM] * n_shot + [SMEM],
        scratch_shapes=[
            pltpu.SMEM(aperture.shape, jnp.int32),
            pltpu.SMEM(tile_slot.shape, jnp.int32),
            pltpu.VMEM(model_tiles.shape, F32),
            pltpu.SemaphoreType.DMA((3,)),
        ],
        compiler_params=params(8),
        name="pack",
    )(in_hbm(aperture), in_hbm(tile_slot), in_hbm(model_tiles))
    return blocks, table


def places(aperture_ref, slot_ref, lat_dev, n_shot, capacity, seen_ref, place_ref):
    me = lax.axis_index("shot")
    for h in range(n_shot):
        seen_ref[h] = 0

    def tile(p, carry):
        holder = quotient(slot_ref[aperture_ref[me, p]], lat_dev)
        rank = seen_ref[holder]
        seen_ref[holder] = rank + 1
        place_ref[p] = round_of(me, holder, n_shot) * capacity + rank
        return carry

    lax.fori_loop(0, aperture_ref.shape[1], tile, 0)


def perturb_kernel(lat_dev, tile_side, aperture_hbm, slot_hbm, *rest):
    *blocks, out_ref, tiles_ref, seen_ref, place_ref, aperture_ref, slot_ref, sems = rest
    copies = [
        pltpu.make_async_copy(aperture_hbm, aperture_ref, sems.at[0]),
        pltpu.make_async_copy(slot_hbm, slot_ref, sems.at[1]),
    ]
    for copy in copies:
        copy.start()
    n_shot = len(blocks)
    capacity, depth, cells = blocks[0].shape
    side = out_ref.shape[1]
    across = side // tile_side
    flat_ref = out_ref.reshape(depth * side, side)
    for k in range(n_shot):
        tiles_ref[pl.ds(k * capacity, capacity)] = blocks[k][...]
    for copy in copies:
        copy.wait()
    places(aperture_ref, slot_ref, lat_dev, n_shot, capacity, seen_ref, place_ref)

    def tile_row(i, carry):
        for high in range(cells // side):
            parts = [tiles_ref[place_ref[i * across + j], :, pl.ds(high * side, side)] for j in range(across)]
            for low, part in enumerate(swap_segments(parts, tile_side)):
                flat_ref[pl.ds(i * tile_side + high * across + low, depth, stride=side), :] = part
        return carry

    lax.fori_loop(0, across, tile_row, 0)


def pack_back(lat_dev, tile_side, aperture_ref, slot_ref, corr_ref, blocks, tiles_ref, seen_ref, place_ref):
    n_shot = len(blocks)
    capacity, depth, cells = blocks[0].shape
    side = corr_ref.shape[1]
    across = side // tile_side
    flat_ref = corr_ref.reshape(depth * side, side)
    places(aperture_ref, slot_ref, lat_dev, n_shot, capacity, seen_ref, place_ref)

    def tile_row(i, carry):
        for high in range(cells // side):
            parts = [
                flat_ref[pl.ds(i * tile_side + high * across + low, depth, stride=side), :] for low in range(across)
            ]
            for j, part in enumerate(swap_segments(parts, tile_side)):
                tiles_ref[place_ref[i * across + j], :, pl.ds(high * side, side)] = part
        return carry

    lax.fori_loop(0, across, tile_row, 0)
    for k in range(n_shot):
        blocks[k][...] = tiles_ref[pl.ds(k * capacity, capacity)]


def tile_scratch(n_shot, capacity, depth, cells, n_tiles):
    return [
        pltpu.VMEM((n_shot * capacity, depth, cells), F32),
        pltpu.SMEM((n_shot,), jnp.int32),
        pltpu.SMEM((n_tiles,), jnp.int32),
    ]


def perturb_call(aperture, tile_slot, blocks, side, lat_dev, tile_side):
    capacity, depth, cells = blocks[0].shape
    return pl.pallas_call(
        functools.partial(perturb_kernel, lat_dev, tile_side),
        out_shape=sds((depth, side, side)),
        in_specs=[HBM, HBM] + [VMEM] * len(blocks),
        out_specs=VMEM,
        scratch_shapes=[
            *tile_scratch(len(blocks), capacity, depth, cells, aperture.shape[1]),
            pltpu.SMEM(aperture.shape, jnp.int32),
            pltpu.SMEM(tile_slot.shape, jnp.int32),
            pltpu.SemaphoreType.DMA((2,)),
        ],
        compiler_params=params(8),
        name="perturb",
    )(in_hbm(aperture), in_hbm(tile_slot), *blocks)


def finish_kernel(n_shot, table_hbm, *refs):
    refs = Refs(refs)
    blocks = refs.take(n_shot)
    parts = refs.refs[:-4]
    sum_ref, record_ref, table_ref, sem = refs.refs[-4:]
    fetch = pltpu.make_async_copy(table_hbm, table_ref, sem)
    fetch.start()
    capacity = blocks[0].shape[0]
    total = parts[0][...]
    for part in parts[1:]:
        total = total + part[...]
    for step in range(total.shape[0]):
        record_ref[step] = total[step : step + 1]
    sum_ref[...] = jnp.zeros(sum_ref.shape, F32)
    fetch.wait()
    for k in range(n_shot):
        base = partner_of(lax.axis_index("shot"), k, n_shot) * (capacity + 1)
        for r in range(capacity):

            @pl.when(r < table_ref[base + capacity])
            def _():
                slot = table_ref[base + r]
                sum_ref[slot] = sum_ref[slot] + blocks[k][r]


def finish_call(table, blocks, parts, lat_dev):
    depth, cells = blocks[0].shape[1:]
    steps, n = parts[0].shape
    return pl.pallas_call(
        functools.partial(finish_kernel, len(blocks)),
        out_shape=[sds((lat_dev, depth, cells)), sds((steps, 1, n))],
        in_specs=[HBM] + [VMEM] * (len(blocks) + len(parts)),
        out_specs=[VMEM, VMEM],
        scratch_shapes=[pltpu.SMEM(table.shape, jnp.int32), pltpu.SemaphoreType.DMA(())],
        compiler_params=params(8),
        name="finish",
    )(table, *blocks, *parts)


def swap(edges):
    count = lax.axis_size("slab")
    shots = lax.axis_size("shot")
    got = []
    for start, edge in enumerate(edges):
        pairs = {}
        for shot in range(shots):
            for i in range(count):
                other = i + 1 if (i - start) % 2 == 0 else i - 1
                if 0 <= other < count:
                    pairs[shot * count + i] = shot * count + other
                elif shots % 2 == 0:
                    pairs[shot * count + i] = (shot ^ 1) * count + i
        got.append(lax.ppermute(edge, ("shot", "slab"), sorted(pairs.items())))
    return tuple(got)


def edges_kernel(n, *refs):
    fields, outs, sems = refs[:n], refs[n:-1], refs[-1]
    depth = fields[0].shape[1]
    low = jnp.where(place()[0] == 1, 0, depth - HALO)
    copies = []
    for out_ref, at in zip(outs, (low, depth - HALO - low)):
        for index, field_ref in enumerate(fields):
            copies.append(
                pltpu.make_async_copy(field_ref.at[0, pl.ds(at, HALO)], out_ref.at[index], sems.at[len(copies)])
            )
    for copy in copies:
        copy.start()
    for copy in copies:
        copy.wait()


def first_edges(fields):
    n = len(fields)
    edge = sds((n, HALO) + fields[0].shape[2:])
    return pl.pallas_call(
        functools.partial(edges_kernel, n),
        out_shape=[edge, edge],
        in_specs=[HBM] * n,
        out_specs=[VMEM, VMEM],
        scratch_shapes=[pltpu.SemaphoreType.DMA((2 * n,))],
        compiler_params=params(8),
    )(*map(in_hbm, fields))


def partners():
    count = lax.axis_size("shot")
    if count & (count - 1) == 0:
        return [[s ^ k for s in range(count)] for k in range(count)]
    return [[(k - s) % count for s in range(count)] for k in range(count)]


def rounds(count):
    return sorted(range(count), key=lambda k: (-(k >> 1).bit_count(), k))


def exchange(blocks):
    got = [None] * len(blocks)
    for k in rounds(len(blocks)):
        block, to = blocks[k], partners()[k]
        moves = [(s, t) for s, t in enumerate(to) if s != t]
        kept = [s for s, t in enumerate(to) if s == t]
        if kept and moves:
            moves = moves + [(s, s) for s in kept]
        got[k] = lax.ppermute(block, "shot", moves) if moves else block
    return got


def slab_parts(part):
    count = lax.axis_size("slab")
    parts = [part]
    for k in range(count - 1, 0, -1):
        to = [s ^ k for s in range(count)] if count & (count - 1) == 0 else [(s + k) % count for s in range(count)]
        parts.append(lax.ppermute(part, "slab", list(enumerate(to))))
    return parts


def per_device(
    model_tiles,
    background,
    u_prev,
    u_now,
    du_prev,
    du_now,
    w_prev,
    w_now,
    wavelet,
    source_cell,
    receiver_cells,
    aperture,
    tile_slot,
):
    lat_dev, depth, tile_cells = model_tiles.shape
    side = background.shape[-1]
    tile_side = math.isqrt(tile_cells)
    capacity = aperture.shape[1] // 4
    steps = wavelet.shape[1]
    speed = background[0]
    u, d, w = u_now[0], du_now[0], w_now[0]
    up, dp, wp = u_prev[0], du_prev[0], w_prev[0]

    tiling = (aperture, tile_slot, lat_dev, tile_side)
    u_halo = swap(first_edges([u_now]))
    dw_halo = swap(first_edges([du_now, w_now]))
    outgoing, table = pack_call(aperture, tile_slot, model_tiles, capacity)
    incoming = exchange(outgoing)
    count, outer = count_call(receiver_cells, depth, side)
    perturb = perturb_call(aperture, tile_slot, incoming, side, lat_dev, tile_side)

    u_next, lap, corr, *edges = u_call(0, False, wavelet, source_cell, u, up, u_halo, speed, w_now, None, None, *tiling)
    u_halo = swap(edges)
    bare, *edges = w_bare_call(w, wp, dw_halo, 1, speed)
    w_halo = swap(edges)
    d_next, w_next, *edges = d_call(d, dp, dw_halo, 0, speed, perturb, lap, bare, count)
    d_halo = swap(edges)
    traces = u_local = None
    for step in range(1, steps - 1):
        traces, receiver_rows = record_call(receiver_cells, traces, [d_next])
        u, up, d, dp, w, wp = u_next, u, d_next, d, w_next, w
        u_next, lap, corr, *edges = u_call(
            step, False, wavelet, source_cell, u, up, u_halo, speed, w, corr, u_local, *tiling
        )
        u_halo = swap(edges)
        u_local, d_local, w_local = ahead_call([u_next, d, w])
        d_next, w_next, *edges = dw_call(
            d, dp, w, wp, d_halo, w_halo, d_local, w_local, speed, perturb, lap, count, outer if step == 1 else None
        )
        d_halo = swap(edges[:2])
        w_halo = swap(edges[2:])
    u, up, d, dp, w, wp = u_next, u, d_next, d, w_next, w
    step = steps - 1
    lap, *returning = u_call(step, True, wavelet, source_cell, u, up, u_halo, speed, w, corr, u_local, *tiling)
    arrived = exchange(returning)
    d_final, d_next, traces = last_d_call(
        step, d, dp, d_halo, speed, perturb, lap, receiver_cells, receiver_rows, traces
    )
    parts = slab_parts(traces)
    w_final, u_final = last_w_call(w, wp, w_halo, speed, count, d_next, u, up, lap, source_cell, wavelet)
    sensitivity, traces = finish_call(table, arrived, parts, lat_dev)
    return (sensitivity, u_final, d_final, w_final, jnp.transpose(traces, (1, 0, 2)))


def solution(mesh):
    field = P("shot", "slab", None, None)
    tiles = P("shot", "slab", None)
    in_specs = (tiles,) + (field,) * 7 + (P("shot", None), P("shot"), P("shot", None), P(), P())
    out_specs = (tiles, field, field, field, P("shot", None, None))


    return jax.shard_map(per_device, mesh=mesh, in_specs=in_specs, out_specs=out_specs, check_vma=False)
```

```python
import functools
import math

import jax
import jax.numpy as jnp
from jax import lax
from jax.experimental import pallas as pl
from jax.experimental.pallas import tpu as pltpu
from jax.sharding import PartitionSpec as P


COEFFS = (-205.0 / 72.0, 8.0 / 5.0, -1.0 / 5.0, 8.0 / 315.0, -1.0 / 560.0)
HALO = len(COEFFS) - 1
SUB = 8
F32 = jnp.float32
VMEM = pl.BlockSpec(memory_space=pltpu.VMEM)
SMEM = pl.BlockSpec(memory_space=pltpu.SMEM)
HBM = pl.BlockSpec(memory_space=pltpu.HBM)


def params(mib):
    return pltpu.CompilerParams(vmem_limit_bytes=mib * 1024 * 1024)


def in_hbm(x):
    return pltpu.with_memory_space_constraint(x, pltpu.HBM)


def sds(shape, dtype=F32):
    return jax.ShapeDtypeStruct(shape, dtype)


def place():
    slab, count = lax.axis_index("slab"), lax.axis_size("slab")
    odd = lax.bitwise_and(slab, 1)
    above, below = slab < count - 1, slab > 0
    is_odd = odd == 1
    return odd, (is_odd & below) | (~is_odd & above), (is_odd & above) | (~is_odd & below)


def quotient(x, m):
    return lax.shift_right_logical(x, m.bit_length() - 1) if m & (m - 1) == 0 else lax.div(x, m)


def remainder(x, m):
    return lax.bitwise_and(x, m - 1) if m & (m - 1) == 0 else lax.rem(x, m)


SCALE = 5040.0
PARTS = 4


def band_weights(side):
    i = lax.broadcasted_iota(jnp.int32, (2 * side, 2 * side), 0)
    j = lax.broadcasted_iota(jnp.int32, (2 * side, 2 * side), 1)
    far = jnp.where((i < side) == (j < side), jnp.abs(i - j), 0)
    out = jnp.zeros((2 * side, 2 * side), F32)
    for k in range(1, HALO + 1):
        out = jnp.where(far == k, round(COEFFS[k] * SCALE) * 1.0, out)
    out = out.astype(jnp.bfloat16)
    return jnp.concatenate([out, out, out], axis=0)


def split3(x):
    high = x.astype(jnp.bfloat16)
    rest = x - high.astype(F32)
    mid = rest.astype(jnp.bfloat16)
    low = (rest - mid.astype(F32)).astype(jnp.bfloat16)
    return high, mid, low


def prepare_local(rows_ref, lanes_ref, now_ref, weights):
    depth, side, _ = now_ref.shape
    zeros = jnp.zeros((SUB, side), F32)
    half = depth // 2
    parts = []
    for low, high in zip(split3(now_ref[pl.ds(0, half)]), split3(now_ref[pl.ds(half, half)])):
        parts += [low.reshape(half * side, side), high.reshape(half * side, side)]
    lanes = jnp.dot(jnp.concatenate(parts, axis=1), weights, preferred_element_type=F32)
    lanes_ref[pl.ds(0, half)] = lanes[:, :side].reshape(half, side, side)
    lanes_ref[pl.ds(half, half)] = lanes[:, side:].reshape(half, side, side)
    for z in range(depth):
        rows_ref[z, pl.ds(0, SUB), :] = zeros
        rows_ref[z, pl.ds(SUB + side, SUB), :] = zeros
        rows_ref[z, pl.ds(SUB, side), :] = now_ref[z]


def prepare_halo(halo_ref, first_ref, second_ref, index, inject=None):
    odd, has_first, has_second = place()

    def halo(z, carry):
        halo_ref[1 - odd, z] = jnp.where(has_first, first_ref[index, z], 0.0)
        halo_ref[odd, z] = jnp.where(has_second, second_ref[index, z], 0.0)
        return carry

    lax.fori_loop(0, HALO, halo, 0)
    if inject:
        outer_ref, other_ref = inject
        for end in range(2):
            for z in range(HALO):
                halo_ref[end, z] = halo_ref[end, z] + outer_ref[end, z] * other_ref[end, z]


def prepare(work, now_ref, first_ref, second_ref, index, weights):
    rows_ref, halo_ref, lanes_ref = work
    prepare_local(rows_ref, lanes_ref, now_ref, weights)
    prepare_halo(halo_ref, first_ref, second_ref, index)


def each_laplacian(work, now_ref, emit, finish=None, parts=1):
    rows_ref, halo_ref, lanes_ref = work
    depth, side, _ = now_ref.shape

    def block(g, carry):
        start = pl.multiple_of(g * SUB, SUB)
        rows = pl.ds(start, SUB)
        column = [halo_ref[0, z, rows, :] for z in range(HALO)]
        column += [now_ref[z, rows, :] for z in range(depth)]
        column += [halo_ref[1, z, rows, :] for z in range(HALO)]
        for z in range(depth):
            centre = column[HALO + z]
            total = (3.0 * COEFFS[0]) * centre + (1.0 / SCALE) * lanes_ref[z, rows, :]
            for k in range(1, HALO + 1):
                ring = (column[HALO + z + k] + column[HALO + z - k]) + (
                    rows_ref[z, pl.ds(start + (SUB + k), SUB), :] + rows_ref[z, pl.ds(start + (SUB - k), SUB), :]
                )
                total = total + COEFFS[k] * ring
            emit(z, rows, centre, total)
        return carry

    blocks = side // SUB // parts
    for part in range(parts):
        lax.fori_loop(part * blocks, (part + 1) * blocks, block, 0)
        if finish:
            finish(part, parts)


def halo_space(side):
    return pltpu.VMEM((2, HALO, side, side), F32)


def work_space(depth, side):
    return [
        pltpu.VMEM((depth, side + 2 * SUB, side), F32),
        halo_space(side),
        pltpu.VMEM((depth, side, side), F32),
    ]


def ahead_kernel(n, *refs):
    fields, outs, (rows_ref, lanes_ref) = refs[:n], refs[n:-2], refs[-2:]
    depth, side, _ = fields[0].shape
    weights = band_weights(side)
    for now_ref, out_ref in zip(fields, outs):
        prepare_local(rows_ref, lanes_ref, now_ref, weights)

        def block(g, carry, now_ref=now_ref, out_ref=out_ref):
            start = pl.multiple_of(g * SUB, SUB)
            rows = pl.ds(start, SUB)
            column = [now_ref[z, rows, :] for z in range(depth)]
            for z in range(depth):
                total = (3.0 * COEFFS[0]) * column[z] + (1.0 / SCALE) * lanes_ref[z, rows, :]
                for k in range(1, HALO + 1):
                    ring = (
                        rows_ref[z, pl.ds(start + (SUB + k), SUB), :] + rows_ref[z, pl.ds(start + (SUB - k), SUB), :]
                    )
                    if z + k < depth:
                        ring = ring + column[z + k]
                    if z - k >= 0:
                        ring = ring + column[z - k]
                    total = total + COEFFS[k] * ring
                out_ref[z, rows, :] = total
            return carry

        lax.fori_loop(0, side // SUB, block, 0)


def ahead_call(fields):
    depth, side, _ = fields[0].shape
    outs = [sds((depth, side, side))] * len(fields)
    rows, _, lanes = work_space(depth, side)
    return pl.pallas_call(
        functools.partial(ahead_kernel, len(fields)),
        out_shape=outs,
        in_specs=[VMEM] * len(fields),
        out_specs=[VMEM] * len(outs),
        scratch_shapes=[rows, lanes],
        compiler_params=params(16),
    )(*fields)


def each_remainder(halo_ref, local_ref, now_ref, emit):
    depth, side, _ = now_ref.shape

    def block(g, carry):
        rows = pl.ds(pl.multiple_of(g * SUB, SUB), SUB)
        below = [halo_ref[0, z, rows, :] for z in range(HALO)]
        above = [halo_ref[1, z, rows, :] for z in range(HALO)]
        for z in range(depth):
            total = local_ref[z, rows, :]
            for k in range(1, HALO + 1):
                if z - k < 0:
                    total = total + COEFFS[k] * below[HALO + z - k]
                if z + k >= depth:
                    total = total + COEFFS[k] * above[z + k - depth]
            emit(z, rows, now_ref[z, rows, :], total)
        return carry

    lax.fori_loop(0, side // SUB, block, 0)


def copy_sends(next_ref, first_ref, second_ref, index):
    depth = next_ref.shape[0]
    odd = place()[0] == 1
    first = jnp.where(odd, 0, depth - HALO)
    second = jnp.where(odd, depth - HALO, 0)
    for z in range(HALO):
        first_ref[index, z] = next_ref[first + z]
        second_ref[index, z] = next_ref[second + z]


def store_out(next_ref, out_ref, sems, step, steps):
    rows = pl.ds(step * (next_ref.shape[1] // steps), next_ref.shape[1] // steps)
    return pltpu.make_async_copy(next_ref.at[:, rows], out_ref.at[0, :, rows], sems.at[step])


def add_source(next_ref, source_ref, wavelet_ref, step, first, rows):
    depth, side, _ = next_ref.shape
    local = source_ref[0] - lax.axis_index("slab") * (depth * side * side)
    mine = (local >= 0) & (local < depth * side * side)
    cell = jnp.where(mine, local, 0)
    z = quotient(cell, side * side)
    x = remainder(quotient(cell, side), side)
    lane = lax.broadcasted_iota(jnp.int32, (1, side), 1)

    @pl.when(mine & (x >= first) & (x < first + rows))
    def _():
        add = jnp.where(lane == remainder(cell, side), wavelet_ref[0, step], 0.0)
        next_ref[z, pl.ds(x, 1), :] = next_ref[z, pl.ds(x, 1), :] + add


class Refs:
    def __init__(self, refs):
        self.refs = list(refs)

    def take(self, n=None):
        if n is None:
            return self.refs.pop(0)
        return [self.refs.pop(0) for _ in range(n)]


def u_kernel(step, last, ahead, tiles, *refs):
    refs = Refs(refs)
    now_ref, ha_ref, hb_ref, w_in = refs.take(4)
    if not last:
        source_ref, wavelet_hbm, prev_ref, speed_ref = refs.take(4)
    corr_in = refs.take() if step else None
    local_ref = refs.take() if ahead else None
    tables = refs.take(2) if last else []
    if last:
        lap_ref = refs.take()
        blocks = refs.take(tiles[0])
        corr_ref = refs.take()
    else:
        next_ref, lap_ref, corr_ref = refs.take(3)
        sends = refs.take(2)
    halo_ref = refs.take()
    if not ahead:
        rows_ref, lanes_ref = refs.take(2)
    own_sems = refs.take()
    copies, late = [], []
    if not last:
        wavelet_ref = refs.take()
        late.append(pltpu.make_async_copy(wavelet_hbm, wavelet_ref, own_sems.at[0]))
    w_ref = w_in
    if not step:
        w_ref = refs.take()
        half = w_ref.shape[0] // 2
        for i in range(2):
            part = pl.ds(i * half, half)
            copies.append(pltpu.make_async_copy(w_in.at[0, part], w_ref.at[part], own_sems.at[1 + i]))
    if last:
        fetched = refs.take(2)
        tiles_ref, seen_ref, place_ref = refs.take(3)
        for i, (a, b) in enumerate(zip(tables, fetched)):
            late.append(pltpu.make_async_copy(a, b, own_sems.at[1 + i]))
    for copy in copies + late:
        copy.start()
    _, side, _ = now_ref.shape
    if not ahead:
        prepare_local(rows_ref, lanes_ref, now_ref, band_weights(side))
    prepare_halo(halo_ref, ha_ref, hb_ref, 0)
    for copy in copies:
        copy.wait()

    def emit(z, block, centre, lap):
        lap_ref[z, block, :] = lap
        part = lap * w_ref[z, block, :]
        corr_ref[z, block, :] = corr_in[z, block, :] + part if step else part
        if not last:
            next_ref[z, block, :] = (2.0 * centre - prev_ref[z, block, :]) + speed_ref[z, block, :] * lap

    if ahead:
        each_remainder(halo_ref, local_ref, now_ref, emit)
    else:
        each_laplacian((rows_ref, halo_ref, lanes_ref), now_ref, emit)
    for copy in late:
        copy.wait()
    if last:
        pack_back(*tiles[1:], *fetched, corr_ref, blocks, tiles_ref, seen_ref, place_ref)
    else:
        add_source(next_ref, source_ref, wavelet_ref, step, 0, side)
        copy_sends(next_ref, *sends, 0)


def w_bare_kernel(index, now_ref, prev_ref, ha_ref, hb_ref, speed_ref, next_ref, *rest):
    sends, work = rest[:2], rest[2:]
    _, side, _ = now_ref.shape
    prepare(work, now_ref, ha_ref, hb_ref, index, band_weights(side))

    def emit(z, block, centre, lap):
        next_ref[z, block, :] = (2.0 * centre - prev_ref[z, block, :]) + speed_ref[z, block, :] * lap

    each_laplacian(work, now_ref, emit)
    copy_sends(next_ref, *sends, 0)


def d_kernel(index, now_ref, prev_ref, ha_ref, hb_ref, speed_ref, perturb_ref, lap_u_ref, bare_ref, count_ref, *rest):
    next_ref, w_ref, *sends = rest[:4]
    work = rest[4:]
    _, side, _ = now_ref.shape
    prepare(work, now_ref, ha_ref, hb_ref, index, band_weights(side))

    def emit(z, block, centre, lap):
        new = ((2.0 * centre - prev_ref[z, block, :]) + speed_ref[z, block, :] * lap) + (
            perturb_ref[z, block, :] * lap_u_ref[z, block, :]
        )
        next_ref[z, block, :] = new
        w_ref[z, block, :] = bare_ref[z, block, :] + count_ref[z, block, :] * new

    each_laplacian(work, now_ref, emit)
    copy_sends(next_ref, *sends, 0)


def dw_kernel(bare, *refs):
    refs = Refs(refs)
    speed_ref, d_ref, d_prev, w_ref, w_prev, perturb_ref, lap_u_ref, count_ref = refs.take(8)
    d_halo, w_halo = refs.take(2), refs.take(2)
    d_local, w_local = refs.take(2)
    outer_ref = refs.take() if bare else None
    d_next, w_next = refs.take(2)
    d_sends, w_sends = refs.take(2), refs.take(2)
    d_halos, w_halos = refs.take(2)
    prepare_halo(d_halos, *d_halo, 0)
    prepare_halo(w_halos, *w_halo, 0, (outer_ref, d_halos) if bare else None)

    def emit_d(z, block, centre, lap):
        d_next[z, block, :] = ((2.0 * centre - d_prev[z, block, :]) + speed_ref[z, block, :] * lap) + (
            perturb_ref[z, block, :] * lap_u_ref[z, block, :]
        )

    def emit_w(z, block, centre, lap):
        w_next[z, block, :] = ((2.0 * centre - w_prev[z, block, :]) + speed_ref[z, block, :] * lap) + (
            count_ref[z, block, :] * d_next[z, block, :]
        )

    each_remainder(d_halos, d_local, d_ref, emit_d)
    copy_sends(d_next, *d_sends, 0)
    each_remainder(w_halos, w_local, w_ref, emit_w)
    copy_sends(w_next, *w_sends, 0)


def last_d_kernel(before, *refs):
    refs = Refs(refs)
    now_ref, prev_ref, ha_ref, hb_ref, speed_ref, perturb_ref, lap_u_ref, cells_ref, rows_hbm = refs.take(9)
    early_ref = refs.take() if before else None
    out_ref, next_ref, record_ref = refs.take(3)
    work = refs.take(3)
    rows_smem, rows_ref, sems, table_sem = refs.take(4)
    fetch = pltpu.make_async_copy(rows_hbm, rows_smem, table_sem)
    fetch.start()
    _, side, _ = now_ref.shape
    prepare(work, now_ref, ha_ref, hb_ref, 0, band_weights(side))

    def emit(z, block, centre, lap):
        next_ref[z, block, :] = ((2.0 * centre - prev_ref[z, block, :]) + speed_ref[z, block, :] * lap) + (
            perturb_ref[z, block, :] * lap_u_ref[z, block, :]
        )

    def finish(part, parts):
        store_out(next_ref, out_ref, sems, part, parts).start()

    each_laplacian(work, now_ref, emit, finish, PARTS)
    fetch.wait()
    if before:
        record_ref[pl.ds(0, before), :] = early_ref[...]
    fields = [now_ref, next_ref] if record_ref.shape[0] > before + 1 else [next_ref]
    gather_records(before, lambda r: rows_smem[0, r], cells_ref, fields, record_ref, rows_ref)
    for part in range(PARTS):
        store_out(next_ref, out_ref, sems, part, PARTS).wait()


def last_w_kernel(*refs):
    refs = Refs(refs)
    now_ref, prev_ref, ha_ref, hb_ref, speed_ref, count_ref, d_next = refs.take(7)
    u_ref, u_prev, lap_u_ref, source_ref, wavelet_hbm = refs.take(5)
    out_ref, u_out = refs.take(2)
    next_ref, u_next = refs.take(2)
    work = refs.take(3)
    wavelet_ref, sems, table_sem = refs.take(3)
    fetch = pltpu.make_async_copy(wavelet_hbm, wavelet_ref, table_sem)
    fetch.start()
    _, side, _ = now_ref.shape
    prepare(work, now_ref, ha_ref, hb_ref, 0, band_weights(side))
    last_step = wavelet_ref.shape[1] - 1

    def emit(z, block, centre, lap):
        speed = speed_ref[z, block, :]
        next_ref[z, block, :] = ((2.0 * centre - prev_ref[z, block, :]) + speed * lap) + (
            count_ref[z, block, :] * d_next[z, block, :]
        )
        u_next[z, block, :] = (2.0 * u_ref[z, block, :] - u_prev[z, block, :]) + speed * lap_u_ref[z, block, :]

    def finish(part, parts):
        size = side // parts
        if part == 0:
            fetch.wait()
        add_source(u_next, source_ref, wavelet_ref, last_step, part * size, size)
        store_out(next_ref, out_ref, sems.at[0], part, parts).start()
        store_out(u_next, u_out, sems.at[1], part, parts).start()

    each_laplacian(work, now_ref, emit, finish, PARTS)
    for part in range(PARTS):
        store_out(next_ref, out_ref, sems.at[0], part, PARTS).wait()
        store_out(u_next, u_out, sems.at[1], part, PARTS).wait()


def stencil_call(body, in_specs, args, outs, kinds, scratch):
    return pl.pallas_call(
        body, out_shape=outs, in_specs=in_specs, out_specs=kinds, scratch_shapes=scratch, compiler_params=params(20)
    )(*args)


def u_call(step, last, wavelet, source, u, u_prev, halo, speed, w, corr, local, aperture, tile_slot, lat_dev, tile_side):
    field = sds(u.shape)
    edge = sds((1, HALO) + u.shape[1:])
    args, specs = [u, *halo, w], [VMEM] * 4
    if not step:
        args[3], specs[3] = in_hbm(w), HBM
    if not last:
        args, specs = args + [source, in_hbm(wavelet), u_prev, speed], specs + [SMEM, HBM, VMEM, VMEM]
    if step:
        args, specs = args + [corr], specs + [VMEM]
    ahead = local is not None
    if ahead:
        args, specs = args + [local], specs + [VMEM]
    n_shot, n_tiles = aperture.shape
    cells = tile_side * tile_side
    capacity = n_tiles // 4
    rows, halos, lanes = work_space(*u.shape[:2])
    scratch = [halos] + ([] if ahead else [rows, lanes]) + [pltpu.SemaphoreType.DMA((3,))]
    if not last:
        scratch += [pltpu.SMEM(wavelet.shape, F32)]
    if not step:
        scratch += [pltpu.VMEM(u.shape, F32)]
    if last:
        args += [in_hbm(aperture), in_hbm(tile_slot)]
        specs += [HBM, HBM]
        outs = [field] + [sds((capacity, u.shape[0], cells))] * n_shot
        scratch = [pltpu.VMEM(u.shape, F32)] + scratch + [
            pltpu.SMEM(aperture.shape, jnp.int32),
            pltpu.SMEM(tile_slot.shape, jnp.int32),
            *tile_scratch(n_shot, capacity, u.shape[0], cells, n_tiles),
        ]
    else:
        outs = [field] * 3 + [edge] * 2
    body = functools.partial(u_kernel, step, last, ahead, (n_shot, lat_dev, tile_side))
    return stencil_call(body, specs, args, outs, [VMEM] * len(outs), scratch)


def w_bare_call(w, w_prev, halo, index, speed):
    field, edge = sds(w.shape), sds((1, HALO) + w.shape[1:])
    args = [w, w_prev, *halo, speed]
    body = functools.partial(w_bare_kernel, index)
    return stencil_call(body, [VMEM] * 5, args, [field, edge, edge], [VMEM] * 3, work_space(*w.shape[:2]))


def d_call(d, d_prev, halo, index, speed, perturb, lap_u, bare, count):
    field, edge = sds(d.shape), sds((1, HALO) + d.shape[1:])
    args = [d, d_prev, *halo, speed, perturb, lap_u, bare, count]
    body = functools.partial(d_kernel, index)
    outs = [field, field, edge, edge]
    return stencil_call(body, [VMEM] * 9, args, outs, [VMEM] * 4, work_space(*d.shape[:2]))


def dw_call(d, d_prev, w, w_prev, d_halo, w_halo, d_local, w_local, speed, perturb, lap_u, count, outer):
    field, edge = sds(d.shape), sds((1, HALO) + d.shape[1:])
    bare = outer is not None
    args = [speed, d, d_prev, w, w_prev, perturb, lap_u, count, *d_halo, *w_halo, d_local, w_local]
    args += [outer] if bare else []
    outs = [field, field] + [edge] * 4
    body = functools.partial(dw_kernel, bare)
    return stencil_call(body, [VMEM] * len(args), args, outs, [VMEM] * 6, [halo_space(d.shape[1])] * 2)


def last_d_call(step, d, d_prev, halo, speed, perturb, lap_u, cells, rows, early):
    before = 0 if early is None else early.shape[0]
    n = cells.shape[1]
    fields = step + 1 - before
    args = [d, d_prev, *halo, speed, perturb, lap_u, cells, rows]
    specs = [VMEM] * 8 + [HBM]
    if before:
        args, specs = args + [early], specs + [VMEM]
    scratch = work_space(*d.shape[:2]) + [
        pltpu.SMEM(cells.shape, jnp.int32),
        pltpu.VMEM((fields, n, d.shape[-1]), F32),
        pltpu.SemaphoreType.DMA((PARTS,)),
        pltpu.SemaphoreType.DMA(()),
    ]
    outs = [sds((1,) + d.shape), sds(d.shape), sds((step + 1, n))]
    body = functools.partial(last_d_kernel, before)
    return stencil_call(body, specs, args, outs, [HBM, VMEM, VMEM], scratch)


def last_w_call(w, w_prev, halo, speed, count, d_next, u, u_prev, lap_u, source, wavelet):
    args = [w, w_prev, *halo, speed, count, d_next, u, u_prev, lap_u, source, in_hbm(wavelet)]
    specs = [VMEM] * 10 + [SMEM, HBM]
    scratch = [pltpu.VMEM(w.shape, F32)] * 2 + work_space(*w.shape[:2]) + [
        pltpu.SMEM(wavelet.shape, F32),
        pltpu.SemaphoreType.DMA((2, PARTS)),
        pltpu.SemaphoreType.DMA(()),
    ]
    outs = [sds((1,) + w.shape)] * 2
    return stencil_call(last_w_kernel, specs, args, outs, [HBM] * 2, scratch)


def count_kernel(cells_ref, count_ref, outer_ref):
    depth, side, _ = count_ref.shape
    local = cells_ref[...] - (lax.axis_index("slab") * depth - HALO) * (side * side)
    n = local.shape[1]
    row_of = jnp.where(local >= 0, quotient(jnp.maximum(local, 0), side), -1)
    lane_of = remainder(jnp.maximum(local, 0), side)
    lanes = lax.broadcasted_iota(jnp.int32, (side, n), 0)
    lane_hot = jnp.where(lanes == lane_of, 1.0, 0.0).astype(jnp.bfloat16)
    for z in range(depth + 2 * HALO):
        row_hot = jnp.where(lanes + z * side == row_of, 1.0, 0.0).astype(jnp.bfloat16)
        plane = lax.dot_general(row_hot, lane_hot, (((1,), (1,)), ((), ())), preferred_element_type=F32)
        if z < HALO:
            outer_ref[0, z] = plane
        elif z < HALO + depth:
            count_ref[z - HALO] = plane
        else:
            outer_ref[1, z - HALO - depth] = plane


def count_call(cells, depth, side):
    return pl.pallas_call(
        count_kernel,
        out_shape=[sds((depth, side, side)), sds((2, HALO, side, side))],
        in_specs=[VMEM],
        out_specs=[VMEM, VMEM],
        compiler_params=params(8),
        name="count",
    )(cells)


def gather_records(before, row_of, cells_ref, fields, out_ref, rows_ref):
    depth, side, _ = fields[0].shape
    n = cells_ref.shape[1]
    total = depth * side * side
    local = cells_ref[...] - lax.axis_index("slab") * total
    mine = (local >= 0) & (local < total)
    lane_of = jnp.where(mine, remainder(jnp.maximum(local, 0), side), -1)
    lanes = lax.broadcasted_iota(jnp.int32, (side, n), 0)
    hit = lanes == lane_of
    flat = [field_ref.reshape(depth * side, side) for field_ref in fields]

    def gather(r, carry):
        row = row_of(r)
        for step, field_ref in enumerate(flat):
            rows_ref[step, pl.ds(r, 1), :] = field_ref[pl.ds(row, 1), :]
        return carry

    lax.fori_loop(0, n, gather, 0, unroll=32)
    for step in range(len(fields)):
        turned = rows_ref[step].T
        out_ref[pl.ds(before + step, 1), :] = jnp.sum(jnp.where(hit, turned, 0.0), axis=0, keepdims=True)


def record_kernel(before, cells_smem, cells_ref, *rest):
    if before:
        early_ref, rest = rest[0], rest[1:]
    *fields, out_ref, table_ref, rows_ref = rest
    if before:
        out_ref[pl.ds(0, before), :] = early_ref[...]
    depth, side, _ = fields[0].shape
    total = depth * side * side
    start = lax.axis_index("slab") * total

    def row_of(r):
        row = quotient(jnp.clip(cells_smem[0, r] - start, 0, total - 1), side)
        table_ref[0, r] = row
        return row

    gather_records(before, row_of, cells_ref, fields, out_ref, rows_ref)


def record_call(cells, early, fields):
    side = fields[0].shape[-1]
    n = cells.shape[1]
    before = 0 if early is None else early.shape[0]
    args = [cells, cells] + ([early] if before else []) + list(fields)
    return pl.pallas_call(
        functools.partial(record_kernel, before),
        out_shape=[sds((before + len(fields), n)), sds(cells.shape, jnp.int32)],
        in_specs=[SMEM] + [VMEM] * (len(args) - 1),
        out_specs=[VMEM, SMEM],
        scratch_shapes=[pltpu.VMEM((len(fields), n, side), F32)],
        compiler_params=params(8),
    )(*args)


def swap_segments(parts, segment):
    count = len(parts)
    lanes = count * segment
    lane = lax.broadcasted_iota(jnp.int32, parts[0].shape, 1)
    parts = list(parts)
    bit = count // 2
    while bit:
        low = lax.rem(lax.div(lane, bit * segment), 2) == 0
        for a in range(count):
            if not a & bit:
                first, second = parts[a], parts[a + bit]
                parts[a] = jnp.where(low, first, pltpu.roll(second, bit * segment, 1))
                parts[a + bit] = jnp.where(low, pltpu.roll(first, lanes - bit * segment, 1), second)
        bit //= 2
    return parts


def partner_of(me, k, count):
    if count & (count - 1) == 0:
        return lax.bitwise_xor(me, k)
    return lax.rem(k - me + count, count)


def round_of(me, other, count):
    if count & (count - 1) == 0:
        return lax.bitwise_xor(me, other)
    return lax.rem(me + other, count)


def pack_kernel(aperture_hbm, slot_hbm, tiles_hbm, *rest):
    *outs, table_ref, aperture_ref, slot_ref, tiles_ref, sems = rest
    pairs = ((aperture_hbm, aperture_ref), (slot_hbm, slot_ref), (tiles_hbm, tiles_ref))
    copies = [pltpu.make_async_copy(a, b, sems.at[i]) for i, (a, b) in enumerate(pairs)]
    for copy in copies:
        copy.start()
    lat_dev = tiles_ref.shape[0]
    n_shot = len(outs)
    capacity = outs[0].shape[0]
    me = lax.axis_index("shot")
    n_tiles = aperture_ref.shape[1]
    copies[0].wait()
    copies[1].wait()

    def shot(s, carry):
        for r in range(capacity):
            table_ref[s * (capacity + 1) + r] = 0
        seen = jnp.int32(0)
        for p in range(n_tiles):
            slot = slot_ref[aperture_ref[s, p]]
            mine = quotient(slot, lat_dev) == me

            @pl.when(mine)
            def _():
                table_ref[s * (capacity + 1) + seen] = remainder(slot, lat_dev)

            seen = seen + mine.astype(jnp.int32)
        table_ref[s * (capacity + 1) + capacity] = seen
        return carry

    lax.fori_loop(0, n_shot, shot, 0)
    copies[2].wait()
    for k in range(n_shot):
        base = partner_of(me, k, n_shot) * (capacity + 1)
        for r in range(capacity):
            outs[k][r] = tiles_ref[table_ref[base + r]]


def pack_call(aperture, tile_slot, model_tiles, capacity):
    n_shot = aperture.shape[0]
    _, depth, cells = model_tiles.shape
    *blocks, table = pl.pallas_call(
        pack_kernel,
        out_shape=[sds((capacity, depth, cells))] * n_shot + [sds((n_shot * (capacity + 1),), jnp.int32)],
        in_specs=[HBM, HBM, HBM],
        out_specs=[VMEM] * n_shot + [SMEM],
        scratch_shapes=[
            pltpu.SMEM(aperture.shape, jnp.int32),
            pltpu.SMEM(tile_slot.shape, jnp.int32),
            pltpu.VMEM(model_tiles.shape, F32),
            pltpu.SemaphoreType.DMA((3,)),
        ],
        compiler_params=params(8),
        name="pack",
    )(in_hbm(aperture), in_hbm(tile_slot), in_hbm(model_tiles))
    return blocks, table


def places(aperture_ref, slot_ref, lat_dev, n_shot, capacity, seen_ref, place_ref):
    me = lax.axis_index("shot")
    for h in range(n_shot):
        seen_ref[h] = 0

    def tile(p, carry):
        holder = quotient(slot_ref[aperture_ref[me, p]], lat_dev)
        rank = seen_ref[holder]
        seen_ref[holder] = rank + 1
        place_ref[p] = round_of(me, holder, n_shot) * capacity + rank
        return carry

    lax.fori_loop(0, aperture_ref.shape[1], tile, 0)


def perturb_kernel(lat_dev, tile_side, aperture_hbm, slot_hbm, *rest):
    *blocks, out_ref, tiles_ref, seen_ref, place_ref, aperture_ref, slot_ref, sems = rest
    copies = [
        pltpu.make_async_copy(aperture_hbm, aperture_ref, sems.at[0]),
        pltpu.make_async_copy(slot_hbm, slot_ref, sems.at[1]),
    ]
    for copy in copies:
        copy.start()
    n_shot = len(blocks)
    capacity, depth, cells = blocks[0].shape
    side = out_ref.shape[1]
    across = side // tile_side
    flat_ref = out_ref.reshape(depth * side, side)
    for k in range(n_shot):
        tiles_ref[pl.ds(k * capacity, capacity)] = blocks[k][...]
    for copy in copies:
        copy.wait()
    places(aperture_ref, slot_ref, lat_dev, n_shot, capacity, seen_ref, place_ref)

    def tile_row(i, carry):
        for high in range(cells // side):
            parts = [tiles_ref[place_ref[i * across + j], :, pl.ds(high * side, side)] for j in range(across)]
            for low, part in enumerate(swap_segments(parts, tile_side)):
                flat_ref[pl.ds(i * tile_side + high * across + low, depth, stride=side), :] = part
        return carry

    lax.fori_loop(0, across, tile_row, 0)


def pack_back(lat_dev, tile_side, aperture_ref, slot_ref, corr_ref, blocks, tiles_ref, seen_ref, place_ref):
    n_shot = len(blocks)
    capacity, depth, cells = blocks[0].shape
    side = corr_ref.shape[1]
    across = side // tile_side
    flat_ref = corr_ref.reshape(depth * side, side)
    places(aperture_ref, slot_ref, lat_dev, n_shot, capacity, seen_ref, place_ref)

    def tile_row(i, carry):
        for high in range(cells // side):
            parts = [
                flat_ref[pl.ds(i * tile_side + high * across + low, depth, stride=side), :] for low in range(across)
            ]
            for j, part in enumerate(swap_segments(parts, tile_side)):
                tiles_ref[place_ref[i * across + j], :, pl.ds(high * side, side)] = part
        return carry

    lax.fori_loop(0, across, tile_row, 0)
    for k in range(n_shot):
        blocks[k][...] = tiles_ref[pl.ds(k * capacity, capacity)]


def tile_scratch(n_shot, capacity, depth, cells, n_tiles):
    return [
        pltpu.VMEM((n_shot * capacity, depth, cells), F32),
        pltpu.SMEM((n_shot,), jnp.int32),
        pltpu.SMEM((n_tiles,), jnp.int32),
    ]


def perturb_call(aperture, tile_slot, blocks, side, lat_dev, tile_side):
    capacity, depth, cells = blocks[0].shape
    return pl.pallas_call(
        functools.partial(perturb_kernel, lat_dev, tile_side),
        out_shape=sds((depth, side, side)),
        in_specs=[HBM, HBM] + [VMEM] * len(blocks),
        out_specs=VMEM,
        scratch_shapes=[
            *tile_scratch(len(blocks), capacity, depth, cells, aperture.shape[1]),
            pltpu.SMEM(aperture.shape, jnp.int32),
            pltpu.SMEM(tile_slot.shape, jnp.int32),
            pltpu.SemaphoreType.DMA((2,)),
        ],
        compiler_params=params(8),
        name="perturb",
    )(in_hbm(aperture), in_hbm(tile_slot), *blocks)


def finish_kernel(n_shot, table_hbm, *refs):
    refs = Refs(refs)
    blocks = refs.take(n_shot)
    parts = refs.refs[:-4]
    sum_ref, record_ref, table_ref, sem = refs.refs[-4:]
    fetch = pltpu.make_async_copy(table_hbm, table_ref, sem)
    fetch.start()
    capacity = blocks[0].shape[0]
    total = parts[0][...]
    for part in parts[1:]:
        total = total + part[...]
    for step in range(total.shape[0]):
        record_ref[step] = total[step : step + 1]
    sum_ref[...] = jnp.zeros(sum_ref.shape, F32)
    fetch.wait()
    for k in range(n_shot):
        base = partner_of(lax.axis_index("shot"), k, n_shot) * (capacity + 1)
        for r in range(capacity):

            @pl.when(r < table_ref[base + capacity])
            def _():
                slot = table_ref[base + r]
                sum_ref[slot] = sum_ref[slot] + blocks[k][r]


def finish_call(table, blocks, parts, lat_dev):
    depth, cells = blocks[0].shape[1:]
    steps, n = parts[0].shape
    return pl.pallas_call(
        functools.partial(finish_kernel, len(blocks)),
        out_shape=[sds((lat_dev, depth, cells)), sds((steps, 1, n))],
        in_specs=[HBM] + [VMEM] * (len(blocks) + len(parts)),
        out_specs=[VMEM, VMEM],
        scratch_shapes=[pltpu.SMEM(table.shape, jnp.int32), pltpu.SemaphoreType.DMA(())],
        compiler_params=params(8),
        name="finish",
    )(table, *blocks, *parts)


def swap(edges):
    count = lax.axis_size("slab")
    shots = lax.axis_size("shot")
    got = []
    for start, edge in enumerate(edges):
        pairs = {}
        for shot in range(shots):
            for i in range(count):
                other = i + 1 if (i - start) % 2 == 0 else i - 1
                if 0 <= other < count:
                    pairs[shot * count + i] = shot * count + other
                elif shots % 2 == 0:
                    pairs[shot * count + i] = (shot ^ 1) * count + i
        got.append(lax.ppermute(edge, ("shot", "slab"), sorted(pairs.items())))
    return tuple(got)


def edges_kernel(n, *refs):
    fields, outs, sems = refs[:n], refs[n:-1], refs[-1]
    depth = fields[0].shape[1]
    low = jnp.where(place()[0] == 1, 0, depth - HALO)
    copies = []
    for out_ref, at in zip(outs, (low, depth - HALO - low)):
        for index, field_ref in enumerate(fields):
            copies.append(
                pltpu.make_async_copy(field_ref.at[0, pl.ds(at, HALO)], out_ref.at[index], sems.at[len(copies)])
            )
    for copy in copies:
        copy.start()
    for copy in copies:
        copy.wait()


def first_edges(fields):
    n = len(fields)
    edge = sds((n, HALO) + fields[0].shape[2:])
    return pl.pallas_call(
        functools.partial(edges_kernel, n),
        out_shape=[edge, edge],
        in_specs=[HBM] * n,
        out_specs=[VMEM, VMEM],
        scratch_shapes=[pltpu.SemaphoreType.DMA((2 * n,))],
        compiler_params=params(8),
    )(*map(in_hbm, fields))


def partners():
    count = lax.axis_size("shot")
    if count & (count - 1) == 0:
        return [[s ^ k for s in range(count)] for k in range(count)]
    return [[(k - s) % count for s in range(count)] for k in range(count)]


def rounds(count):
    return sorted(range(count), key=lambda k: (-(k >> 1).bit_count(), k))


def exchange(blocks):
    got = [None] * len(blocks)
    for k in rounds(len(blocks)):
        block, to = blocks[k], partners()[k]
        moves = [(s, t) for s, t in enumerate(to) if s != t]
        kept = [s for s, t in enumerate(to) if s == t]
        if kept and moves:
            moves = moves + [(s, s) for s in kept]
        got[k] = lax.ppermute(block, "shot", moves) if moves else block
    return got


def slab_parts(part):
    count = lax.axis_size("slab")
    parts = [part]
    for k in range(count - 1, 0, -1):
        to = [s ^ k for s in range(count)] if count & (count - 1) == 0 else [(s + k) % count for s in range(count)]
        parts.append(lax.ppermute(part, "slab", list(enumerate(to))))
    return parts


def per_device(
    model_tiles,
    background,
    u_prev,
    u_now,
    du_prev,
    du_now,
    w_prev,
    w_now,
    wavelet,
    source_cell,
    receiver_cells,
    aperture,
    tile_slot,
):
    lat_dev, depth, tile_cells = model_tiles.shape
    side = background.shape[-1]
    tile_side = math.isqrt(tile_cells)
    capacity = aperture.shape[1] // 4
    steps = wavelet.shape[1]
    speed = background[0]
    u, d, w = u_now[0], du_now[0], w_now[0]
    up, dp, wp = u_prev[0], du_prev[0], w_prev[0]

    tiling = (aperture, tile_slot, lat_dev, tile_side)
    u_halo = swap(first_edges([u_now]))
    dw_halo = swap(first_edges([du_now, w_now]))
    outgoing, table = pack_call(aperture, tile_slot, model_tiles, capacity)
    incoming = exchange(outgoing)
    count, outer = count_call(receiver_cells, depth, side)
    perturb = perturb_call(aperture, tile_slot, incoming, side, lat_dev, tile_side)

    u_next, lap, corr, *edges = u_call(0, False, wavelet, source_cell, u, up, u_halo, speed, w_now, None, None, *tiling)
    u_halo = swap(edges)
    bare, *edges = w_bare_call(w, wp, dw_halo, 1, speed)
    w_halo = swap(edges)
    d_next, w_next, *edges = d_call(d, dp, dw_halo, 0, speed, perturb, lap, bare, count)
    d_halo = swap(edges)
    traces = u_local = None
    for step in range(1, steps - 1):
        traces, receiver_rows = record_call(receiver_cells, traces, [d_next])
        u, up, d, dp, w, wp = u_next, u, d_next, d, w_next, w
        u_next, lap, corr, *edges = u_call(
            step, False, wavelet, source_cell, u, up, u_halo, speed, w, corr, u_local, *tiling
        )
        u_halo = swap(edges)
        u_local, d_local, w_local = ahead_call([u_next, d, w])
        d_next, w_next, *edges = dw_call(
            d, dp, w, wp, d_halo, w_halo, d_local, w_local, speed, perturb, lap, count, outer if step == 1 else None
        )
        d_halo = swap(edges[:2])
        w_halo = swap(edges[2:])
    u, up, d, dp, w, wp = u_next, u, d_next, d, w_next, w
    step = steps - 1
    lap, *returning = u_call(step, True, wavelet, source_cell, u, up, u_halo, speed, w, corr, u_local, *tiling)
    arrived = exchange(returning)
    d_final, d_next, traces = last_d_call(
        step, d, dp, d_halo, speed, perturb, lap, receiver_cells, receiver_rows, traces
    )
    parts = slab_parts(traces)
    w_final, u_final = last_w_call(w, wp, w_halo, speed, count, d_next, u, up, lap, source_cell, wavelet)
    sensitivity, traces = finish_call(table, arrived, parts, lat_dev)
    return (sensitivity, u_final, d_final, w_final, jnp.transpose(traces, (1, 0, 2)))


def solution(mesh):
    field = P("shot", "slab", None, None)
    tiles = P("shot", "slab", None)
    in_specs = (tiles,) + (field,) * 7 + (P("shot", None), P("shot"), P("shot", None), P(), P())
    out_specs = (tiles, field, field, field, P("shot", None, None))


    return jax.shard_map(per_device, mesh=mesh, in_specs=in_specs, out_specs=out_specs, check_vma=False)
```

```python
import functools
import math

import jax
import jax.numpy as jnp
from jax import lax
from jax.experimental import pallas as pl
from jax.experimental.pallas import tpu as pltpu
from jax.sharding import PartitionSpec as P


COEFFS = (-205.0 / 72.0, 8.0 / 5.0, -1.0 / 5.0, 8.0 / 315.0, -1.0 / 560.0)
HALO = len(COEFFS) - 1
SUB = 8
F32 = jnp.float32
VMEM = pl.BlockSpec(memory_space=pltpu.VMEM)
SMEM = pl.BlockSpec(memory_space=pltpu.SMEM)
HBM = pl.BlockSpec(memory_space=pltpu.HBM)


def params(mib):
    return pltpu.CompilerParams(vmem_limit_bytes=mib * 1024 * 1024)


def in_hbm(x):
    return pltpu.with_memory_space_constraint(x, pltpu.HBM)


def sds(shape, dtype=F32):
    return jax.ShapeDtypeStruct(shape, dtype)


def place():
    slab, count = lax.axis_index("slab"), lax.axis_size("slab")
    odd = lax.bitwise_and(slab, 1)
    above, below = slab < count - 1, slab > 0
    is_odd = odd == 1
    return odd, (is_odd & below) | (~is_odd & above), (is_odd & above) | (~is_odd & below)


def quotient(x, m):
    return lax.shift_right_logical(x, m.bit_length() - 1) if m & (m - 1) == 0 else lax.div(x, m)


def remainder(x, m):
    return lax.bitwise_and(x, m - 1) if m & (m - 1) == 0 else lax.rem(x, m)


SCALE = 5040.0
PARTS = 4


def band_weights(side):
    i = lax.broadcasted_iota(jnp.int32, (2 * side, 2 * side), 0)
    j = lax.broadcasted_iota(jnp.int32, (2 * side, 2 * side), 1)
    far = jnp.where((i < side) == (j < side), jnp.abs(i - j), 0)
    out = jnp.zeros((2 * side, 2 * side), F32)
    for k in range(1, HALO + 1):
        out = jnp.where(far == k, round(COEFFS[k] * SCALE) * 1.0, out)
    out = out.astype(jnp.bfloat16)
    return jnp.concatenate([out, out, out], axis=0)


def split3(x):
    high = x.astype(jnp.bfloat16)
    rest = x - high.astype(F32)
    mid = rest.astype(jnp.bfloat16)
    low = (rest - mid.astype(F32)).astype(jnp.bfloat16)
    return high, mid, low


def prepare_local(rows_ref, lanes_ref, now_ref, weights):
    depth, side, _ = now_ref.shape
    zeros = jnp.zeros((SUB, side), F32)
    half = depth // 2
    parts = []
    for low, high in zip(split3(now_ref[pl.ds(0, half)]), split3(now_ref[pl.ds(half, half)])):
        parts += [low.reshape(half * side, side), high.reshape(half * side, side)]
    lanes = jnp.dot(jnp.concatenate(parts, axis=1), weights, preferred_element_type=F32)
    lanes_ref[pl.ds(0, half)] = lanes[:, :side].reshape(half, side, side)
    lanes_ref[pl.ds(half, half)] = lanes[:, side:].reshape(half, side, side)
    for z in range(depth):
        rows_ref[z, pl.ds(0, SUB), :] = zeros
        rows_ref[z, pl.ds(SUB + side, SUB), :] = zeros
        rows_ref[z, pl.ds(SUB, side), :] = now_ref[z]


def prepare_halo(halo_ref, first_ref, second_ref, index, inject=None):
    odd, has_first, has_second = place()

    def halo(z, carry):
        halo_ref[1 - odd, z] = jnp.where(has_first, first_ref[index, z], 0.0)
        halo_ref[odd, z] = jnp.where(has_second, second_ref[index, z], 0.0)
        return carry

    lax.fori_loop(0, HALO, halo, 0)
    if inject:
        outer_ref, other_ref = inject
        for end in range(2):
            for z in range(HALO):
                halo_ref[end, z] = halo_ref[end, z] + outer_ref[end, z] * other_ref[end, z]


def prepare(work, now_ref, first_ref, second_ref, index, weights):
    rows_ref, halo_ref, lanes_ref = work
    prepare_local(rows_ref, lanes_ref, now_ref, weights)
    prepare_halo(halo_ref, first_ref, second_ref, index)


def each_laplacian(work, now_ref, emit, finish=None, parts=1):
    rows_ref, halo_ref, lanes_ref = work
    depth, side, _ = now_ref.shape

    def block(g, carry):
        start = pl.multiple_of(g * SUB, SUB)
        rows = pl.ds(start, SUB)
        column = [halo_ref[0, z, rows, :] for z in range(HALO)]
        column += [now_ref[z, rows, :] for z in range(depth)]
        column += [halo_ref[1, z, rows, :] for z in range(HALO)]
        for z in range(depth):
            centre = column[HALO + z]
            total = (3.0 * COEFFS[0]) * centre + (1.0 / SCALE) * lanes_ref[z, rows, :]
            for k in range(1, HALO + 1):
                ring = (column[HALO + z + k] + column[HALO + z - k]) + (
                    rows_ref[z, pl.ds(start + (SUB + k), SUB), :] + rows_ref[z, pl.ds(start + (SUB - k), SUB), :]
                )
                total = total + COEFFS[k] * ring
            emit(z, rows, centre, total)
        return carry

    blocks = side // SUB // parts
    for part in range(parts):
        lax.fori_loop(part * blocks, (part + 1) * blocks, block, 0)
        if finish:
            finish(part, parts)


def halo_space(side):
    return pltpu.VMEM((2, HALO, side, side), F32)


def work_space(depth, side):
    return [
        pltpu.VMEM((depth, side + 2 * SUB, side), F32),
        halo_space(side),
        pltpu.VMEM((depth, side, side), F32),
    ]


def ahead_kernel(n, *refs):
    fields, outs, (rows_ref, lanes_ref) = refs[:n], refs[n:-2], refs[-2:]
    depth, side, _ = fields[0].shape
    weights = band_weights(side)
    for now_ref, out_ref in zip(fields, outs):
        prepare_local(rows_ref, lanes_ref, now_ref, weights)

        def block(g, carry, now_ref=now_ref, out_ref=out_ref):
            start = pl.multiple_of(g * SUB, SUB)
            rows = pl.ds(start, SUB)
            column = [now_ref[z, rows, :] for z in range(depth)]
            for z in range(depth):
                total = (3.0 * COEFFS[0]) * column[z] + (1.0 / SCALE) * lanes_ref[z, rows, :]
                for k in range(1, HALO + 1):
                    ring = (
                        rows_ref[z, pl.ds(start + (SUB + k), SUB), :] + rows_ref[z, pl.ds(start + (SUB - k), SUB), :]
                    )
                    if z + k < depth:
                        ring = ring + column[z + k]
                    if z - k >= 0:
                        ring = ring + column[z - k]
                    total = total + COEFFS[k] * ring
                out_ref[z, rows, :] = total
            return carry

        lax.fori_loop(0, side // SUB, block, 0)


def ahead_call(fields):
    depth, side, _ = fields[0].shape
    outs = [sds((depth, side, side))] * len(fields)
    rows, _, lanes = work_space(depth, side)
    return pl.pallas_call(
        functools.partial(ahead_kernel, len(fields)),
        out_shape=outs,
        in_specs=[VMEM] * len(fields),
        out_specs=[VMEM] * len(outs),
        scratch_shapes=[rows, lanes],
        compiler_params=params(16),
    )(*fields)


def each_remainder(halo_ref, local_ref, now_ref, emit):
    depth, side, _ = now_ref.shape

    def block(g, carry):
        rows = pl.ds(pl.multiple_of(g * SUB, SUB), SUB)
        below = [halo_ref[0, z, rows, :] for z in range(HALO)]
        above = [halo_ref[1, z, rows, :] for z in range(HALO)]
        for z in range(depth):
            total = local_ref[z, rows, :]
            for k in range(1, HALO + 1):
                if z - k < 0:
                    total = total + COEFFS[k] * below[HALO + z - k]
                if z + k >= depth:
                    total = total + COEFFS[k] * above[z + k - depth]
            emit(z, rows, now_ref[z, rows, :], total)
        return carry

    lax.fori_loop(0, side // SUB, block, 0)


def copy_sends(next_ref, first_ref, second_ref, index):
    depth = next_ref.shape[0]
    odd = place()[0] == 1
    first = jnp.where(odd, 0, depth - HALO)
    second = jnp.where(odd, depth - HALO, 0)
    for z in range(HALO):
        first_ref[index, z] = next_ref[first + z]
        second_ref[index, z] = next_ref[second + z]


def store_out(next_ref, out_ref, sems, step, steps):
    rows = pl.ds(step * (next_ref.shape[1] // steps), next_ref.shape[1] // steps)
    return pltpu.make_async_copy(next_ref.at[:, rows], out_ref.at[0, :, rows], sems.at[step])


def add_source(next_ref, source_ref, wavelet_ref, step, first, rows):
    depth, side, _ = next_ref.shape
    local = source_ref[0] - lax.axis_index("slab") * (depth * side * side)
    mine = (local >= 0) & (local < depth * side * side)
    cell = jnp.where(mine, local, 0)
    z = quotient(cell, side * side)
    x = remainder(quotient(cell, side), side)
    lane = lax.broadcasted_iota(jnp.int32, (1, side), 1)

    @pl.when(mine & (x >= first) & (x < first + rows))
    def _():
        add = jnp.where(lane == remainder(cell, side), wavelet_ref[0, step], 0.0)
        next_ref[z, pl.ds(x, 1), :] = next_ref[z, pl.ds(x, 1), :] + add


class Refs:
    def __init__(self, refs):
        self.refs = list(refs)

    def take(self, n=None):
        if n is None:
            return self.refs.pop(0)
        return [self.refs.pop(0) for _ in range(n)]


def u_kernel(step, last, ahead, tiles, *refs):
    refs = Refs(refs)
    now_ref, ha_ref, hb_ref, w_in = refs.take(4)
    if not last:
        source_ref, wavelet_hbm, prev_ref, speed_ref = refs.take(4)
    corr_in = refs.take() if step else None
    local_ref = refs.take() if ahead else None
    place_row = refs.take() if last else None
    if last:
        lap_ref = refs.take()
        blocks = refs.take(tiles[0])
        corr_ref = refs.take()
    else:
        next_ref, lap_ref, corr_ref = refs.take(3)
        sends = refs.take(2)
    halo_ref = refs.take()
    if not ahead:
        rows_ref, lanes_ref = refs.take(2)
    own_sems = refs.take()
    copies, late = [], []
    if not last:
        wavelet_ref = refs.take()
        late.append(pltpu.make_async_copy(wavelet_hbm, wavelet_ref, own_sems.at[0]))
    w_ref = w_in
    if not step:
        w_ref = refs.take()
        half = w_ref.shape[0] // 2
        for i in range(2):
            part = pl.ds(i * half, half)
            copies.append(pltpu.make_async_copy(w_in.at[0, part], w_ref.at[part], own_sems.at[1 + i]))
    if last:
        tiles_ref, place_ref = refs.take(2)
    for copy in copies + late:
        copy.start()
    _, side, _ = now_ref.shape
    if not ahead:
        prepare_local(rows_ref, lanes_ref, now_ref, band_weights(side))
    prepare_halo(halo_ref, ha_ref, hb_ref, 0)
    for copy in copies:
        copy.wait()

    def emit(z, block, centre, lap):
        lap_ref[z, block, :] = lap
        part = lap * w_ref[z, block, :]
        corr_ref[z, block, :] = corr_in[z, block, :] + part if step else part
        if not last:
            next_ref[z, block, :] = (2.0 * centre - prev_ref[z, block, :]) + speed_ref[z, block, :] * lap

    if ahead:
        each_remainder(halo_ref, local_ref, now_ref, emit)
    else:
        each_laplacian((rows_ref, halo_ref, lanes_ref), now_ref, emit)
    for copy in late:
        copy.wait()
    if last:
        pack_back(tiles[1], place_row, corr_ref, blocks, tiles_ref, place_ref)
    else:
        add_source(next_ref, source_ref, wavelet_ref, step, 0, side)
        copy_sends(next_ref, *sends, 0)


def w_bare_kernel(index, now_ref, prev_ref, ha_ref, hb_ref, speed_ref, next_ref, *rest):
    sends, work = rest[:2], rest[2:]
    _, side, _ = now_ref.shape
    prepare(work, now_ref, ha_ref, hb_ref, index, band_weights(side))

    def emit(z, block, centre, lap):
        next_ref[z, block, :] = (2.0 * centre - prev_ref[z, block, :]) + speed_ref[z, block, :] * lap

    each_laplacian(work, now_ref, emit)
    copy_sends(next_ref, *sends, 0)


def d_kernel(index, now_ref, prev_ref, ha_ref, hb_ref, speed_ref, perturb_ref, lap_u_ref, bare_ref, count_ref, *rest):
    next_ref, w_ref, *sends = rest[:4]
    work = rest[4:]
    _, side, _ = now_ref.shape
    prepare(work, now_ref, ha_ref, hb_ref, index, band_weights(side))

    def emit(z, block, centre, lap):
        new = ((2.0 * centre - prev_ref[z, block, :]) + speed_ref[z, block, :] * lap) + (
            perturb_ref[z, block, :] * lap_u_ref[z, block, :]
        )
        next_ref[z, block, :] = new
        w_ref[z, block, :] = bare_ref[z, block, :] + count_ref[z, block, :] * new

    each_laplacian(work, now_ref, emit)
    copy_sends(next_ref, *sends, 0)


def dw_kernel(bare, *refs):
    refs = Refs(refs)
    speed_ref, d_ref, d_prev, w_ref, w_prev, perturb_ref, lap_u_ref, count_ref = refs.take(8)
    d_halo, w_halo = refs.take(2), refs.take(2)
    d_local, w_local = refs.take(2)
    outer_ref = refs.take() if bare else None
    d_next, w_next = refs.take(2)
    d_sends, w_sends = refs.take(2), refs.take(2)
    d_halos, w_halos = refs.take(2)
    prepare_halo(d_halos, *d_halo, 0)
    prepare_halo(w_halos, *w_halo, 0, (outer_ref, d_halos) if bare else None)

    def emit_d(z, block, centre, lap):
        d_next[z, block, :] = ((2.0 * centre - d_prev[z, block, :]) + speed_ref[z, block, :] * lap) + (
            perturb_ref[z, block, :] * lap_u_ref[z, block, :]
        )

    def emit_w(z, block, centre, lap):
        w_next[z, block, :] = ((2.0 * centre - w_prev[z, block, :]) + speed_ref[z, block, :] * lap) + (
            count_ref[z, block, :] * d_next[z, block, :]
        )

    each_remainder(d_halos, d_local, d_ref, emit_d)
    copy_sends(d_next, *d_sends, 0)
    each_remainder(w_halos, w_local, w_ref, emit_w)
    copy_sends(w_next, *w_sends, 0)


def last_d_kernel(before, *refs):
    refs = Refs(refs)
    now_ref, prev_ref, ha_ref, hb_ref, speed_ref, perturb_ref, lap_u_ref, cells_ref, rows_hbm = refs.take(9)
    early_ref = refs.take() if before else None
    out_ref, next_ref, record_ref = refs.take(3)
    work = refs.take(3)
    rows_smem, rows_ref, sems, table_sem = refs.take(4)
    fetch = pltpu.make_async_copy(rows_hbm, rows_smem, table_sem)
    fetch.start()
    _, side, _ = now_ref.shape
    prepare(work, now_ref, ha_ref, hb_ref, 0, band_weights(side))

    def emit(z, block, centre, lap):
        next_ref[z, block, :] = ((2.0 * centre - prev_ref[z, block, :]) + speed_ref[z, block, :] * lap) + (
            perturb_ref[z, block, :] * lap_u_ref[z, block, :]
        )

    def finish(part, parts):
        store_out(next_ref, out_ref, sems, part, parts).start()

    each_laplacian(work, now_ref, emit, finish, PARTS)
    fetch.wait()
    if before:
        record_ref[pl.ds(0, before), :] = early_ref[...]
    fields = [now_ref, next_ref] if record_ref.shape[0] > before + 1 else [next_ref]
    gather_records(before, lambda r: rows_smem[0, r], cells_ref, fields, record_ref, rows_ref)
    for part in range(PARTS):
        store_out(next_ref, out_ref, sems, part, PARTS).wait()


def last_w_kernel(*refs):
    refs = Refs(refs)
    now_ref, prev_ref, ha_ref, hb_ref, speed_ref, count_ref, d_next = refs.take(7)
    u_ref, u_prev, lap_u_ref, source_ref, wavelet_hbm = refs.take(5)
    out_ref, u_out = refs.take(2)
    next_ref, u_next = refs.take(2)
    work = refs.take(3)
    wavelet_ref, sems, table_sem = refs.take(3)
    fetch = pltpu.make_async_copy(wavelet_hbm, wavelet_ref, table_sem)
    fetch.start()
    _, side, _ = now_ref.shape
    prepare(work, now_ref, ha_ref, hb_ref, 0, band_weights(side))
    last_step = wavelet_ref.shape[1] - 1

    def emit(z, block, centre, lap):
        speed = speed_ref[z, block, :]
        next_ref[z, block, :] = ((2.0 * centre - prev_ref[z, block, :]) + speed * lap) + (
            count_ref[z, block, :] * d_next[z, block, :]
        )
        u_next[z, block, :] = (2.0 * u_ref[z, block, :] - u_prev[z, block, :]) + speed * lap_u_ref[z, block, :]

    def finish(part, parts):
        size = side // parts
        if part == 0:
            fetch.wait()
        add_source(u_next, source_ref, wavelet_ref, last_step, part * size, size)
        store_out(next_ref, out_ref, sems.at[0], part, parts).start()
        store_out(u_next, u_out, sems.at[1], part, parts).start()

    each_laplacian(work, now_ref, emit, finish, PARTS)
    for part in range(PARTS):
        store_out(next_ref, out_ref, sems.at[0], part, PARTS).wait()
        store_out(u_next, u_out, sems.at[1], part, PARTS).wait()


def stencil_call(body, in_specs, args, outs, kinds, scratch):
    return pl.pallas_call(
        body, out_shape=outs, in_specs=in_specs, out_specs=kinds, scratch_shapes=scratch, compiler_params=params(20)
    )(*args)


def u_call(step, last, wavelet, source, u, u_prev, halo, speed, w, corr, local, place, n_shot, n_tiles, tile_side):
    field = sds(u.shape)
    edge = sds((1, HALO) + u.shape[1:])
    args, specs = [u, *halo, w], [VMEM] * 4
    if not step:
        args[3], specs[3] = in_hbm(w), HBM
    if not last:
        args, specs = args + [source, in_hbm(wavelet), u_prev, speed], specs + [SMEM, HBM, VMEM, VMEM]
    if step:
        args, specs = args + [corr], specs + [VMEM]
    ahead = local is not None
    if ahead:
        args, specs = args + [local], specs + [VMEM]
    cells = tile_side * tile_side
    capacity = n_tiles // 4
    rows, halos, lanes = work_space(*u.shape[:2])
    scratch = [halos] + ([] if ahead else [rows, lanes]) + [pltpu.SemaphoreType.DMA((3,))]
    if not last:
        scratch += [pltpu.SMEM(wavelet.shape, F32)]
    if not step:
        scratch += [pltpu.VMEM(u.shape, F32)]
    if last:
        args, specs = args + [place], specs + [VMEM]
        outs = [field] + [sds((capacity, u.shape[0], cells))] * n_shot
        scratch = [pltpu.VMEM(u.shape, F32)] + scratch + tile_scratch(n_shot, capacity, u.shape[0], cells, n_tiles)
    else:
        outs = [field] * 3 + [edge] * 2
    body = functools.partial(u_kernel, step, last, ahead, (n_shot, tile_side))
    return stencil_call(body, specs, args, outs, [VMEM] * len(outs), scratch)


def w_bare_call(w, w_prev, halo, index, speed):
    field, edge = sds(w.shape), sds((1, HALO) + w.shape[1:])
    args = [w, w_prev, *halo, speed]
    body = functools.partial(w_bare_kernel, index)
    return stencil_call(body, [VMEM] * 5, args, [field, edge, edge], [VMEM] * 3, work_space(*w.shape[:2]))


def d_call(d, d_prev, halo, index, speed, perturb, lap_u, bare, count):
    field, edge = sds(d.shape), sds((1, HALO) + d.shape[1:])
    args = [d, d_prev, *halo, speed, perturb, lap_u, bare, count]
    body = functools.partial(d_kernel, index)
    outs = [field, field, edge, edge]
    return stencil_call(body, [VMEM] * 9, args, outs, [VMEM] * 4, work_space(*d.shape[:2]))


def dw_call(d, d_prev, w, w_prev, d_halo, w_halo, d_local, w_local, speed, perturb, lap_u, count, outer):
    field, edge = sds(d.shape), sds((1, HALO) + d.shape[1:])
    bare = outer is not None
    args = [speed, d, d_prev, w, w_prev, perturb, lap_u, count, *d_halo, *w_halo, d_local, w_local]
    args += [outer] if bare else []
    outs = [field, field] + [edge] * 4
    body = functools.partial(dw_kernel, bare)
    return stencil_call(body, [VMEM] * len(args), args, outs, [VMEM] * 6, [halo_space(d.shape[1])] * 2)


def last_d_call(step, d, d_prev, halo, speed, perturb, lap_u, cells, rows, early):
    before = 0 if early is None else early.shape[0]
    n = cells.shape[1]
    fields = step + 1 - before
    args = [d, d_prev, *halo, speed, perturb, lap_u, cells, rows]
    specs = [VMEM] * 8 + [HBM]
    if before:
        args, specs = args + [early], specs + [VMEM]
    scratch = work_space(*d.shape[:2]) + [
        pltpu.SMEM(cells.shape, jnp.int32),
        pltpu.VMEM((fields, n, d.shape[-1]), F32),
        pltpu.SemaphoreType.DMA((PARTS,)),
        pltpu.SemaphoreType.DMA(()),
    ]
    outs = [sds((1,) + d.shape), sds(d.shape), sds((step + 1, n))]
    body = functools.partial(last_d_kernel, before)
    return stencil_call(body, specs, args, outs, [HBM, VMEM, VMEM], scratch)


def last_w_call(w, w_prev, halo, speed, count, d_next, u, u_prev, lap_u, source, wavelet):
    args = [w, w_prev, *halo, speed, count, d_next, u, u_prev, lap_u, source, in_hbm(wavelet)]
    specs = [VMEM] * 10 + [SMEM, HBM]
    scratch = [pltpu.VMEM(w.shape, F32)] * 2 + work_space(*w.shape[:2]) + [
        pltpu.SMEM(wavelet.shape, F32),
        pltpu.SemaphoreType.DMA((2, PARTS)),
        pltpu.SemaphoreType.DMA(()),
    ]
    outs = [sds((1,) + w.shape)] * 2
    return stencil_call(last_w_kernel, specs, args, outs, [HBM] * 2, scratch)


def count_kernel(cells_ref, count_ref, outer_ref):
    depth, side, _ = count_ref.shape
    local = cells_ref[...] - (lax.axis_index("slab") * depth - HALO) * (side * side)
    n = local.shape[1]
    row_of = jnp.where(local >= 0, quotient(jnp.maximum(local, 0), side), -1)
    lane_of = remainder(jnp.maximum(local, 0), side)
    lanes = lax.broadcasted_iota(jnp.int32, (side, n), 0)
    lane_hot = jnp.where(lanes == lane_of, 1.0, 0.0).astype(jnp.bfloat16)
    for z in range(depth + 2 * HALO):
        row_hot = jnp.where(lanes + z * side == row_of, 1.0, 0.0).astype(jnp.bfloat16)
        plane = lax.dot_general(row_hot, lane_hot, (((1,), (1,)), ((), ())), preferred_element_type=F32)
        if z < HALO:
            outer_ref[0, z] = plane
        elif z < HALO + depth:
            count_ref[z - HALO] = plane
        else:
            outer_ref[1, z - HALO - depth] = plane


def count_call(cells, depth, side):
    return pl.pallas_call(
        count_kernel,
        out_shape=[sds((depth, side, side)), sds((2, HALO, side, side))],
        in_specs=[VMEM],
        out_specs=[VMEM, VMEM],
        compiler_params=params(8),
        name="count",
    )(cells)


def gather_records(before, row_of, cells_ref, fields, out_ref, rows_ref):
    depth, side, _ = fields[0].shape
    n = cells_ref.shape[1]
    total = depth * side * side
    local = cells_ref[...] - lax.axis_index("slab") * total
    mine = (local >= 0) & (local < total)
    lane_of = jnp.where(mine, remainder(jnp.maximum(local, 0), side), -1)
    lanes = lax.broadcasted_iota(jnp.int32, (side, n), 0)
    hit = lanes == lane_of
    flat = [field_ref.reshape(depth * side, side) for field_ref in fields]

    def gather(r, carry):
        row = row_of(r)
        for step, field_ref in enumerate(flat):
            rows_ref[step, pl.ds(r, 1), :] = field_ref[pl.ds(row, 1), :]
        return carry

    lax.fori_loop(0, n, gather, 0, unroll=32)
    for step in range(len(fields)):
        turned = rows_ref[step].T
        out_ref[pl.ds(before + step, 1), :] = jnp.sum(jnp.where(hit, turned, 0.0), axis=0, keepdims=True)


def record_kernel(before, cells_smem, cells_ref, *rest):
    if before:
        early_ref, rest = rest[0], rest[1:]
    *fields, out_ref, table_ref, rows_ref = rest
    if before:
        out_ref[pl.ds(0, before), :] = early_ref[...]
    depth, side, _ = fields[0].shape
    total = depth * side * side
    start = lax.axis_index("slab") * total

    def row_of(r):
        row = quotient(jnp.clip(cells_smem[0, r] - start, 0, total - 1), side)
        table_ref[0, r] = row
        return row

    gather_records(before, row_of, cells_ref, fields, out_ref, rows_ref)


def record_call(cells, early, fields):
    side = fields[0].shape[-1]
    n = cells.shape[1]
    before = 0 if early is None else early.shape[0]
    args = [cells, cells] + ([early] if before else []) + list(fields)
    return pl.pallas_call(
        functools.partial(record_kernel, before),
        out_shape=[sds((before + len(fields), n)), sds(cells.shape, jnp.int32)],
        in_specs=[SMEM] + [VMEM] * (len(args) - 1),
        out_specs=[VMEM, SMEM],
        scratch_shapes=[pltpu.VMEM((len(fields), n, side), F32)],
        compiler_params=params(8),
    )(*args)


def swap_segments(parts, segment):
    count = len(parts)
    lanes = count * segment
    lane = lax.broadcasted_iota(jnp.int32, parts[0].shape, 1)
    parts = list(parts)
    bit = count // 2
    while bit:
        low = lax.rem(lax.div(lane, bit * segment), 2) == 0
        for a in range(count):
            if not a & bit:
                first, second = parts[a], parts[a + bit]
                parts[a] = jnp.where(low, first, pltpu.roll(second, bit * segment, 1))
                parts[a + bit] = jnp.where(low, pltpu.roll(first, lanes - bit * segment, 1), second)
        bit //= 2
    return parts


def partner_of(me, k, count):
    if count & (count - 1) == 0:
        return lax.bitwise_xor(me, k)
    return lax.rem(k - me + count, count)


def round_of(me, other, count):
    if count & (count - 1) == 0:
        return lax.bitwise_xor(me, other)
    return lax.rem(me + other, count)


LANES = 128


def to_row(values):
    lane = lax.broadcasted_iota(jnp.int32, (1, LANES), 1)
    row = jnp.zeros((1, LANES), jnp.int32)
    for i, value in enumerate(values):
        row = jnp.where(lane == i, value, row)
    return row


def from_row(row_ref, scalars_ref):
    row = row_ref[...]
    for i in range(scalars_ref.shape[0]):
        scalars_ref[i] = row[0, i]


def pack_kernel(aperture_hbm, slot_hbm, tiles_hbm, *rest):
    *outs, table_row, place_row, table_ref, aperture_ref, slot_ref, tiles_ref, seen_ref, place_ref, sems = rest
    pairs = ((aperture_hbm, aperture_ref), (slot_hbm, slot_ref), (tiles_hbm, tiles_ref))
    copies = [pltpu.make_async_copy(a, b, sems.at[i]) for i, (a, b) in enumerate(pairs)]
    for copy in copies:
        copy.start()
    lat_dev = tiles_ref.shape[0]
    n_shot = len(outs)
    capacity = outs[0].shape[0]
    me = lax.axis_index("shot")
    n_tiles = aperture_ref.shape[1]
    copies[0].wait()
    copies[1].wait()

    def shot(s, carry):
        for r in range(capacity):
            table_ref[s * (capacity + 1) + r] = 0
        seen = jnp.int32(0)
        for p in range(n_tiles):
            slot = slot_ref[aperture_ref[s, p]]
            mine = quotient(slot, lat_dev) == me

            @pl.when(mine)
            def _():
                table_ref[s * (capacity + 1) + seen] = remainder(slot, lat_dev)

            seen = seen + mine.astype(jnp.int32)
        table_ref[s * (capacity + 1) + capacity] = seen
        return carry

    lax.fori_loop(0, n_shot, shot, 0)
    places(aperture_ref, slot_ref, lat_dev, n_shot, capacity, seen_ref, place_ref)
    table_row[...] = to_row([table_ref[i] for i in range(table_ref.shape[0])])
    place_row[...] = to_row([place_ref[i] for i in range(place_ref.shape[0])])
    copies[2].wait()
    for k in range(n_shot):
        base = partner_of(me, k, n_shot) * (capacity + 1)
        for r in range(capacity):
            outs[k][r] = tiles_ref[table_ref[base + r]]


def pack_call(aperture, tile_slot, model_tiles, capacity):
    n_shot = aperture.shape[0]
    _, depth, cells = model_tiles.shape
    row = sds((1, LANES), jnp.int32)
    *blocks, table, place = pl.pallas_call(
        pack_kernel,
        out_shape=[sds((capacity, depth, cells))] * n_shot + [row, row],
        in_specs=[HBM, HBM, HBM],
        out_specs=[VMEM] * (n_shot + 2),
        scratch_shapes=[
            pltpu.SMEM((n_shot * (capacity + 1),), jnp.int32),
            pltpu.SMEM(aperture.shape, jnp.int32),
            pltpu.SMEM(tile_slot.shape, jnp.int32),
            pltpu.VMEM(model_tiles.shape, F32),
            pltpu.SMEM((n_shot,), jnp.int32),
            pltpu.SMEM((aperture.shape[1],), jnp.int32),
            pltpu.SemaphoreType.DMA((3,)),
        ],
        compiler_params=params(8),
        name="pack",
    )(in_hbm(aperture), in_hbm(tile_slot), in_hbm(model_tiles))
    return blocks, table, place


def places(aperture_ref, slot_ref, lat_dev, n_shot, capacity, seen_ref, place_ref):
    me = lax.axis_index("shot")
    for h in range(n_shot):
        seen_ref[h] = 0

    def tile(p, carry):
        holder = quotient(slot_ref[aperture_ref[me, p]], lat_dev)
        rank = seen_ref[holder]
        seen_ref[holder] = rank + 1
        place_ref[p] = round_of(me, holder, n_shot) * capacity + rank
        return carry

    lax.fori_loop(0, aperture_ref.shape[1], tile, 0)


def perturb_kernel(tile_side, place_row, *rest):
    *blocks, out_ref, tiles_ref, place_ref = rest
    n_shot = len(blocks)
    capacity, depth, cells = blocks[0].shape
    side = out_ref.shape[1]
    across = side // tile_side
    flat_ref = out_ref.reshape(depth * side, side)
    from_row(place_row, place_ref)
    for k in range(n_shot):
        tiles_ref[pl.ds(k * capacity, capacity)] = blocks[k][...]

    def tile_row(i, carry):
        for high in range(cells // side):
            parts = [tiles_ref[place_ref[i * across + j], :, pl.ds(high * side, side)] for j in range(across)]
            for low, part in enumerate(swap_segments(parts, tile_side)):
                flat_ref[pl.ds(i * tile_side + high * across + low, depth, stride=side), :] = part
        return carry

    lax.fori_loop(0, across, tile_row, 0)


def pack_back(tile_side, place_row, corr_ref, blocks, tiles_ref, place_ref):
    n_shot = len(blocks)
    capacity, depth, cells = blocks[0].shape
    side = corr_ref.shape[1]
    across = side // tile_side
    flat_ref = corr_ref.reshape(depth * side, side)
    from_row(place_row, place_ref)

    def tile_row(i, carry):
        for high in range(cells // side):
            parts = [
                flat_ref[pl.ds(i * tile_side + high * across + low, depth, stride=side), :] for low in range(across)
            ]
            for j, part in enumerate(swap_segments(parts, tile_side)):
                tiles_ref[place_ref[i * across + j], :, pl.ds(high * side, side)] = part
        return carry

    lax.fori_loop(0, across, tile_row, 0)
    for k in range(n_shot):
        blocks[k][...] = tiles_ref[pl.ds(k * capacity, capacity)]


def tile_scratch(n_shot, capacity, depth, cells, n_tiles):
    return [pltpu.VMEM((n_shot * capacity, depth, cells), F32), pltpu.SMEM((n_tiles,), jnp.int32)]


def perturb_call(place, blocks, side, tile_side, n_tiles):
    capacity, depth, cells = blocks[0].shape
    return pl.pallas_call(
        functools.partial(perturb_kernel, tile_side),
        out_shape=sds((depth, side, side)),
        in_specs=[VMEM] * (1 + len(blocks)),
        out_specs=VMEM,
        scratch_shapes=tile_scratch(len(blocks), capacity, depth, cells, n_tiles),
        compiler_params=params(8),
        name="perturb",
    )(place, *blocks)


def finish_kernel(n_shot, table_row, *refs):
    refs = Refs(refs)
    blocks = refs.take(n_shot)
    parts = refs.refs[:-3]
    sum_ref, record_ref, table_ref = refs.refs[-3:]
    from_row(table_row, table_ref)
    capacity = blocks[0].shape[0]
    total = parts[0][...]
    for part in parts[1:]:
        total = total + part[...]
    for step in range(total.shape[0]):
        record_ref[step] = total[step : step + 1]
    sum_ref[...] = jnp.zeros(sum_ref.shape, F32)
    for k in range(n_shot):
        base = partner_of(lax.axis_index("shot"), k, n_shot) * (capacity + 1)
        for r in range(capacity):

            @pl.when(r < table_ref[base + capacity])
            def _():
                slot = table_ref[base + r]
                sum_ref[slot] = sum_ref[slot] + blocks[k][r]


def finish_call(table, blocks, parts, lat_dev):
    depth, cells = blocks[0].shape[1:]
    steps, n = parts[0].shape
    return pl.pallas_call(
        functools.partial(finish_kernel, len(blocks)),
        out_shape=[sds((lat_dev, depth, cells)), sds((steps, 1, n))],
        in_specs=[VMEM] * (1 + len(blocks) + len(parts)),
        out_specs=[VMEM, VMEM],
        scratch_shapes=[pltpu.SMEM((len(blocks) * (blocks[0].shape[0] + 1),), jnp.int32)],
        compiler_params=params(8),
        name="finish",
    )(table, *blocks, *parts)


def swap(edges):
    count = lax.axis_size("slab")
    shots = lax.axis_size("shot")
    got = []
    for start, edge in enumerate(edges):
        pairs = {}
        for shot in range(shots):
            for i in range(count):
                other = i + 1 if (i - start) % 2 == 0 else i - 1
                if 0 <= other < count:
                    pairs[shot * count + i] = shot * count + other
                elif shots % 2 == 0:
                    pairs[shot * count + i] = (shot ^ 1) * count + i
        got.append(lax.ppermute(edge, ("shot", "slab"), sorted(pairs.items())))
    return tuple(got)


def edges_kernel(n, *refs):
    fields, outs, sems = refs[:n], refs[n:-1], refs[-1]
    depth = fields[0].shape[1]
    low = jnp.where(place()[0] == 1, 0, depth - HALO)
    copies = []
    for out_ref, at in zip(outs, (low, depth - HALO - low)):
        for index, field_ref in enumerate(fields):
            copies.append(
                pltpu.make_async_copy(field_ref.at[0, pl.ds(at, HALO)], out_ref.at[index], sems.at[len(copies)])
            )
    for copy in copies:
        copy.start()
    for copy in copies:
        copy.wait()


def first_edges(fields):
    n = len(fields)
    edge = sds((n, HALO) + fields[0].shape[2:])
    return pl.pallas_call(
        functools.partial(edges_kernel, n),
        out_shape=[edge, edge],
        in_specs=[HBM] * n,
        out_specs=[VMEM, VMEM],
        scratch_shapes=[pltpu.SemaphoreType.DMA((2 * n,))],
        compiler_params=params(8),
    )(*map(in_hbm, fields))


def partners():
    count = lax.axis_size("shot")
    if count & (count - 1) == 0:
        return [[s ^ k for s in range(count)] for k in range(count)]
    return [[(k - s) % count for s in range(count)] for k in range(count)]


def rounds(count):
    return sorted(range(count), key=lambda k: (-(k >> 1).bit_count(), k))


def exchange(blocks):
    got = [None] * len(blocks)
    for k in rounds(len(blocks)):
        block, to = blocks[k], partners()[k]
        moves = [(s, t) for s, t in enumerate(to) if s != t]
        kept = [s for s, t in enumerate(to) if s == t]
        if kept and moves:
            moves = moves + [(s, s) for s in kept]
        got[k] = lax.ppermute(block, "shot", moves) if moves else block
    return got


def slab_parts(part):
    count = lax.axis_size("slab")
    parts = [part]
    for k in range(count - 1, 0, -1):
        to = [s ^ k for s in range(count)] if count & (count - 1) == 0 else [(s + k) % count for s in range(count)]
        parts.append(lax.ppermute(part, "slab", list(enumerate(to))))
    return parts


def per_device(
    model_tiles,
    background,
    u_prev,
    u_now,
    du_prev,
    du_now,
    w_prev,
    w_now,
    wavelet,
    source_cell,
    receiver_cells,
    aperture,
    tile_slot,
):
    lat_dev, depth, tile_cells = model_tiles.shape
    side = background.shape[-1]
    tile_side = math.isqrt(tile_cells)
    capacity = aperture.shape[1] // 4
    n_shot = lax.axis_size("shot")
    steps = wavelet.shape[1]
    speed = background[0]
    u, d, w = u_now[0], du_now[0], w_now[0]
    up, dp, wp = u_prev[0], du_prev[0], w_prev[0]

    u_halo = swap(first_edges([u_now]))
    dw_halo = swap(first_edges([du_now, w_now]))
    outgoing, table, place_row = pack_call(aperture, tile_slot, model_tiles, capacity)
    incoming = exchange(outgoing)
    count, outer = count_call(receiver_cells, depth, side)
    perturb = perturb_call(place_row, incoming, side, tile_side, aperture.shape[1])
    tiling = (place_row, n_shot, aperture.shape[1], tile_side)

    u_next, lap, corr, *edges = u_call(0, False, wavelet, source_cell, u, up, u_halo, speed, w_now, None, None, *tiling)
    u_halo = swap(edges)
    bare, *edges = w_bare_call(w, wp, dw_halo, 1, speed)
    w_halo = swap(edges)
    d_next, w_next, *edges = d_call(d, dp, dw_halo, 0, speed, perturb, lap, bare, count)
    d_halo = swap(edges)
    traces = u_local = None
    for step in range(1, steps - 1):
        traces, receiver_rows = record_call(receiver_cells, traces, [d_next])
        u, up, d, dp, w, wp = u_next, u, d_next, d, w_next, w
        u_next, lap, corr, *edges = u_call(
            step, False, wavelet, source_cell, u, up, u_halo, speed, w, corr, u_local, *tiling
        )
        u_halo = swap(edges)
        u_local, d_local, w_local = ahead_call([u_next, d, w])
        d_next, w_next, *edges = dw_call(
            d, dp, w, wp, d_halo, w_halo, d_local, w_local, speed, perturb, lap, count, outer if step == 1 else None
        )
        d_halo = swap(edges[:2])
        w_halo = swap(edges[2:])
    u, up, d, dp, w, wp = u_next, u, d_next, d, w_next, w
    step = steps - 1
    lap, *returning = u_call(step, True, wavelet, source_cell, u, up, u_halo, speed, w, corr, u_local, *tiling)
    arrived = exchange(returning)
    d_final, d_next, traces = last_d_call(
        step, d, dp, d_halo, speed, perturb, lap, receiver_cells, receiver_rows, traces
    )
    parts = slab_parts(traces)
    w_final, u_final = last_w_call(w, wp, w_halo, speed, count, d_next, u, up, lap, source_cell, wavelet)
    sensitivity, traces = finish_call(table, arrived, parts, lat_dev)
    return (sensitivity, u_final, d_final, w_final, jnp.transpose(traces, (1, 0, 2)))


def solution(mesh):
    field = P("shot", "slab", None, None)
    tiles = P("shot", "slab", None)
    in_specs = (tiles,) + (field,) * 7 + (P("shot", None), P("shot"), P("shot", None), P(), P())
    out_specs = (tiles, field, field, field, P("shot", None, None))


    return jax.shard_map(per_device, mesh=mesh, in_specs=in_specs, out_specs=out_specs, check_vma=False)
```

```python
import functools
import math

import jax
import jax.numpy as jnp
from jax import lax
from jax.experimental import pallas as pl
from jax.experimental.pallas import tpu as pltpu
from jax.sharding import PartitionSpec as P


COEFFS = (-205.0 / 72.0, 8.0 / 5.0, -1.0 / 5.0, 8.0 / 315.0, -1.0 / 560.0)
HALO = len(COEFFS) - 1
SUB = 8
F32 = jnp.float32
VMEM = pl.BlockSpec(memory_space=pltpu.VMEM)
SMEM = pl.BlockSpec(memory_space=pltpu.SMEM)
HBM = pl.BlockSpec(memory_space=pltpu.HBM)


def params(mib):
    return pltpu.CompilerParams(vmem_limit_bytes=mib * 1024 * 1024)


def in_hbm(x):
    return pltpu.with_memory_space_constraint(x, pltpu.HBM)


def sds(shape, dtype=F32):
    return jax.ShapeDtypeStruct(shape, dtype)


def place():
    slab, count = lax.axis_index("slab"), lax.axis_size("slab")
    odd = lax.bitwise_and(slab, 1)
    above, below = slab < count - 1, slab > 0
    is_odd = odd == 1
    return odd, (is_odd & below) | (~is_odd & above), (is_odd & above) | (~is_odd & below)


def quotient(x, m):
    return lax.shift_right_logical(x, m.bit_length() - 1) if m & (m - 1) == 0 else lax.div(x, m)


def remainder(x, m):
    return lax.bitwise_and(x, m - 1) if m & (m - 1) == 0 else lax.rem(x, m)


SCALE = 5040.0
PARTS = 4


def band_weights(side):
    i = lax.broadcasted_iota(jnp.int32, (2 * side, 2 * side), 0)
    j = lax.broadcasted_iota(jnp.int32, (2 * side, 2 * side), 1)
    far = jnp.where((i < side) == (j < side), jnp.abs(i - j), 0)
    out = jnp.zeros((2 * side, 2 * side), F32)
    for k in range(1, HALO + 1):
        out = jnp.where(far == k, round(COEFFS[k] * SCALE) * 1.0, out)
    out = out.astype(jnp.bfloat16)
    return jnp.concatenate([out, out, out], axis=0)


def split3(x):
    high = x.astype(jnp.bfloat16)
    rest = x - high.astype(F32)
    mid = rest.astype(jnp.bfloat16)
    low = (rest - mid.astype(F32)).astype(jnp.bfloat16)
    return high, mid, low


def prepare_local(rows_ref, lanes_ref, now_ref, weights):
    depth, side, _ = now_ref.shape
    zeros = jnp.zeros((SUB, side), F32)
    half = depth // 2
    parts = []
    for low, high in zip(split3(now_ref[pl.ds(0, half)]), split3(now_ref[pl.ds(half, half)])):
        parts += [low.reshape(half * side, side), high.reshape(half * side, side)]
    lanes = jnp.dot(jnp.concatenate(parts, axis=1), weights, preferred_element_type=F32)
    lanes_ref[pl.ds(0, half)] = lanes[:, :side].reshape(half, side, side)
    lanes_ref[pl.ds(half, half)] = lanes[:, side:].reshape(half, side, side)
    for z in range(depth):
        rows_ref[z, pl.ds(0, SUB), :] = zeros
        rows_ref[z, pl.ds(SUB + side, SUB), :] = zeros
        rows_ref[z, pl.ds(SUB, side), :] = now_ref[z]


def prepare_halo(halo_ref, first_ref, second_ref, index, inject=None):
    odd, has_first, has_second = place()

    def halo(z, carry):
        halo_ref[1 - odd, z] = jnp.where(has_first, first_ref[index, z], 0.0)
        halo_ref[odd, z] = jnp.where(has_second, second_ref[index, z], 0.0)
        return carry

    lax.fori_loop(0, HALO, halo, 0)
    if inject:
        outer_ref, other_ref = inject
        for end in range(2):
            for z in range(HALO):
                halo_ref[end, z] = halo_ref[end, z] + outer_ref[end, z] * other_ref[end, z]


def prepare(work, now_ref, first_ref, second_ref, index, weights):
    rows_ref, halo_ref, lanes_ref = work
    prepare_local(rows_ref, lanes_ref, now_ref, weights)
    prepare_halo(halo_ref, first_ref, second_ref, index)


def each_laplacian(work, now_ref, emit, finish=None, parts=1):
    rows_ref, halo_ref, lanes_ref = work
    depth, side, _ = now_ref.shape

    def block(g, carry):
        start = pl.multiple_of(g * SUB, SUB)
        rows = pl.ds(start, SUB)
        column = [halo_ref[0, z, rows, :] for z in range(HALO)]
        column += [now_ref[z, rows, :] for z in range(depth)]
        column += [halo_ref[1, z, rows, :] for z in range(HALO)]
        for z in range(depth):
            centre = column[HALO + z]
            total = (3.0 * COEFFS[0]) * centre + (1.0 / SCALE) * lanes_ref[z, rows, :]
            for k in range(1, HALO + 1):
                ring = (column[HALO + z + k] + column[HALO + z - k]) + (
                    rows_ref[z, pl.ds(start + (SUB + k), SUB), :] + rows_ref[z, pl.ds(start + (SUB - k), SUB), :]
                )
                total = total + COEFFS[k] * ring
            emit(z, rows, centre, total)
        return carry

    blocks = side // SUB // parts
    for part in range(parts):
        lax.fori_loop(part * blocks, (part + 1) * blocks, block, 0)
        if finish:
            finish(part, parts)


def halo_space(side):
    return pltpu.VMEM((2, HALO, side, side), F32)


def work_space(depth, side):
    return [
        pltpu.VMEM((depth, side + 2 * SUB, side), F32),
        halo_space(side),
        pltpu.VMEM((depth, side, side), F32),
    ]


def ahead_kernel(n, *refs):
    fields, outs, (rows_ref, lanes_ref) = refs[:n], refs[n:-2], refs[-2:]
    depth, side, _ = fields[0].shape
    weights = band_weights(side)
    for now_ref, out_ref in zip(fields, outs):
        prepare_local(rows_ref, lanes_ref, now_ref, weights)

        def block(g, carry, now_ref=now_ref, out_ref=out_ref):
            start = pl.multiple_of(g * SUB, SUB)
            rows = pl.ds(start, SUB)
            column = [now_ref[z, rows, :] for z in range(depth)]
            for z in range(depth):
                total = (3.0 * COEFFS[0]) * column[z] + (1.0 / SCALE) * lanes_ref[z, rows, :]
                for k in range(1, HALO + 1):
                    ring = (
                        rows_ref[z, pl.ds(start + (SUB + k), SUB), :] + rows_ref[z, pl.ds(start + (SUB - k), SUB), :]
                    )
                    if z + k < depth:
                        ring = ring + column[z + k]
                    if z - k >= 0:
                        ring = ring + column[z - k]
                    total = total + COEFFS[k] * ring
                out_ref[z, rows, :] = total
            return carry

        lax.fori_loop(0, side // SUB, block, 0)


def ahead_call(fields):
    depth, side, _ = fields[0].shape
    outs = [sds((depth, side, side))] * len(fields)
    rows, _, lanes = work_space(depth, side)
    return pl.pallas_call(
        functools.partial(ahead_kernel, len(fields)),
        out_shape=outs,
        in_specs=[VMEM] * len(fields),
        out_specs=[VMEM] * len(outs),
        scratch_shapes=[rows, lanes],
        compiler_params=params(16),
    )(*fields)


def each_remainder(halo_ref, local_ref, now_ref, emit):
    depth, side, _ = now_ref.shape

    def block(g, carry):
        rows = pl.ds(pl.multiple_of(g * SUB, SUB), SUB)
        below = [halo_ref[0, z, rows, :] for z in range(HALO)]
        above = [halo_ref[1, z, rows, :] for z in range(HALO)]
        for z in range(depth):
            total = local_ref[z, rows, :]
            for k in range(1, HALO + 1):
                if z - k < 0:
                    total = total + COEFFS[k] * below[HALO + z - k]
                if z + k >= depth:
                    total = total + COEFFS[k] * above[z + k - depth]
            emit(z, rows, now_ref[z, rows, :], total)
        return carry

    lax.fori_loop(0, side // SUB, block, 0)


def copy_sends(next_ref, first_ref, second_ref, index):
    depth = next_ref.shape[0]
    odd = place()[0] == 1
    first = jnp.where(odd, 0, depth - HALO)
    second = jnp.where(odd, depth - HALO, 0)
    for z in range(HALO):
        first_ref[index, z] = next_ref[first + z]
        second_ref[index, z] = next_ref[second + z]


def store_out(next_ref, out_ref, sems, step, steps):
    rows = pl.ds(step * (next_ref.shape[1] // steps), next_ref.shape[1] // steps)
    return pltpu.make_async_copy(next_ref.at[:, rows], out_ref.at[0, :, rows], sems.at[step])


def add_source(next_ref, source_ref, wavelet_ref, step, first, rows):
    depth, side, _ = next_ref.shape
    local = source_ref[0] - lax.axis_index("slab") * (depth * side * side)
    mine = (local >= 0) & (local < depth * side * side)
    cell = jnp.where(mine, local, 0)
    z = quotient(cell, side * side)
    x = remainder(quotient(cell, side), side)
    lane = lax.broadcasted_iota(jnp.int32, (1, side), 1)

    @pl.when(mine & (x >= first) & (x < first + rows))
    def _():
        add = jnp.where(lane == remainder(cell, side), wavelet_ref[0, step], 0.0)
        next_ref[z, pl.ds(x, 1), :] = next_ref[z, pl.ds(x, 1), :] + add


class Refs:
    def __init__(self, refs):
        self.refs = list(refs)

    def take(self, n=None):
        if n is None:
            return self.refs.pop(0)
        return [self.refs.pop(0) for _ in range(n)]


def u_kernel(step, last, ahead, tiles, *refs):
    refs = Refs(refs)
    now_ref, ha_ref, hb_ref, w_in = refs.take(4)
    if not last:
        source_ref, wavelet_hbm, prev_ref, speed_ref = refs.take(4)
    corr_in = refs.take() if step else None
    local_ref = refs.take() if ahead else None
    place_row = refs.take() if last else None
    if last:
        lap_ref = refs.take()
        blocks = refs.take(tiles[0])
        corr_ref = refs.take()
    else:
        next_ref, lap_ref, corr_ref = refs.take(3)
        sends = refs.take(2)
    halo_ref = refs.take()
    if not ahead:
        rows_ref, lanes_ref = refs.take(2)
    own_sems = refs.take()
    copies, late = [], []
    if not last:
        wavelet_ref = refs.take()
        late.append(pltpu.make_async_copy(wavelet_hbm, wavelet_ref, own_sems.at[0]))
    w_ref = w_in
    if not step:
        w_ref = refs.take()
        half = w_ref.shape[0] // 2
        for i in range(2):
            part = pl.ds(i * half, half)
            copies.append(pltpu.make_async_copy(w_in.at[0, part], w_ref.at[part], own_sems.at[1 + i]))
    if last:
        tiles_ref, place_ref = refs.take(2)
    for copy in copies + late:
        copy.start()
    _, side, _ = now_ref.shape
    if not ahead:
        prepare_local(rows_ref, lanes_ref, now_ref, band_weights(side))
    prepare_halo(halo_ref, ha_ref, hb_ref, 0)
    for copy in copies:
        copy.wait()

    def emit(z, block, centre, lap):
        lap_ref[z, block, :] = lap
        part = lap * w_ref[z, block, :]
        corr_ref[z, block, :] = corr_in[z, block, :] + part if step else part
        if not last:
            next_ref[z, block, :] = (2.0 * centre - prev_ref[z, block, :]) + speed_ref[z, block, :] * lap

    if ahead:
        each_remainder(halo_ref, local_ref, now_ref, emit)
    else:
        each_laplacian((rows_ref, halo_ref, lanes_ref), now_ref, emit)
    for copy in late:
        copy.wait()
    if last:
        pack_back(tiles[1], place_row, corr_ref, blocks, tiles_ref, place_ref)
    else:
        add_source(next_ref, source_ref, wavelet_ref, step, 0, side)
        copy_sends(next_ref, *sends, 0)


def w_bare_kernel(index, now_ref, prev_ref, ha_ref, hb_ref, speed_ref, next_ref, *rest):
    sends, work = rest[:2], rest[2:]
    _, side, _ = now_ref.shape
    prepare(work, now_ref, ha_ref, hb_ref, index, band_weights(side))

    def emit(z, block, centre, lap):
        next_ref[z, block, :] = (2.0 * centre - prev_ref[z, block, :]) + speed_ref[z, block, :] * lap

    each_laplacian(work, now_ref, emit)
    copy_sends(next_ref, *sends, 0)


def d_kernel(index, now_ref, prev_ref, ha_ref, hb_ref, speed_ref, perturb_ref, lap_u_ref, bare_ref, count_ref, *rest):
    next_ref, w_ref, *sends = rest[:4]
    work = rest[4:]
    _, side, _ = now_ref.shape
    prepare(work, now_ref, ha_ref, hb_ref, index, band_weights(side))

    def emit(z, block, centre, lap):
        new = ((2.0 * centre - prev_ref[z, block, :]) + speed_ref[z, block, :] * lap) + (
            perturb_ref[z, block, :] * lap_u_ref[z, block, :]
        )
        next_ref[z, block, :] = new
        w_ref[z, block, :] = bare_ref[z, block, :] + count_ref[z, block, :] * new

    each_laplacian(work, now_ref, emit)
    copy_sends(next_ref, *sends, 0)


def dw_kernel(bare, *refs):
    refs = Refs(refs)
    speed_ref, d_ref, d_prev, w_ref, w_prev, perturb_ref, lap_u_ref, count_ref = refs.take(8)
    d_halo, w_halo = refs.take(2), refs.take(2)
    d_local, w_local = refs.take(2)
    outer_ref = refs.take() if bare else None
    d_next, w_next = refs.take(2)
    d_sends, w_sends = refs.take(2), refs.take(2)
    d_halos, w_halos = refs.take(2)
    prepare_halo(d_halos, *d_halo, 0)
    prepare_halo(w_halos, *w_halo, 0, (outer_ref, d_halos) if bare else None)

    def emit_d(z, block, centre, lap):
        d_next[z, block, :] = ((2.0 * centre - d_prev[z, block, :]) + speed_ref[z, block, :] * lap) + (
            perturb_ref[z, block, :] * lap_u_ref[z, block, :]
        )

    def emit_w(z, block, centre, lap):
        w_next[z, block, :] = ((2.0 * centre - w_prev[z, block, :]) + speed_ref[z, block, :] * lap) + (
            count_ref[z, block, :] * d_next[z, block, :]
        )

    each_remainder(d_halos, d_local, d_ref, emit_d)
    copy_sends(d_next, *d_sends, 0)
    each_remainder(w_halos, w_local, w_ref, emit_w)
    copy_sends(w_next, *w_sends, 0)


def last_d_kernel(before, *refs):
    refs = Refs(refs)
    now_ref, prev_ref, ha_ref, hb_ref, speed_ref, perturb_ref, lap_u_ref, cells_ref, rows_hbm = refs.take(9)
    early_ref = refs.take() if before else None
    out_ref, next_ref, record_ref = refs.take(3)
    work = refs.take(3)
    rows_smem, rows_ref, sems, table_sem = refs.take(4)
    fetch = pltpu.make_async_copy(rows_hbm, rows_smem, table_sem)
    fetch.start()
    _, side, _ = now_ref.shape
    prepare(work, now_ref, ha_ref, hb_ref, 0, band_weights(side))

    def emit(z, block, centre, lap):
        next_ref[z, block, :] = ((2.0 * centre - prev_ref[z, block, :]) + speed_ref[z, block, :] * lap) + (
            perturb_ref[z, block, :] * lap_u_ref[z, block, :]
        )

    def finish(part, parts):
        store_out(next_ref, out_ref, sems, part, parts).start()

    each_laplacian(work, now_ref, emit, finish, PARTS)
    fetch.wait()
    if before:
        record_ref[pl.ds(0, before), :] = early_ref[...]
    fields = [now_ref, next_ref] if record_ref.shape[0] > before + 1 else [next_ref]
    gather_records(before, lambda r: rows_smem[0, r], cells_ref, fields, record_ref, rows_ref)
    for part in range(PARTS):
        store_out(next_ref, out_ref, sems, part, PARTS).wait()


def last_w_kernel(*refs):
    refs = Refs(refs)
    now_ref, prev_ref, ha_ref, hb_ref, speed_ref, count_ref, d_next = refs.take(7)
    u_ref, u_prev, lap_u_ref, source_ref, wavelet_hbm = refs.take(5)
    out_ref, u_out = refs.take(2)
    next_ref, u_next = refs.take(2)
    work = refs.take(3)
    wavelet_ref, sems, table_sem = refs.take(3)
    fetch = pltpu.make_async_copy(wavelet_hbm, wavelet_ref, table_sem)
    fetch.start()
    _, side, _ = now_ref.shape
    prepare(work, now_ref, ha_ref, hb_ref, 0, band_weights(side))
    last_step = wavelet_ref.shape[1] - 1

    def emit(z, block, centre, lap):
        speed = speed_ref[z, block, :]
        next_ref[z, block, :] = ((2.0 * centre - prev_ref[z, block, :]) + speed * lap) + (
            count_ref[z, block, :] * d_next[z, block, :]
        )
        u_next[z, block, :] = (2.0 * u_ref[z, block, :] - u_prev[z, block, :]) + speed * lap_u_ref[z, block, :]

    def finish(part, parts):
        size = side // parts
        if part == 0:
            fetch.wait()
        add_source(u_next, source_ref, wavelet_ref, last_step, part * size, size)
        store_out(next_ref, out_ref, sems.at[0], part, parts).start()
        store_out(u_next, u_out, sems.at[1], part, parts).start()

    each_laplacian(work, now_ref, emit, finish, PARTS)
    for part in range(PARTS):
        store_out(next_ref, out_ref, sems.at[0], part, PARTS).wait()
        store_out(u_next, u_out, sems.at[1], part, PARTS).wait()


def stencil_call(body, in_specs, args, outs, kinds, scratch):
    return pl.pallas_call(
        body, out_shape=outs, in_specs=in_specs, out_specs=kinds, scratch_shapes=scratch, compiler_params=params(20)
    )(*args)


def u_call(step, last, wavelet, source, u, u_prev, halo, speed, w, corr, local, place, n_shot, n_tiles, tile_side):
    field = sds(u.shape)
    edge = sds((1, HALO) + u.shape[1:])
    args, specs = [u, *halo, w], [VMEM] * 4
    if not step:
        args[3], specs[3] = in_hbm(w), HBM
    if not last:
        args, specs = args + [source, in_hbm(wavelet), u_prev, speed], specs + [SMEM, HBM, VMEM, VMEM]
    if step:
        args, specs = args + [corr], specs + [VMEM]
    ahead = local is not None
    if ahead:
        args, specs = args + [local], specs + [VMEM]
    cells = tile_side * tile_side
    capacity = n_tiles // 4
    rows, halos, lanes = work_space(*u.shape[:2])
    scratch = [halos] + ([] if ahead else [rows, lanes]) + [pltpu.SemaphoreType.DMA((3,))]
    if not last:
        scratch += [pltpu.SMEM(wavelet.shape, F32)]
    if not step:
        scratch += [pltpu.VMEM(u.shape, F32)]
    if last:
        args, specs = args + [place], specs + [VMEM]
        outs = [field] + [sds((capacity, u.shape[0], cells))] * n_shot
        scratch = [pltpu.VMEM(u.shape, F32)] + scratch + tile_scratch(n_shot, capacity, u.shape[0], cells, n_tiles)
    else:
        outs = [field] * 3 + [edge] * 2
    body = functools.partial(u_kernel, step, last, ahead, (n_shot, tile_side))
    return stencil_call(body, specs, args, outs, [VMEM] * len(outs), scratch)


def w_bare_call(w, w_prev, halo, index, speed):
    field, edge = sds(w.shape), sds((1, HALO) + w.shape[1:])
    args = [w, w_prev, *halo, speed]
    body = functools.partial(w_bare_kernel, index)
    return stencil_call(body, [VMEM] * 5, args, [field, edge, edge], [VMEM] * 3, work_space(*w.shape[:2]))


def d_call(d, d_prev, halo, index, speed, perturb, lap_u, bare, count):
    field, edge = sds(d.shape), sds((1, HALO) + d.shape[1:])
    args = [d, d_prev, *halo, speed, perturb, lap_u, bare, count]
    body = functools.partial(d_kernel, index)
    outs = [field, field, edge, edge]
    return stencil_call(body, [VMEM] * 9, args, outs, [VMEM] * 4, work_space(*d.shape[:2]))


def dw_call(d, d_prev, w, w_prev, d_halo, w_halo, d_local, w_local, speed, perturb, lap_u, count, outer):
    field, edge = sds(d.shape), sds((1, HALO) + d.shape[1:])
    bare = outer is not None
    args = [speed, d, d_prev, w, w_prev, perturb, lap_u, count, *d_halo, *w_halo, d_local, w_local]
    args += [outer] if bare else []
    outs = [field, field] + [edge] * 4
    body = functools.partial(dw_kernel, bare)
    return stencil_call(body, [VMEM] * len(args), args, outs, [VMEM] * 6, [halo_space(d.shape[1])] * 2)


def last_d_call(step, d, d_prev, halo, speed, perturb, lap_u, cells, rows, early):
    before = 0 if early is None else early.shape[0]
    n = cells.shape[1]
    fields = step + 1 - before
    args = [d, d_prev, *halo, speed, perturb, lap_u, cells, rows]
    specs = [VMEM] * 8 + [HBM]
    if before:
        args, specs = args + [early], specs + [VMEM]
    scratch = work_space(*d.shape[:2]) + [
        pltpu.SMEM(cells.shape, jnp.int32),
        pltpu.VMEM((fields, n, d.shape[-1]), F32),
        pltpu.SemaphoreType.DMA((PARTS,)),
        pltpu.SemaphoreType.DMA(()),
    ]
    outs = [sds((1,) + d.shape), sds(d.shape), sds((step + 1, n))]
    body = functools.partial(last_d_kernel, before)
    return stencil_call(body, specs, args, outs, [HBM, VMEM, VMEM], scratch)


def last_w_call(w, w_prev, halo, speed, count, d_next, u, u_prev, lap_u, source, wavelet):
    args = [w, w_prev, *halo, speed, count, d_next, u, u_prev, lap_u, source, in_hbm(wavelet)]
    specs = [VMEM] * 10 + [SMEM, HBM]
    scratch = [pltpu.VMEM(w.shape, F32)] * 2 + work_space(*w.shape[:2]) + [
        pltpu.SMEM(wavelet.shape, F32),
        pltpu.SemaphoreType.DMA((2, PARTS)),
        pltpu.SemaphoreType.DMA(()),
    ]
    outs = [sds((1,) + w.shape)] * 2
    return stencil_call(last_w_kernel, specs, args, outs, [HBM] * 2, scratch)


def count_kernel(cells_ref, count_ref, outer_ref):
    depth, side, _ = count_ref.shape
    local = cells_ref[...] - (lax.axis_index("slab") * depth - HALO) * (side * side)
    n = local.shape[1]
    row_of = jnp.where(local >= 0, quotient(jnp.maximum(local, 0), side), -1)
    lane_of = remainder(jnp.maximum(local, 0), side)
    lanes = lax.broadcasted_iota(jnp.int32, (side, n), 0)
    lane_hot = jnp.where(lanes == lane_of, 1.0, 0.0).astype(jnp.bfloat16)
    for z in range(depth + 2 * HALO):
        row_hot = jnp.where(lanes + z * side == row_of, 1.0, 0.0).astype(jnp.bfloat16)
        plane = lax.dot_general(row_hot, lane_hot, (((1,), (1,)), ((), ())), preferred_element_type=F32)
        if z < HALO:
            outer_ref[0, z] = plane
        elif z < HALO + depth:
            count_ref[z - HALO] = plane
        else:
            outer_ref[1, z - HALO - depth] = plane


def count_call(cells, depth, side):
    return pl.pallas_call(
        count_kernel,
        out_shape=[sds((depth, side, side)), sds((2, HALO, side, side))],
        in_specs=[VMEM],
        out_specs=[VMEM, VMEM],
        compiler_params=params(8),
        name="count",
    )(cells)


def gather_records(before, row_of, cells_ref, fields, out_ref, rows_ref):
    depth, side, _ = fields[0].shape
    n = cells_ref.shape[1]
    total = depth * side * side
    local = cells_ref[...] - lax.axis_index("slab") * total
    mine = (local >= 0) & (local < total)
    lane_of = jnp.where(mine, remainder(jnp.maximum(local, 0), side), -1)
    lanes = lax.broadcasted_iota(jnp.int32, (side, n), 0)
    hit = lanes == lane_of
    flat = [field_ref.reshape(depth * side, side) for field_ref in fields]

    def gather(r, carry):
        row = row_of(r)
        for step, field_ref in enumerate(flat):
            rows_ref[step, pl.ds(r, 1), :] = field_ref[pl.ds(row, 1), :]
        return carry

    lax.fori_loop(0, n, gather, 0, unroll=32)
    for step in range(len(fields)):
        turned = rows_ref[step].T
        out_ref[pl.ds(before + step, 1), :] = jnp.sum(jnp.where(hit, turned, 0.0), axis=0, keepdims=True)


def record_kernel(before, cells_smem, cells_ref, *rest):
    if before:
        early_ref, rest = rest[0], rest[1:]
    *fields, out_ref, table_ref, rows_ref = rest
    if before:
        out_ref[pl.ds(0, before), :] = early_ref[...]
    depth, side, _ = fields[0].shape
    total = depth * side * side
    start = lax.axis_index("slab") * total

    def row_of(r):
        row = quotient(jnp.clip(cells_smem[0, r] - start, 0, total - 1), side)
        table_ref[0, r] = row
        return row

    gather_records(before, row_of, cells_ref, fields, out_ref, rows_ref)


def record_call(cells, early, fields):
    side = fields[0].shape[-1]
    n = cells.shape[1]
    before = 0 if early is None else early.shape[0]
    args = [cells, cells] + ([early] if before else []) + list(fields)
    return pl.pallas_call(
        functools.partial(record_kernel, before),
        out_shape=[sds((before + len(fields), n)), sds(cells.shape, jnp.int32)],
        in_specs=[SMEM] + [VMEM] * (len(args) - 1),
        out_specs=[VMEM, SMEM],
        scratch_shapes=[pltpu.VMEM((len(fields), n, side), F32)],
        compiler_params=params(8),
    )(*args)


def swap_segments(parts, segment):
    count = len(parts)
    lanes = count * segment
    lane = lax.broadcasted_iota(jnp.int32, parts[0].shape, 1)
    parts = list(parts)
    bit = count // 2
    while bit:
        low = lax.rem(lax.div(lane, bit * segment), 2) == 0
        for a in range(count):
            if not a & bit:
                first, second = parts[a], parts[a + bit]
                parts[a] = jnp.where(low, first, pltpu.roll(second, bit * segment, 1))
                parts[a + bit] = jnp.where(low, pltpu.roll(first, lanes - bit * segment, 1), second)
        bit //= 2
    return parts


def partner_of(me, k, count):
    if count & (count - 1) == 0:
        return lax.bitwise_xor(me, k)
    return lax.rem(k - me + count, count)


def round_of(me, other, count):
    if count & (count - 1) == 0:
        return lax.bitwise_xor(me, other)
    return lax.rem(me + other, count)


LANES = 128


def to_row(values):
    lane = lax.broadcasted_iota(jnp.int32, (1, LANES), 1)
    row = jnp.zeros((1, LANES), jnp.int32)
    for i, value in enumerate(values):
        row = jnp.where(lane == i, value, row)
    return row


def from_row(row_ref, scalars_ref):
    row = row_ref[...]
    for i in range(scalars_ref.shape[0]):
        scalars_ref[i] = row[0, i]


def pack_kernel(aperture_hbm, slot_hbm, tiles_hbm, *rest):
    *outs, table_row, place_row, table_ref, aperture_ref, slot_ref, tiles_ref, seen_ref, place_ref, sems = rest
    pairs = ((aperture_hbm, aperture_ref), (slot_hbm, slot_ref), (tiles_hbm, tiles_ref))
    copies = [pltpu.make_async_copy(a, b, sems.at[i]) for i, (a, b) in enumerate(pairs)]
    for copy in copies:
        copy.start()
    lat_dev = tiles_ref.shape[0]
    n_shot = len(outs)
    capacity = outs[0].shape[0]
    me = lax.axis_index("shot")
    n_tiles = aperture_ref.shape[1]
    copies[0].wait()
    copies[1].wait()

    def shot(s, carry):
        for r in range(capacity):
            table_ref[s * (capacity + 1) + r] = 0
        seen = jnp.int32(0)
        for p in range(n_tiles):
            slot = slot_ref[aperture_ref[s, p]]
            mine = quotient(slot, lat_dev) == me

            @pl.when(mine)
            def _():
                table_ref[s * (capacity + 1) + seen] = remainder(slot, lat_dev)

            seen = seen + mine.astype(jnp.int32)
        table_ref[s * (capacity + 1) + capacity] = seen
        return carry

    lax.fori_loop(0, n_shot, shot, 0)
    places(aperture_ref, slot_ref, lat_dev, n_shot, capacity, seen_ref, place_ref)
    table_row[...] = to_row([table_ref[i] for i in range(table_ref.shape[0])])
    place_row[...] = to_row([place_ref[i] for i in range(place_ref.shape[0])])
    copies[2].wait()
    for k in range(n_shot):
        base = partner_of(me, k, n_shot) * (capacity + 1)
        for r in range(capacity):
            outs[k][r] = tiles_ref[table_ref[base + r]]


def pack_call(aperture, tile_slot, model_tiles, capacity):
    n_shot = aperture.shape[0]
    _, depth, cells = model_tiles.shape
    row = sds((1, LANES), jnp.int32)
    *blocks, table, place = pl.pallas_call(
        pack_kernel,
        out_shape=[sds((capacity, depth, cells))] * n_shot + [row, row],
        in_specs=[HBM, HBM, HBM],
        out_specs=[VMEM] * (n_shot + 2),
        scratch_shapes=[
            pltpu.SMEM((n_shot * (capacity + 1),), jnp.int32),
            pltpu.SMEM(aperture.shape, jnp.int32),
            pltpu.SMEM(tile_slot.shape, jnp.int32),
            pltpu.VMEM(model_tiles.shape, F32),
            pltpu.SMEM((n_shot,), jnp.int32),
            pltpu.SMEM((aperture.shape[1],), jnp.int32),
            pltpu.SemaphoreType.DMA((3,)),
        ],
        compiler_params=params(8),
        name="pack",
    )(in_hbm(aperture), in_hbm(tile_slot), in_hbm(model_tiles))
    return blocks, table, place


def places(aperture_ref, slot_ref, lat_dev, n_shot, capacity, seen_ref, place_ref):
    me = lax.axis_index("shot")
    for h in range(n_shot):
        seen_ref[h] = 0

    def tile(p, carry):
        holder = quotient(slot_ref[aperture_ref[me, p]], lat_dev)
        rank = seen_ref[holder]
        seen_ref[holder] = rank + 1
        place_ref[p] = round_of(me, holder, n_shot) * capacity + rank
        return carry

    lax.fori_loop(0, aperture_ref.shape[1], tile, 0)


def perturb_kernel(tile_side, place_row, *rest):
    *blocks, out_ref, tiles_ref, place_ref = rest
    n_shot = len(blocks)
    capacity, depth, cells = blocks[0].shape
    side = out_ref.shape[1]
    across = side // tile_side
    flat_ref = out_ref.reshape(depth * side, side)
    from_row(place_row, place_ref)
    for k in range(n_shot):
        tiles_ref[pl.ds(k * capacity, capacity)] = blocks[k][...]

    def tile_row(i, carry):
        for high in range(cells // side):
            parts = [tiles_ref[place_ref[i * across + j], :, pl.ds(high * side, side)] for j in range(across)]
            for low, part in enumerate(swap_segments(parts, tile_side)):
                flat_ref[pl.ds(i * tile_side + high * across + low, depth, stride=side), :] = part
        return carry

    lax.fori_loop(0, across, tile_row, 0)


def pack_back(tile_side, place_row, corr_ref, blocks, tiles_ref, place_ref):
    n_shot = len(blocks)
    capacity, depth, cells = blocks[0].shape
    side = corr_ref.shape[1]
    across = side // tile_side
    flat_ref = corr_ref.reshape(depth * side, side)
    from_row(place_row, place_ref)

    def tile_row(i, carry):
        for high in range(cells // side):
            parts = [
                flat_ref[pl.ds(i * tile_side + high * across + low, depth, stride=side), :] for low in range(across)
            ]
            for j, part in enumerate(swap_segments(parts, tile_side)):
                tiles_ref[place_ref[i * across + j], :, pl.ds(high * side, side)] = part
        return carry

    lax.fori_loop(0, across, tile_row, 0)
    for k in range(n_shot):
        blocks[k][...] = tiles_ref[pl.ds(k * capacity, capacity)]


def tile_scratch(n_shot, capacity, depth, cells, n_tiles):
    return [pltpu.VMEM((n_shot * capacity, depth, cells), F32), pltpu.SMEM((n_tiles,), jnp.int32)]


def perturb_call(place, blocks, side, tile_side, n_tiles):
    capacity, depth, cells = blocks[0].shape
    return pl.pallas_call(
        functools.partial(perturb_kernel, tile_side),
        out_shape=sds((depth, side, side)),
        in_specs=[VMEM] * (1 + len(blocks)),
        out_specs=VMEM,
        scratch_shapes=tile_scratch(len(blocks), capacity, depth, cells, n_tiles),
        compiler_params=params(8),
        name="perturb",
    )(place, *blocks)


def finish_kernel(n_shot, table_row, *refs):
    refs = Refs(refs)
    blocks = refs.take(n_shot)
    parts = refs.refs[:-3]
    sum_ref, record_ref, table_ref = refs.refs[-3:]
    from_row(table_row, table_ref)
    capacity = blocks[0].shape[0]
    total = parts[0][...]
    for part in parts[1:]:
        total = total + part[...]
    for step in range(total.shape[0]):
        record_ref[step] = total[step : step + 1]
    sum_ref[...] = jnp.zeros(sum_ref.shape, F32)
    for k in range(n_shot):
        base = partner_of(lax.axis_index("shot"), k, n_shot) * (capacity + 1)
        for r in range(capacity):

            @pl.when(r < table_ref[base + capacity])
            def _():
                slot = table_ref[base + r]
                sum_ref[slot] = sum_ref[slot] + blocks[k][r]


def finish_call(table, blocks, parts, lat_dev):
    depth, cells = blocks[0].shape[1:]
    steps, n = parts[0].shape
    return pl.pallas_call(
        functools.partial(finish_kernel, len(blocks)),
        out_shape=[sds((lat_dev, depth, cells)), sds((steps, 1, n))],
        in_specs=[VMEM] * (1 + len(blocks) + len(parts)),
        out_specs=[VMEM, VMEM],
        scratch_shapes=[pltpu.SMEM((len(blocks) * (blocks[0].shape[0] + 1),), jnp.int32)],
        compiler_params=params(8),
        name="finish",
    )(table, *blocks, *parts)


def swap(edges):
    count = lax.axis_size("slab")
    shots = lax.axis_size("shot")
    got = []
    for start, edge in enumerate(edges):
        pairs = {}
        for shot in range(shots):
            for i in range(count):
                other = i + 1 if (i - start) % 2 == 0 else i - 1
                if 0 <= other < count:
                    pairs[shot * count + i] = shot * count + other
                elif shots % 2 == 0:
                    pairs[shot * count + i] = (shot ^ 1) * count + i
        got.append(lax.ppermute(edge, ("shot", "slab"), sorted(pairs.items())))
    return tuple(got)


def edges_kernel(n, *refs):
    fields, outs, sems = refs[:n], refs[n:-1], refs[-1]
    depth = fields[0].shape[1]
    low = jnp.where(place()[0] == 1, 0, depth - HALO)
    copies = []
    for out_ref, at in zip(outs, (low, depth - HALO - low)):
        for index, field_ref in enumerate(fields):
            for z in range(HALO):
                copies.append(
                    pltpu.make_async_copy(field_ref.at[0, at + z], out_ref.at[index, z], sems.at[len(copies)])
                )
    for copy in copies:
        copy.start()
    for copy in copies:
        copy.wait()


def first_edges(fields):
    n = len(fields)
    edge = sds((n, HALO) + fields[0].shape[2:])
    return pl.pallas_call(
        functools.partial(edges_kernel, n),
        out_shape=[edge, edge],
        in_specs=[HBM] * n,
        out_specs=[VMEM, VMEM],
        scratch_shapes=[pltpu.SemaphoreType.DMA((2 * n * HALO,))],
        compiler_params=params(8),
    )(*map(in_hbm, fields))


def partners():
    count = lax.axis_size("shot")
    if count & (count - 1) == 0:
        return [[s ^ k for s in range(count)] for k in range(count)]
    return [[(k - s) % count for s in range(count)] for k in range(count)]


def rounds(count):
    return sorted(range(count), key=lambda k: (-(k >> 1).bit_count(), k))


def exchange(blocks):
    got = [None] * len(blocks)
    for k in rounds(len(blocks)):
        block, to = blocks[k], partners()[k]
        moves = [(s, t) for s, t in enumerate(to) if s != t]
        kept = [s for s, t in enumerate(to) if s == t]
        if kept and moves:
            moves = moves + [(s, s) for s in kept]
        got[k] = lax.ppermute(block, "shot", moves) if moves else block
    return got


def slab_parts(part):
    count = lax.axis_size("slab")
    parts = [part]
    for k in range(count - 1, 0, -1):
        to = [s ^ k for s in range(count)] if count & (count - 1) == 0 else [(s + k) % count for s in range(count)]
        parts.append(lax.ppermute(part, "slab", list(enumerate(to))))
    return parts


def per_device(
    model_tiles,
    background,
    u_prev,
    u_now,
    du_prev,
    du_now,
    w_prev,
    w_now,
    wavelet,
    source_cell,
    receiver_cells,
    aperture,
    tile_slot,
):
    lat_dev, depth, tile_cells = model_tiles.shape
    side = background.shape[-1]
    tile_side = math.isqrt(tile_cells)
    capacity = aperture.shape[1] // 4
    n_shot = lax.axis_size("shot")
    steps = wavelet.shape[1]
    speed = background[0]
    u, d, w = u_now[0], du_now[0], w_now[0]
    up, dp, wp = u_prev[0], du_prev[0], w_prev[0]

    u_halo = swap(first_edges([u_now]))
    dw_halo = swap(first_edges([du_now, w_now]))
    outgoing, table, place_row = pack_call(aperture, tile_slot, model_tiles, capacity)
    incoming = exchange(outgoing)
    count, outer = count_call(receiver_cells, depth, side)
    perturb = perturb_call(place_row, incoming, side, tile_side, aperture.shape[1])
    tiling = (place_row, n_shot, aperture.shape[1], tile_side)

    u_next, lap, corr, *edges = u_call(0, False, wavelet, source_cell, u, up, u_halo, speed, w_now, None, None, *tiling)
    u_halo = swap(edges)
    bare, *edges = w_bare_call(w, wp, dw_halo, 1, speed)
    w_halo = swap(edges)
    d_next, w_next, *edges = d_call(d, dp, dw_halo, 0, speed, perturb, lap, bare, count)
    d_halo = swap(edges)
    traces = u_local = None
    for step in range(1, steps - 1):
        traces, receiver_rows = record_call(receiver_cells, traces, [d_next])
        u, up, d, dp, w, wp = u_next, u, d_next, d, w_next, w
        u_next, lap, corr, *edges = u_call(
            step, False, wavelet, source_cell, u, up, u_halo, speed, w, corr, u_local, *tiling
        )
        u_halo = swap(edges)
        u_local, d_local, w_local = ahead_call([u_next, d, w])
        d_next, w_next, *edges = dw_call(
            d, dp, w, wp, d_halo, w_halo, d_local, w_local, speed, perturb, lap, count, outer if step == 1 else None
        )
        d_halo = swap(edges[:2])
        w_halo = swap(edges[2:])
    u, up, d, dp, w, wp = u_next, u, d_next, d, w_next, w
    step = steps - 1
    lap, *returning = u_call(step, True, wavelet, source_cell, u, up, u_halo, speed, w, corr, u_local, *tiling)
    arrived = exchange(returning)
    d_final, d_next, traces = last_d_call(
        step, d, dp, d_halo, speed, perturb, lap, receiver_cells, receiver_rows, traces
    )
    parts = slab_parts(traces)
    w_final, u_final = last_w_call(w, wp, w_halo, speed, count, d_next, u, up, lap, source_cell, wavelet)
    sensitivity, traces = finish_call(table, arrived, parts, lat_dev)
    return (sensitivity, u_final, d_final, w_final, jnp.transpose(traces, (1, 0, 2)))


def solution(mesh):
    field = P("shot", "slab", None, None)
    tiles = P("shot", "slab", None)
    in_specs = (tiles,) + (field,) * 7 + (P("shot", None), P("shot"), P("shot", None), P(), P())
    out_specs = (tiles, field, field, field, P("shot", None, None))


    return jax.shard_map(per_device, mesh=mesh, in_specs=in_specs, out_specs=out_specs, check_vma=False)
```
